512 devices in a mesh: gx: 8 (over y), gy: 8 (over x, core), gz: 8 (over z).
Axes of the slice: x: 4, y: 8, z: 8, core: 2. Of those that a mesh axis runs over, the one named last changes fastest.
Arguments:
- pressure: float32 [96, 128, 1024], P('gx', 'gy', 'gz'), may hold values from -8 to 8
- wind: float32 [3, 96, 128, 1024], P(None, 'gx', 'gy', 'gz'), may hold values from -6 to 6
Outputs:
- result: float32 [96, 128, 1024], P('gx', 'gy', 'gz')
The draws below stay inside these ranges and needn't reach their ends.
All inputs are finite; a program needn't handle non-finite values.
Results may differ from the reference program's by a relative error of at most 0.00019.
Values sent between devices are 32-bit elements; how exact they have to be, the bound alone decides.
A program may use at most 64 MiB of HBM per device.

```python
import jax
import jax.numpy as jnp

SWEEPS = 2
COARSE_SWEEPS = 4
CYCLES = 1
NX = 96
NY = 128
NZ = 1024


def draw_pressure(key, part):
    noise = jax.random.normal(key, (NX, NY, NZ), jnp.float32)
    return jnp.clip(noise, -8.0, 8.0)


def level_of(own_key, dims, split, low, high):
    factor_of = 1.0
    for dim, blocks in split:
        draws = jax.random.uniform(jax.random.fold_in(jax.random.fold_in(own_key, 6), dim), (blocks,), jnp.float32, low / len(split), high / len(split))
        factor_of = factor_of * jnp.repeat(jnp.exp(draws), dims[dim] // blocks).reshape((-1,) + (1,) * (len(dims) - 1 - dim))
    return factor_of


def normal_values(key, shape, deviation, limit, shards=(), held_as=jnp.bfloat16):
    array = jax.random.normal(key, shape, jnp.float32) * deviation
    if len(shards) > 0:
        array = level_of(key, shape, shards, -0.22, 0.18) * array
    return jnp.clip(array, min=-limit, max=limit).astype(held_as)


def setup_inputs(seed: int = 0) -> dict:
    keys = jax.random.split(jax.random.key(seed), 3)
    pressure = draw_pressure(jax.random.fold_in(keys[2], 71), 0)
    wind = normal_values(keys[1], (3, NX, NY, NZ), 1.0, 6.0, ((1, 8), (2, 8), (3, 8)), jnp.float32)
    return {"pressure": pressure, "wind": wind}


OMEGA = 0.8
VISCOSITY = 1.0
REACTION = 1.0


def six_sum(padded):
    return (padded[..., 2:, 1:-1, 1:-1] + padded[..., :-2, 1:-1, 1:-1]
            + padded[..., 1:-1, 2:, 1:-1] + padded[..., 1:-1, :-2, 1:-1]
            + padded[..., 1:-1, 1:-1, 2:] + padded[..., 1:-1, 1:-1, :-2])


def central_parts(padded):
    return ((padded[..., 2:, 1:-1, 1:-1] - padded[..., :-2, 1:-1, 1:-1]) * 0.5,
            (padded[..., 1:-1, 2:, 1:-1] - padded[..., 1:-1, :-2, 1:-1]) * 0.5,
            (padded[..., 1:-1, 1:-1, 2:] - padded[..., 1:-1, 1:-1, :-2]) * 0.5)


def pad_space(values):
    return jnp.pad(values, [(0, 0)] * (values.ndim - 3) + [(1, 1), (1, 1), (1, 1)])


def laplace(values, padded, weight_scale):
    return weight_scale * (6.0 * values - six_sum(padded))


def sweep(source, values, padded, weight_scale):
    return values + (OMEGA / (6.0 * weight_scale)) * (source - laplace(values, padded, weight_scale))


def start_sweep(source, weight_scale):
    return (OMEGA / (6.0 * weight_scale)) * source


def smooth(source, values, weight_scale, sweep_count):
    for sweep_number in range(sweep_count):
        if values is None:
            values = start_sweep(source, weight_scale)
        else:
            values = sweep(source, values, pad_space(values), weight_scale)
    return values


def restrict(values):
    extent_x, extent_y, extent_z = values.shape
    blocks = values.reshape(extent_x // 2, 2, extent_y // 2, 2, extent_z // 2, 2)
    return 0.125 * jnp.sum(blocks, axis=(1, 3, 5))


def prolong(values):
    extent_x, extent_y, extent_z = values.shape
    spread = jnp.broadcast_to(values[:, None, :, None, :, None], (extent_x, 2, extent_y, 2, extent_z, 2))
    return spread.reshape(2 * extent_x, 2 * extent_y, 2 * extent_z)


def vcycle(source, values, depth_index):
    weight_scale = 0.25 ** depth_index
    if depth_index == 2:
        return smooth(source, None, weight_scale, COARSE_SWEEPS)
    values = smooth(source, values, weight_scale, SWEEPS)
    residual = source - laplace(values, pad_space(values), weight_scale)
    correction = vcycle(restrict(residual), None, depth_index + 1)
    values = values + prolong(correction)
    return smooth(source, values, weight_scale, SWEEPS)


def solve(source):
    values = None
    for cycle_number in range(CYCLES):
        values = vcycle(source, values, 0)
    return values


def momentum(padded_velocity, wind):
    centre = padded_velocity[:, 1:-1, 1:-1, 1:-1]
    diffusion = 6.0 * centre - six_sum(padded_velocity)
    slopes = central_parts(padded_velocity)
    convection = wind[0:1] * slopes[0] + wind[1:2] * slopes[1] + wind[2:3] * slopes[2]
    return REACTION * centre + VISCOSITY * diffusion + convection


def reference(pressure, wind):
    first = solve(pressure)
    velocity = jnp.stack(central_parts(pad_space(first)))
    flux = momentum(pad_space(velocity), wind)
    slopes = central_parts(pad_space(flux))
    product = -(slopes[0][0] + slopes[1][1] + slopes[2][2])
    return solve(product)
```

```python
import functools

import jax
import jax.numpy as jnp
from jax import lax
from jax.experimental import pallas as pl
from jax.experimental.pallas import tpu as pltpu
from jax.sharding import PartitionSpec as P

MESH = pl.DeviceIdType.MESH
AXES = ("gx", "gy", "gz")
BX, BY, BZ = 12, 16, 128
OMEGA = 0.8
KEEP = 1.0 - OMEGA
SIXTH = OMEGA / 6.0

AROUND = [
    (dx, dy, dz)
    for dz in (0, 1, -1)
    for dx in (0, 1, -1)
    for dy in (0, 1, -1)
    if (dx, dy, dz) != (0, 0, 0)
]
AROUND.sort(key=lambda d: -(abs(d[0]) + abs(d[1]) + abs(d[2])))
COARSE_X = [(2, 0, 0), (-2, 0, 0), (1, 0, 0), (-1, 0, 0)]
COARSE_YZ = [(0, dy, dz) for dz in (1, -1, 0) for dy in (2, -2, 1, -1, 0) if (dy, dz) != (0, 0)]
GREETED = AROUND + [d for d in COARSE_X + COARSE_YZ if d not in AROUND]


def part(delta, count, width):
    if delta == 0:
        return 0, 0, count
    if delta > 0:
        return count - width, -width, width
    return 0, count, width


class Place:
    def __init__(self, sizes):
        self.sizes = sizes
        self.at = [lax.axis_index(a) for a in AXES]
        self.has = []
        for g, n in zip(self.at, sizes):
            self.has.append({d: (g + d >= 0) & (g + d < n) for d in (-2, -1, 1, 2)})

    def exists(self, offset):
        found = None
        for table, d in zip(self.has, offset):
            if d:
                found = table[d] if found is None else found & table[d]
        return found

    def device(self, offset):
        return tuple(
            lax.rem(g + (d + n), n) if d else g for g, d, n in zip(self.at, offset, self.sizes)
        )


class Exchange:
    def __init__(self, place, copies, send_sems, recv_sems, base):
        self.place, self.items = place, []
        for k, (offset, src, dst) in enumerate(copies):
            copy = pltpu.make_async_remote_copy(
                src_ref=src,
                dst_ref=dst,
                send_sem=send_sems.at[base + k],
                recv_sem=recv_sems.at[base + k],
                device_id=place.device(offset),
                device_id_type=MESH,
            )
            self.items.append((offset, copy))

    def start(self):
        for offset, copy in self.items:
            pl.when(self.place.exists(offset))(copy.start)

    def wait_recv(self):
        for offset, copy in self.items:
            pl.when(self.place.exists(tuple(-d for d in offset)))(copy.wait_recv)

    def wait_send(self):
        for offset, copy in self.items:
            pl.when(self.place.exists(offset))(copy.wait_send)


def lanes(rows):
    return lax.broadcasted_iota(jnp.int32, (rows, 128), 1)


def row_mask(place, first_row, rows, extent):
    y = first_row + lax.broadcasted_iota(jnp.int32, (rows, 128), 0)
    low = jnp.where(place.has[1][-1], -64, 0)
    high = jnp.where(place.has[1][1], 64, extent)
    return (y >= low) & (y < high)


def rim_lanes(place, rows, start, right_end):
    lane = lanes(rows)
    right_stop = jnp.where(place.has[2][1], right_end, 0)
    left_start = jnp.where(place.has[2][-1], 120, 128)
    return ((lane >= start) & (lane < right_stop)) | (lane >= left_start)


def slab_weight(place, x, extent):
    if x < 0:
        return place.has[0][-1].astype(jnp.float32)
    if x >= extent:
        return place.has[0][1].astype(jnp.float32)
    return None


def z_back(a, h):
    lane0 = lanes(a.shape[0]) == 0
    ra, rh = pltpu.roll(a, 1, 1), pltpu.roll(h, 1, 1)
    return jnp.where(lane0, rh, ra), jnp.where(lane0, ra, rh)


def z_next(a, h):
    lane127 = lanes(a.shape[0]) == 127
    ra, rh = pltpu.roll(a, 127, 1), pltpu.roll(h, 127, 1)
    return jnp.where(lane127, rh, ra), jnp.where(lane127, ra, rh)


def masks0(place, first_row, rows):
    inner = row_mask(place, first_row, rows, BY)
    rim = inner & rim_lanes(place, rows, 0, 8)
    return inner.astype(jnp.float32), rim.astype(jnp.float32)


def scaled(value, mask, weight):
    value = value * mask
    return value if weight is None else value * weight


def six0(ref, i, r, n, rim=True):
    a, h = ref[0, i, r : r + n, :], ref[1, i, r : r + n, :]
    ba, bh = z_back(a, h)
    na, nh = z_next(a, h)
    out = []
    for t, (c, b, f) in enumerate(((a, ba, na), (h, bh, nh))):
        if t and not rim:
            break
        s = (
            (ref[t, i - 1, r : r + n, :] + ref[t, i + 1, r : r + n, :])
            + (ref[t, i, r - 1 : r - 1 + n, :] + ref[t, i, r + 1 : r + 1 + n, :])
            + (b + f)
        )
        out.append((c, s))
    return out


def six1(ref, i, r, n):
    c = ref[i, r : r + n, :]
    s = (
        (ref[i - 1, r : r + n, :] + ref[i + 1, r : r + n, :])
        + (ref[i, r - 1 : r - 1 + n, :] + ref[i, r + 1 : r + 1 + n, :])
        + (pltpu.roll(c, 1, 1) + pltpu.roll(c, 127, 1))
    )
    return c, s


def dot(a, b):
    return jnp.dot(
        a, b, precision=lax.Precision.HIGHEST, preferred_element_type=jnp.float32
    )


def pack0(load, store):
    lane = lanes(BY)
    first = jnp.zeros((BY, 128), jnp.float32)
    last = jnp.zeros((BY, 128), jnp.float32)
    for i in range(BX):
        turned = pltpu.roll(load(i), 8 * i, 1) if i else load(i)
        first = jnp.where((lane >= 8 * i) & (lane < 8 * i + 8), turned, first)
        at = (8 * i - 8) % 128
        last = jnp.where((lane >= at) & (lane < at + 8), turned, last)
    store(first, last)


def unpack0(land, x, rows):
    dx, i = (0, x) if 0 <= x < BX else ((-1, x + BX) if x < 0 else (1, x - BX))
    left, right = land[0, dx + 1], land[1, dx + 1]
    if i:
        left, right = pltpu.roll(left, 128 - 8 * i, 1), pltpu.roll(right, 128 - 8 * i, 1)
    lane = lanes(rows)
    return jnp.where(lane < 8, right, jnp.where(lane >= 120, left, 0.0))


def rim_copies(source, land):
    out = []
    for offset in AROUND:
        dx, dy, dz = offset
        if dz == 0:
            continue
        y0, yd, ny = part(dy, BY, 8)
        side = 0 if dz > 0 else 1
        out.append((offset, source(side, y0, ny), land(side, 1 - dx, yd, ny)))
    return out


def block_copies(source, land, h):
    out = []
    for offset in AROUND:
        dx, dy, dz = offset
        if dz != 0:
            continue
        x0, xd, nx = part(dx, BX, h)
        y0, yd, ny = part(dy, BY, 8)
        out.append((offset, source(x0, nx, y0, ny), land(xd, nx, yd, ny)))
    return out


def ordered(copies):
    return sorted(copies, key=lambda c: -sum(abs(d) for d in c[0]))


def kernel(
    sizes, p_ref, w_ref, out_ref,
    b0, v0, zs0, zr0, first, zsf, zrf, wind, zsw, zrw, velocity, flux,
    s1, l1, b1, v1, zs1, zr1, gathered, merged, c2, e2a, e2b,
    rows0, rows2, up1, up0, m_down0, m_down1, m_up1, m_up0,
    send_sems, recv_sems, load_sem,
):
    place = Place(sizes)

    load = pltpu.make_async_copy(w_ref, wind.at[:, 0, pl.ds(4, BX), pl.ds(8, BY), :], load_sem)
    for ref in (b0, zr0, first, zrf, zrw, l1, zr1, gathered):
        ref[...] = jnp.zeros(ref.shape, ref.dtype)
    wind[...] = jnp.zeros(wind.shape, wind.dtype)

    barrier = pltpu.get_barrier_semaphore()
    total = jnp.int32(0)
    for offset in GREETED:
        there = place.exists(offset)
        total = total + there.astype(jnp.int32)

        def greet(offset=offset):
            pl.semaphore_signal(
                barrier, inc=1, device_id=place.device(offset), device_id_type=MESH
            )

        pl.when(there)(greet)

    load.start()
    pack0(lambda i: p_ref[i], lambda f, l: (zs0.__setitem__(0, l), zs0.__setitem__(1, f)))
    for i in range(BX):
        b0[0, 3 + i, 8:24, :] = p_ref[i]
    for ref in (v0, velocity, flux, b1, v1, merged, c2, e2a, e2b, rows0, rows2, up1, up0):
        ref[...] = jnp.zeros(ref.shape, ref.dtype)

    k = lax.broadcasted_iota(jnp.int32, (128, 128), 0)
    l = lax.broadcasted_iota(jnp.int32, (128, 128), 1)
    m_down0[...] = (k // 2 == l).astype(jnp.float32) * 0.125
    for i in range(3):
        m_down1[i * 128 : i * 128 + 128, :] = (
            (l // 32 == i) & (k // 2 == l % 32)
        ).astype(jnp.float32) * 0.125
    m_up1[...] = (((l < 72) & (k == l // 2)) | ((l >= 120) & (k == 64 + l // 2))).astype(jnp.float32)
    m_up0[:, 0:128] = (k == l // 2).astype(jnp.float32)
    m_up0[:, 128:256] = (((l < 8) | (l >= 120)) & (k == 64 + l // 2)).astype(jnp.float32)

    def rows8(ref, x, nx, y, ny, lead):
        return ref.at[pl.ds(x, nx), pl.ds(y + lead, ny), :]

    ex0 = Exchange(place, ordered(
        block_copies(
            lambda x, nx, y, ny: p_ref.at[pl.ds(x, nx), pl.ds(y, ny), :],
            lambda x, nx, y, ny: b0.at[0, pl.ds(x + 3, nx), pl.ds(y + 8, ny), :], 3)
        + rim_copies(
            lambda s, y, ny: zs0.at[s, pl.ds(y, ny), :],
            lambda s, dx, y, ny: zr0.at[s, dx, pl.ds(y + 8, ny), :])
    ), send_sems, recv_sems, 0)
    exw = Exchange(place, ordered(
        block_copies(
            lambda x, nx, y, ny: w_ref.at[:, pl.ds(x, nx), pl.ds(y, ny), :],
            lambda x, nx, y, ny: wind.at[:, 0, pl.ds(x + 4, nx), pl.ds(y + 8, ny), :], 4)
        + rim_copies(
            lambda s, y, ny: zsw.at[s, :, pl.ds(y, ny), :],
            lambda s, dx, y, ny: zrw.at[s, dx, :, pl.ds(y + 8, ny), :])
    ), send_sems, recv_sems, 26)
    exf = Exchange(place, ordered(
        block_copies(
            lambda x, nx, y, ny: first.at[0, pl.ds(x + 6, nx), pl.ds(y + 16, ny), :],
            lambda x, nx, y, ny: first.at[0, pl.ds(x + 6, nx), pl.ds(y + 16, ny), :], 6)
        + rim_copies(
            lambda s, y, ny: zsf.at[s, pl.ds(y, ny), :],
            lambda s, dx, y, ny: zrf.at[s, dx, pl.ds(y + 8, ny), :])
    ), send_sems, recv_sems, 52)

    def level1_exchange(solve, base):
        out = []
        for offset in AROUND:
            dx, dy, dz = offset
            if dz == 0:
                x0, xd, nx = part(dx, 6, 4)
                out.append((
                    offset,
                    s1.at[solve, pl.ds(x0, nx)],
                    l1.at[solve, pl.ds(xd + 4, nx), pl.ds(8 - 8 * dy, 8), :],
                ))
            else:
                side = 0 if dz > 0 else 1
                out.append((
                    offset, zs1.at[solve, side], zr1.at[solve, side, 1 - dx, pl.ds(8 - 8 * dy, 8), :],
                ))
        return Exchange(place, ordered(out), send_sems, recv_sems, base)

    def coarse_exchanges(solve, base):
        a = [(d, gathered.at[solve, 2, 1, 2], gathered.at[solve, 2, 1, 2 - d[0]]) for d in COARSE_X]
        b = [(d, gathered.at[solve, 2, 1], gathered.at[solve, 2 - d[1], 1 - d[2]]) for d in COARSE_YZ]
        return (
            Exchange(place, a, send_sems, recv_sems, base),
            Exchange(place, b, send_sems, recv_sems, base + 4),
        )

    pl.semaphore_wait(barrier, total)
    ex0.start()

    load.wait()

    def store_wind_pack(d):
        def store(f, l):
            zsw[0, d] = l
            zsw[1, d] = f
        return store

    for d in range(3):
        pack0(lambda i: wind[d, 0, 4 + i, 8:24, :], store_wind_pack(d))

    ex0.wait_recv()
    for x in range(-3, BX + 3):
        b0[1, x + 3] = unpack0(zr0, x, 32)

    def solve(number, base, result):
        c0 = OMEGA / 6.0
        mask_a, mask_h = masks0(place, -4, 24)
        for x in range(-2, BX + 2):
            weight = slab_weight(place, x, BX)
            for t, (c, s) in enumerate(six0(b0, x + 3, 4, 24)):
                value = (1.0 + KEEP) * c0 * c + SIXTH * c0 * s
                v0[t, x + 3, 4:28, :] = scaled(value, (mask_a, mask_h)[t], weight)
        for i in range(6):
            pair = None
            for x in (2 * i, 2 * i + 1):
                ((c, s),) = six0(v0, x + 3, 8, 16, rim=False)
                r = b0[0, x + 3, 8:24, :] - (6.0 * c - s)
                pair = r if pair is None else pair + r
            rows0[i] = pair
        halves = [rows0[i, pl.ds(0, 8, stride=2), :] + rows0[i, pl.ds(1, 8, stride=2), :] for i in range(6)]
        source = dot(jnp.concatenate(halves, axis=0), m_down0[...])

        lane8 = lanes(8)
        low = jnp.zeros((8, 128), jnp.float32)
        high = jnp.zeros((8, 128), jnp.float32)
        for i in range(6):
            block = source[8 * i : 8 * i + 8, :]
            s1[number, i] = block
            l1[number, 4 + i, 8:16, :] = block
            group = (lane8 >= 8 * i) & (lane8 < 8 * i + 8)
            low = jnp.where(group, pltpu.roll(block, 8 * i, 1) if i else block, low)
            high = jnp.where(group, pltpu.roll(block, (8 * i - 56) % 128, 1), high)
        zs1[number, 0] = high
        zs1[number, 1] = low
        ex1 = level1_exchange(number, base)
        ex1.start()
        if number == 0:
            exw.start()
        (ex0 if number == 0 else exf).wait_send()
        ex1.wait_recv()
        lane24 = lanes(24)
        for x in range(-4, 10):
            dx, i = (0, x) if 0 <= x < 6 else ((-1, x + 6) if x < 0 else (1, x - 6))
            left = pltpu.roll(zr1[number, 0, dx + 1], (120 - 8 * i) % 128, 1)
            right = pltpu.roll(zr1[number, 1, dx + 1], (64 - 8 * i) % 128, 1)
            b1[x + 4] = jnp.where(
                lane24 < 64,
                l1[number, x + 4],
                jnp.where(lane24 < 72, right, jnp.where(lane24 >= 120, left, 0.0)),
            )
        w1 = 0.25
        c1 = OMEGA / (6.0 * w1)
        inside = row_mask(place, -4, 16, 8)
        lane16 = lanes(16)
        mask1 = (inside & ((lane16 < 64) | rim_lanes(place, 16, 64, 72))).astype(jnp.float32)
        for x in range(-3, 9):
            c, s = six1(b1, x + 4, 4, 16)
            value = (1.0 + KEEP) * c1 * c + SIXTH * c1 * s
            v1[x + 4, 4:20, :] = scaled(value, mask1, slab_weight(place, x, 6))
        pairs = []
        for i in range(3):
            pair = None
            for x in (2 * i, 2 * i + 1):
                c, s = six1(v1, x + 4, 8, 8)
                r = b1[x + 4, 8:16, :] - w1 * (6.0 * c - s)
                pair = r if pair is None else pair + r
            pairs.append(pair)
        rows2[...] = dot(jnp.concatenate(pairs, axis=1), m_down1[...])
        gathered[number, 2, 1, 2] = rows2[pl.ds(0, 4, stride=2), :] + rows2[pl.ds(1, 4, stride=2), :]

        exa, exb = coarse_exchanges(number, base + 26)
        exa.start()
        ex1.wait_send()
        exa.wait_recv()
        exb.start()
        exb.wait_recv()
        for az in range(3):
            for ax in range(5):
                for ay in range(5):
                    merged[az, ax, 4 * ay : 4 * ay + 4, :] = gathered[number, ay, az, ax]
        for x in range(-5, 8):
            ax, i = (x + 6) // 3, (x + 6) % 3
            parts = [
                pltpu.roll(merged[az, ax], (to - 32 * i) % 128, 1) if (to - 32 * i) % 128 else merged[az, ax]
                for az, to in ((0, 96), (1, 0), (2, 32))
            ]
            c2[x + 5] = jnp.where(
                lane24 < 32,
                parts[1],
                jnp.where(lane24 < 40, parts[2], jnp.where(lane24 >= 120, parts[0], 0.0)),
            )
        w2 = 0.0625
        c2_scale = OMEGA / (6.0 * w2)
        inside = row_mask(place, -6, 16, 4)
        mask2 = (inside & ((lane16 < 32) | rim_lanes(place, 16, 32, 40))).astype(jnp.float32)
        for x in range(-4, 7):
            c, s = six1(c2, x + 5, 2, 16)
            value = (1.0 + KEEP) * c2_scale * c + SIXTH * c2_scale * s
            e2a[x + 5, 2:18, :] = scaled(value, mask2, slab_weight(place, x, 3))
        source_ref, target = e2a, e2b
        for reach in (3, 2):
            for x in range(-reach, 3 + reach):
                c, s = six1(source_ref, x + 5, 2, 16)
                value = KEEP * c + SIXTH * s + c2_scale * c2[x + 5, 2:18, :]
                target[x + 5, 2:18, :] = scaled(value, mask2, slab_weight(place, x, 3))
            source_ref, target = target, source_ref

        spread = dot(
            jnp.concatenate([source_ref[x + 5, 6:14, :] for x in range(-2, 5)], axis=0), m_up1[...]
        )
        for j in range(7):
            value = spread[8 * j : 8 * j + 8, :]
            up1[j, pl.ds(0, 8, stride=2), :] = value
            up1[j, pl.ds(1, 8, stride=2), :] = value
        for x in range(-3, 9):
            v1[x + 4, 4:20, :] += scaled(up1[(x + 4) // 2], mask1, slab_weight(place, x, 6))
        for x in range(-2, 8):
            c, s = six1(v1, x + 4, 4, 16)
            value = KEEP * c + SIXTH * s + c1 * b1[x + 4, 4:20, :]
            up0[0, x + 2, 4:20, :] = scaled(value, mask1, slab_weight(place, x, 6))
        for x in range(-1, 7):
            c, s = six1(up0.at[0], x + 2, 4, 16)
            value = KEEP * c + SIXTH * s + c1 * b1[x + 4, 4:20, :]
            v1[x + 4, 4:20, :] = scaled(value, mask1, slab_weight(place, x, 6))

        spread = dot(
            jnp.concatenate([v1[x + 4, 6:22, :] for x in range(-1, 7)], axis=0), m_up0[...]
        )
        for j in range(8):
            for t in range(2):
                value = spread[16 * j : 16 * j + 12, 128 * t : 128 * t + 128]
                up0[t, j, pl.ds(0, 12, stride=2), :] = value
                up0[t, j, pl.ds(1, 12, stride=2), :] = value
        for x in range(-2, BX + 2):
            weight = slab_weight(place, x, BX)
            for t in range(2):
                v0[t, x + 3, 4:28, :] += scaled(
                    up0[t, (x + 2) // 2, 0:24, :], (mask_a, mask_h)[t], weight
                )
        for x in range(-1, BX + 1):
            weight = slab_weight(place, x, BX)
            for t, (c, s) in enumerate(six0(v0, x + 3, 4, 24)):
                value = KEEP * c + SIXTH * s + c0 * b0[t, x + 3, 4:28, :]
                flux[t // 2, t, x + 1, 4:28, :] = scaled(value, (mask_a, mask_h)[t], weight)
        for x in range(BX):
            ((c, s),) = six0(flux.at[0], x + 1, 8, 16, rim=False)
            result(x, KEEP * c + SIXTH * s + c0 * b0[0, x + 3, 8:24, :])
        return exa, exb

    def keep_first(x, value):
        first[0, x + 6, 16:32, :] = value

    exa, exb = solve(0, 78, keep_first)
    pack0(
        lambda i: first[0, 6 + i, 16:32, :],
        lambda f, l: (zsf.__setitem__(0, l), zsf.__setitem__(1, f)),
    )
    exf.start()
    exa.wait_send()
    exb.wait_send()
    exw.wait_recv()
    exw.wait_send()
    for d in range(3):
        for x in range(-4, BX + 4):
            wind[d, 1, x + 4] = unpack0(zrw.at[:, :, d], x, 32)
    exf.wait_recv()
    for x in range(-6, BX + 6):
        first[1, x + 6, 8:40, :] = unpack0(zrf, x, 32)

    mask_a, mask_h = masks0(place, -8, 32)
    for x in range(-5, BX + 5):
        weight = slab_weight(place, x, BX)
        half = 0.5 if weight is None else 0.5 * weight
        half_a, half_h = mask_a * half, mask_h * half
        i = x + 6
        a, h = first[0, i, 8:40, :], first[1, i, 8:40, :]
        ba, bh = z_back(a, h)
        na, nh = z_next(a, h)
        for t, (b, n, m) in enumerate(((ba, na, half_a), (bh, nh, half_h))):
            velocity[0, t, x + 5, 8:40, :] = (first[t, i + 1, 8:40, :] - first[t, i - 1, 8:40, :]) * m
            velocity[1, t, x + 5, 8:40, :] = (first[t, i, 9:41, :] - first[t, i, 7:39, :]) * m
            velocity[2, t, x + 5, 8:40, :] = (n - b) * m
    mask_a, mask_h = masks0(place, -4, 24)
    for x in range(-4, BX + 4):
        weight = slab_weight(place, x, BX)
        i = x + 5
        half_wind = [[0.5 * wind[e, t, x + 4, 4:28, :] for t in range(2)] for e in range(3)]
        for d in range(3):
            u = velocity.at[d]
            a, h = u[0, i, 12:36, :], u[1, i, 12:36, :]
            ba, bh = z_back(a, h)
            na, nh = z_next(a, h)
            for t, (c, b, n, m) in enumerate(((a, ba, na, mask_a), (h, bh, nh, mask_h))):
                x_low, x_high = u[t, i - 1, 12:36, :], u[t, i + 1, 12:36, :]
                y_low, y_high = u[t, i, 11:35, :], u[t, i, 13:37, :]
                value = (
                    7.0 * c
                    - ((x_low + x_high) + (y_low + y_high) + (b + n))
                    + half_wind[0][t] * (x_high - x_low)
                    + half_wind[1][t] * (y_high - y_low)
                    + half_wind[2][t] * (n - b)
                )
                flux[d, t, x + 4, 4:28, :] = scaled(value, m, weight)
    for x in range(-3, BX + 3):
        weight = slab_weight(place, x, BX)
        i = x + 4
        a, h = flux[2, 0, i, 4:28, :], flux[2, 1, i, 4:28, :]
        ba, bh = z_back(a, h)
        na, nh = z_next(a, h)
        for t, (b, n, m) in enumerate(((ba, na, mask_a), (bh, nh, mask_h))):
            value = (
                (flux[0, t, i + 1, 4:28, :] - flux[0, t, i - 1, 4:28, :])
                + (flux[1, t, i, 5:29, :] - flux[1, t, i, 3:27, :])
                + (n - b)
            ) * -0.5
            b0[t, x + 3, 4:28, :] = scaled(value, m, weight)

    def keep_result(x, value):
        out_ref[x] = value

    exa, exb = solve(1, 122, keep_result)
    exa.wait_send()
    exb.wait_send()


def solution(mesh):
    sizes = tuple(mesh.shape[a] for a in AXES)
    copies = 26 * 3 + 2 * (26 + 18)
    f32 = jnp.float32

    def vmem(*shape):
        return pltpu.VMEM(shape, f32)

    def body(pressure, wind):
        return pl.pallas_call(
            functools.partial(kernel, sizes),
            out_shape=jax.ShapeDtypeStruct((BX, BY, BZ), f32),
            in_specs=[
                pl.BlockSpec(memory_space=pltpu.VMEM),
                pl.BlockSpec(memory_space=pl.ANY),
            ],
            out_specs=pl.BlockSpec(memory_space=pltpu.VMEM),
            scratch_shapes=[
                vmem(2, 18, 32, 128),
                vmem(2, 18, 32, 128),
                vmem(2, 16, 128),
                vmem(2, 3, 32, 128),
                vmem(2, 24, 48, 128),
                vmem(2, 16, 128),
                vmem(2, 3, 32, 128),
                vmem(3, 2, 20, 32, 128),
                vmem(2, 3, 16, 128),
                vmem(2, 3, 3, 32, 128),
                vmem(3, 2, 22, 48, 128),
                vmem(3, 2, 20, 32, 128),
                vmem(2, 6, 8, 128),
                vmem(2, 14, 24, 128),
                vmem(14, 24, 128),
                vmem(14, 24, 128),
                vmem(2, 2, 8, 128),
                vmem(2, 2, 3, 24, 128),
                vmem(2, 5, 3, 5, 4, 128),
                vmem(3, 5, 24, 128),
                vmem(13, 24, 128),
                vmem(13, 24, 128),
                vmem(13, 24, 128),
                vmem(6, 16, 128),
                vmem(8, 128),
                vmem(7, 16, 128),
                vmem(2, 10, 24, 128),
                vmem(128, 128),
                vmem(384, 128),
                vmem(128, 128),
                vmem(128, 256),
                pltpu.SemaphoreType.DMA((copies,)),
                pltpu.SemaphoreType.DMA((copies,)),
                pltpu.SemaphoreType.DMA,
            ],
            compiler_params=pltpu.CompilerParams(
                collective_id=0, has_side_effects=True, vmem_limit_bytes=48 * 1024 * 1024
            ),
            name="schur",
        )(pressure, wind)

    in_specs = (P("gx", "gy", "gz"), P(None, "gx", "gy", "gz"))
    return jax.shard_map(
        body, mesh=mesh, in_specs=in_specs, out_specs=P("gx", "gy", "gz"), check_vma=False
    )
```

```python
import functools

import jax
import jax.numpy as jnp
from jax import lax
from jax.experimental import pallas as pl
from jax.experimental.pallas import tpu as pltpu
from jax.sharding import PartitionSpec as P

MESH = pl.DeviceIdType.MESH
AXES = ("gx", "gy", "gz")
BX, BY, BZ = 12, 16, 128
OMEGA = 0.8
KEEP = 1.0 - OMEGA
SIXTH = OMEGA / 6.0

AROUND = [
    (dx, dy, dz)
    for dz in (0, 1, -1)
    for dx in (0, 1, -1)
    for dy in (0, 1, -1)
    if (dx, dy, dz) != (0, 0, 0)
]
AROUND.sort(key=lambda d: -(abs(d[0]) + abs(d[1]) + abs(d[2])))

NEAR = [d for d in AROUND if sum(map(abs, d)) <= 2]


def coarse_offsets(far_edges):
    out = []
    for dx in range(-2, 3):
        for dy in range(-2, 3):
            for dz in (-1, 0, 1):
                shape = (abs(dx), abs(dy), abs(dz))
                if shape[:2] in ((0, 0), (0, 1), (1, 0), (1, 1), (0, 2), (2, 0), (2, 1)):
                    keep = shape != (0, 0, 0)
                else:
                    keep = far_edges and shape[:2] == (1, 2)
                if keep:
                    out.append((dx, dy, dz))
    return sorted(out, key=lambda d: -sum(map(abs, d)))


COARSE = (coarse_offsets(True), coarse_offsets(False))
GREETED = coarse_offsets(True)


def part(delta, count, width):
    if delta == 0:
        return 0, 0, count
    if delta > 0:
        return count - width, -width, width
    return 0, count, width


class Place:
    def __init__(self, sizes):
        self.sizes = sizes
        self.at = [lax.axis_index(a) for a in AXES]
        self.has = []
        for g, n in zip(self.at, sizes):
            self.has.append({d: (g + d >= 0) & (g + d < n) for d in (-2, -1, 1, 2)})

    def exists(self, offset):
        found = None
        for table, d in zip(self.has, offset):
            if d:
                found = table[d] if found is None else found & table[d]
        return found

    def device(self, offset):
        return tuple(
            lax.rem(g + (d + n), n) if d else g for g, d, n in zip(self.at, offset, self.sizes)
        )


class Exchange:
    def __init__(self, place, copies, send_sems, recv_sems, base):
        self.place, self.items = place, []
        for k, (offset, src, dst) in enumerate(copies):
            copy = pltpu.make_async_remote_copy(
                src_ref=src,
                dst_ref=dst,
                send_sem=send_sems.at[base + k],
                recv_sem=recv_sems.at[base + k],
                device_id=place.device(offset),
                device_id_type=MESH,
            )
            self.items.append((offset, copy))

    def start(self):
        for offset, copy in self.items:
            pl.when(self.place.exists(offset))(copy.start)

    def wait_recv(self):
        for offset, copy in self.items:
            pl.when(self.place.exists(tuple(-d for d in offset)))(copy.wait_recv)

    def wait_send(self):
        for offset, copy in self.items:
            pl.when(self.place.exists(offset))(copy.wait_send)


def lanes(rows):
    return lax.broadcasted_iota(jnp.int32, (rows, 128), 1)


def row_mask(place, first_row, rows, extent):
    y = first_row + lax.broadcasted_iota(jnp.int32, (rows, 128), 0)
    low = jnp.where(place.has[1][-1], -64, 0)
    high = jnp.where(place.has[1][1], 64, extent)
    return (y >= low) & (y < high)


def rim_lanes(place, rows, start, right_end):
    lane = lanes(rows)
    right_stop = jnp.where(place.has[2][1], right_end, 0)
    left_start = jnp.where(place.has[2][-1], 120, 128)
    return ((lane >= start) & (lane < right_stop)) | (lane >= left_start)


def slab_weight(place, x, extent):
    if x < 0:
        return place.has[0][-1].astype(jnp.float32)
    if x >= extent:
        return place.has[0][1].astype(jnp.float32)
    return None


def z_back(a, h):
    lane0 = lanes(a.shape[0]) == 0
    ra, rh = pltpu.roll(a, 1, 1), pltpu.roll(h, 1, 1)
    return jnp.where(lane0, rh, ra), jnp.where(lane0, ra, rh)


def z_next(a, h):
    lane127 = lanes(a.shape[0]) == 127
    ra, rh = pltpu.roll(a, 127, 1), pltpu.roll(h, 127, 1)
    return jnp.where(lane127, rh, ra), jnp.where(lane127, ra, rh)


def masks0(place, first_row, rows):
    inner = row_mask(place, first_row, rows, BY)
    rim = inner & rim_lanes(place, rows, 0, 8)
    return inner.astype(jnp.float32), rim.astype(jnp.float32)


def scaled(value, mask, weight):
    value = value * mask
    return value if weight is None else value * weight


def six0(ref, i, r, n, rim=True):
    a, h = ref[0, i, r : r + n, :], ref[1, i, r : r + n, :]
    ba, bh = z_back(a, h)
    na, nh = z_next(a, h)
    out = []
    for t, (c, b, f) in enumerate(((a, ba, na), (h, bh, nh))):
        if t and not rim:
            break
        s = (
            (ref[t, i - 1, r : r + n, :] + ref[t, i + 1, r : r + n, :])
            + (ref[t, i, r - 1 : r - 1 + n, :] + ref[t, i, r + 1 : r + 1 + n, :])
            + (b + f)
        )
        out.append((c, s))
    return out


def six1(ref, i, r, n):
    c = ref[i, r : r + n, :]
    s = (
        (ref[i - 1, r : r + n, :] + ref[i + 1, r : r + n, :])
        + (ref[i, r - 1 : r - 1 + n, :] + ref[i, r + 1 : r + 1 + n, :])
        + (pltpu.roll(c, 1, 1) + pltpu.roll(c, 127, 1))
    )
    return c, s


def pick(a, m):
    high = a.astype(jnp.bfloat16)
    low = (a - high.astype(jnp.float32)).astype(jnp.bfloat16)
    return jnp.dot(high, m, preferred_element_type=jnp.float32) + jnp.dot(
        low, m, preferred_element_type=jnp.float32
    )


def turn(value, shift):
    shift %= 128
    return pltpu.roll(value, shift, 1) if shift else value


def pack0(load, store):
    lane = lanes(BY)
    first = jnp.zeros((BY, 128), jnp.float32)
    last = jnp.zeros((BY, 128), jnp.float32)
    for i in range(BX):
        turned = turn(load(i), 8 * i)
        first = jnp.where((lane >= 8 * i) & (lane < 8 * i + 8), turned, first)
        at = (8 * i - 8) % 128
        last = jnp.where((lane >= at) & (lane < at + 8), turned, last)
    store(first, last)


def beside(x, count):
    return (0, x) if 0 <= x < count else ((-1, x + count) if x < 0 else (1, x - count))


def unpack0(land, x, rows):
    dx, i = beside(x, BX)
    left, right = turn(land[0, dx + 1], -8 * i), turn(land[1, dx + 1], -8 * i)
    lane = lanes(rows)
    return jnp.where(lane < 8, right, jnp.where(lane >= 120, left, 0.0))


def rim_copies(source, land, offsets):
    out = []
    for offset in offsets:
        dx, dy, dz = offset
        if dz == 0:
            continue
        y0, yd, ny = part(dy, BY, 8)
        side = 0 if dz > 0 else 1
        out.append((offset, source(side, y0, ny), land(side, 1 - dx, yd, ny)))
    return out


def block_copies(source, land, h, offsets):
    out = []
    for offset in offsets:
        dx, dy, dz = offset
        if dz != 0:
            continue
        x0, xd, nx = part(dx, BX, h)
        y0, yd, ny = part(dy, BY, 8)
        out.append((offset, source(x0, nx, y0, ny), land(xd, nx, yd, ny)))
    return out


def ordered(copies):
    return sorted(copies, key=lambda c: -sum(abs(d) for d in c[0]))


def clear_around(ref, lead_x, lead_y, count_y):
    nx, ny = ref.shape[0], ref.shape[1]
    ref[0:lead_x] = jnp.zeros((lead_x, ny, 128), jnp.float32)
    ref[lead_x + BX : nx] = jnp.zeros((nx - lead_x - BX, ny, 128), jnp.float32)
    ref[lead_x : lead_x + BX, 0:lead_y, :] = jnp.zeros((BX, lead_y, 128), jnp.float32)
    end = lead_y + count_y
    ref[lead_x : lead_x + BX, end:ny, :] = jnp.zeros((BX, ny - end, 128), jnp.float32)


def clear(*refs):
    for ref in refs:
        ref[...] = jnp.zeros(ref.shape, ref.dtype)


def kernel(
    sizes, p_ref, w_ref, out_ref,
    b0, v0, t0, zs0, zr0, wind, zsw, zrw, velocity, flux,
    vp, zsv, zrv,
    bv, zsb, zrb, s1, l1, zs1, zr1, b1, v1, t1,
    gathered, merged, c2, e2a, e2b,
    rows0, rows2, up1, up0, m_down0, m_down1, m_up1, m_up0,
    send_sems, recv_sems, load_sems,
):
    place = Place(sizes)
    load_p = pltpu.make_async_copy(
        p_ref, b0.at[0, pl.ds(8, BX), pl.ds(16, BY), :], load_sems.at[0])
    load_w = pltpu.make_async_copy(
        w_ref, wind.at[:, 0, pl.ds(3, BX), pl.ds(8, BY), :], load_sems.at[1])
    load_p.start()
    load_w.start()

    clear_around(b0.at[0], 8, 16, BY)
    for d in range(3):
        clear_around(wind.at[d, 0], 3, 8, BY)
    clear(zr0, zrw, vp, zrv, bv, zrb, l1, zr1, gathered)

    barrier = pltpu.get_barrier_semaphore()
    total = jnp.int32(0)
    for offset in GREETED:
        there = place.exists(offset)
        total = total + there.astype(jnp.int32)

        def greet(offset=offset):
            pl.semaphore_signal(
                barrier, inc=1, device_id=place.device(offset), device_id_type=MESH
            )

        pl.when(there)(greet)

    def storer(ref):
        def store(f, l):
            ref[0] = l
            ref[1] = f
        return store

    clear(b0.at[1], v0, t0, rows0)
    load_p.wait()
    pack0(lambda i: b0[0, 8 + i, 16:32, :], storer(zs0))

    used = [0]

    def exchange(copies):
        base = used[0]
        used[0] += len(copies)
        return Exchange(place, ordered(copies), send_sems, recv_sems, base)

    def b0_block(x, nx, y, ny):
        return b0.at[0, pl.ds(x + 8, nx), pl.ds(y + 16, ny), :]

    def wind_block(x, nx, y, ny):
        return wind.at[:, 0, pl.ds(x + 3, nx), pl.ds(y + 8, ny), :]

    def vp_block(x, nx, y, ny):
        return vp.at[pl.ds(x + 2, nx), pl.ds(y + 16, ny), :]

    ex0 = exchange(
        block_copies(b0_block, b0_block, 8, AROUND)
        + rim_copies(
            lambda s, y, ny: zs0.at[s, pl.ds(y, ny), :],
            lambda s, dx, y, ny: zr0.at[s, dx, pl.ds(y + 8, ny), :], AROUND))
    exw = exchange(
        block_copies(wind_block, wind_block, 3, AROUND)
        + rim_copies(
            lambda s, y, ny: zsw.at[s, :, pl.ds(y, ny), :],
            lambda s, dx, y, ny: zrw.at[s, dx, :, pl.ds(y + 8, ny), :], AROUND))
    exv = exchange(
        block_copies(vp_block, vp_block, 2, NEAR)
        + rim_copies(
            lambda s, y, ny: zsv.at[s, pl.ds(y, ny), :],
            lambda s, dx, y, ny: zrv.at[s, dx, pl.ds(y + 8, ny), :], NEAR))

    def bv_copies():
        out = []
        for offset in AROUND:
            dx, dy, dz = offset
            if dz == 0:
                out.append((
                    offset, bv.at[pl.ds(6, 6), pl.ds(16, 8), :],
                    bv.at[pl.ds(6 - 6 * dx, 6), pl.ds(16 - 8 * dy, 8), :]))
            else:
                side = 0 if dz > 0 else 1
                out.append((
                    offset, zsb.at[side], zrb.at[side, 1 - dx, pl.ds(8 - 8 * dy, 8), :]))
        return out

    def level1_copies():
        out = []
        for offset in AROUND:
            dx, dy, dz = offset
            if dz == 0:
                x0, xd, nx = part(dx, 6, 4)
                out.append((
                    offset, s1.at[pl.ds(x0, nx)],
                    l1.at[pl.ds(xd + 4, nx), pl.ds(8 - 8 * dy, 8), :]))
            else:
                side = 0 if dz > 0 else 1
                out.append((
                    offset, zs1.at[side], zr1.at[side, 1 - dx, pl.ds(8 - 8 * dy, 8), :]))
        return out

    def coarse_copies(number):
        return [
            (d, gathered.at[number, 2, 1, 2], gathered.at[number, 2 - d[1], 1 - d[2], 2 - d[0]])
            for d in COARSE[number]
        ]

    exb = exchange(bv_copies())
    ex1 = exchange(level1_copies())
    ex2 = [exchange(coarse_copies(0)), exchange(coarse_copies(1))]

    pl.semaphore_wait(barrier, total)
    ex0.start()

    load_w.wait()
    for d in range(3):
        pack0(lambda i: wind[d, 0, 3 + i, 8:24, :], storer(zsw.at[:, d]))
    exw.start()

    clear(velocity, flux, b1, v1, t1, merged, c2, e2a, e2b, rows2, up1, up0)

    bf16 = jnp.bfloat16
    k = lax.broadcasted_iota(jnp.int32, (128, 128), 0)
    l = lax.broadcasted_iota(jnp.int32, (128, 128), 1)
    eighth = jnp.float32(0.125)
    m_down0[0:128, :] = jnp.where(k // 2 == l, eighth, 0.0).astype(bf16)
    m_down0[128:256, :] = jnp.where(
        ((k < 8) | (k >= 120)) & (k // 2 + 64 == l), eighth, 0.0).astype(bf16)
    for i in range(3):
        m_down1[i * 128 : i * 128 + 128, :] = jnp.where(
            (l // 32 == i) & (k // 2 == l % 32), eighth, 0.0).astype(bf16)
    m_up1[...] = jnp.where(
        ((l < 72) & (k == l // 2)) | ((l >= 120) & (k == 64 + l // 2)), 1.0, 0.0).astype(bf16)
    m_up0[:, 0:128] = jnp.where(k == l // 2, 1.0, 0.0).astype(bf16)
    m_up0[:, 128:256] = jnp.where(
        ((l < 8) | (l >= 120)) & (k == 64 + l // 2), 1.0, 0.0).astype(bf16)

    c0 = OMEGA / 6.0
    w1 = 0.25
    c1 = OMEGA / (6.0 * w1)
    w2 = 0.0625
    c2s = OMEGA / (6.0 * w2)
    lane8, lane16, lane24, lane40 = lanes(8), lanes(16), lanes(24), lanes(40)
    m32a, m32h = masks0(place, -8, 32)
    m24a, m24h = masks0(place, -4, 24)
    mask32, mask24 = (m32a, m32h), (m24a, m24h)

    def level1_mask(first_row, rows):
        lane = lanes(rows)
        inside = row_mask(place, first_row, rows, 8)
        return (inside & ((lane < 64) | rim_lanes(place, rows, 64, 72))).astype(jnp.float32)

    def first_two0(reach, r, n, masks):
        for x in range(-reach, BX + reach):
            weight = slab_weight(place, x, BX)
            for t, (c, s) in enumerate(six0(b0, x + 8, r, n)):
                value = (1.0 + KEEP) * c0 * c + SIXTH * c0 * s
                v0[t, x + 8, r : r + n, :] = scaled(value, masks[t], weight)

    def down1_and_send(number, r, n):
        pairs = []
        for i in range(3):
            pair = None
            for x in (2 * i, 2 * i + 1):
                c, s = six1(v1, x + 6, 16, 8)
                res = b1[x + 6, 16:24, :] - w1 * (6.0 * c - s)
                pair = res if pair is None else pair + res
            pairs.append(jnp.where(lane8 < 64, pair, 0.0))
        rows2[...] = pick(jnp.concatenate(pairs, axis=1), m_down1[...])
        gathered[number, 2, 1, 2] = (
            rows2[pl.ds(0, 4, stride=2), :] + rows2[pl.ds(1, 4, stride=2), :])
        ex2[number].start()

    def coarse(number, reach):
        for az in range(3):
            for ax in range(5):
                for ay in range(5):
                    merged[az, ax, 4 * ay : 4 * ay + 4, :] = gathered[number, ay, az, ax]
        for x in range(-reach - 3, 3 + reach + 3):
            ax, i = (x + 6) // 3, (x + 6) % 3
            left = turn(merged[0, ax], 96 - 32 * i)
            own = turn(merged[1, ax], -32 * i)
            right = turn(merged[2, ax], 32 - 32 * i)
            c2[x + 6] = jnp.where(
                lane24 < 32, own, jnp.where(lane24 < 40, right, jnp.where(lane24 >= 120, left, 0.0)))
        inside = row_mask(place, -6, 16, 4)
        mask2 = (inside & ((lane16 < 32) | rim_lanes(place, 16, 32, 40))).astype(jnp.float32)
        for x in range(-reach - 2, 3 + reach + 2):
            c, s = six1(c2, x + 6, 2, 16)
            value = (1.0 + KEEP) * c2s * c + SIXTH * c2s * s
            e2a[x + 6, 2:18, :] = scaled(value, mask2, slab_weight(place, x, 3))
        here, there = e2a, e2b
        for more in (1, 0):
            for x in range(-reach - more, 3 + reach + more):
                c, s = six1(here, x + 6, 2, 16)
                value = KEEP * c + SIXTH * s + c2s * c2[x + 6, 2:18, :]
                there[x + 6, 2:18, :] = scaled(value, mask2, slab_weight(place, x, 3))
            here, there = there, here
        return here

    def spread1(here, reach, y, n):
        slabs = 3 + 2 * reach
        spread = pick(
            jnp.concatenate([here[x - reach + 6, y + 8 : y + 8 + n, :] for x in range(slabs)], axis=0),
            m_up1[...])
        for j in range(slabs):
            value = spread[n * j : n * j + n, :]
            up1[j, pl.ds(0, n, stride=2), :] = value
            up1[j, pl.ds(1, n, stride=2), :] = value

    def last_two1(reach, r, n, mask):
        for x in range(-reach - 1, 6 + reach + 1):
            c, s = six1(v1, x + 6, r, n)
            value = KEEP * c + SIXTH * s + c1 * b1[x + 6, r : r + n, :]
            t1[x + 6, r : r + n, :] = scaled(value, mask, slab_weight(place, x, 6))
        for x in range(-reach, 6 + reach):
            c, s = six1(t1, x + 6, r, n)
            value = KEEP * c + SIXTH * s + c1 * b1[x + 6, r : r + n, :]
            v1[x + 6, r : r + n, :] = scaled(value, mask, slab_weight(place, x, 6))

    def spread0(reach, n):
        y = -(n - 8) // 2
        slabs = 6 + 2 * reach
        spread = pick(
            jnp.concatenate(
                [v1[x - reach + 6, y + 16 : y + 32, :] for x in range(slabs)], axis=0),
            m_up0[...])
        for j in range(slabs):
            for t in range(2):
                value = spread[16 * j : 16 * j + n, 128 * t : 128 * t + 128]
                up0[t, j, pl.ds(0, n, stride=2), :] = value
                up0[t, j, pl.ds(1, n, stride=2), :] = value

    ex0.wait_recv()
    for x in range(-8, BX + 8):
        b0[1, x + 8, 8:40, :] = unpack0(zr0, x, 32)
    first_two0(7, 8, 32, mask32)
    for i in range(10):
        pair = [None, None]
        for x in (2 * i - 4, 2 * i - 3):
            for t, (c, s) in enumerate(six0(v0, x + 8, 12, 24)):
                res = b0[t, x + 8, 12:36, :] - (6.0 * c - s)
                pair[t] = res if pair[t] is None else pair[t] + res
        for t in range(2):
            rows0[t, i, 0:24, :] = pair[t]
    cells = [
        jnp.concatenate(
            [rows0[t, i, pl.ds(0, 16, stride=2), :] + rows0[t, i, pl.ds(1, 16, stride=2), :]
             for t in range(2)], axis=1)
        for i in range(10)
    ]
    source = pick(jnp.concatenate(cells, axis=0), m_down0[...])
    mask = level1_mask(-2, 16)
    for x in range(-2, 8):
        b1[x + 6, 14:30, :] = scaled(
            source[16 * (x + 2) : 16 * (x + 2) + 16, :], mask, slab_weight(place, x, 6))
    for x in range(-1, 7):
        c, s = six1(b1, x + 6, 14, 16)
        value = (1.0 + KEEP) * c1 * c + SIXTH * c1 * s
        v1[x + 6, 14:30, :] = scaled(value, mask, slab_weight(place, x, 6))
    down1_and_send(0, 14, 16)

    low = jnp.zeros((8, 128), jnp.float32)
    high = jnp.zeros((8, 128), jnp.float32)
    for i in range(6):
        block_b, block_v = b1[i + 6, 16:24, :], v1[i + 6, 16:24, :]
        bv[i + 6, 16:24, :] = jnp.where(lane8 < 64, block_b, pltpu.roll(block_v, 64, 1))
        for block, lead in ((block_b, 0), (block_v, 64)):
            group = (lane8 >= lead + 8 * i) & (lane8 < lead + 8 * i + 8)
            low = jnp.where(group, turn(block, lead + 8 * i), low)
            high = jnp.where(group, turn(block, lead + 8 * i - 56), high)
    zsb[0] = high
    zsb[1] = low
    exb.start()
    ex0.wait_send()
    exw.wait_recv()
    for d in range(3):
        for x in range(-3, BX + 3):
            wind[d, 1, x + 3] = unpack0(zrw.at[:, :, d], x, 32)
    exw.wait_send()
    ex2[0].wait_recv()
    here = coarse(0, 3)
    spread1(here, 3, -4, 16)
    exb.wait_recv()
    mask = level1_mask(-8, 24)
    for x in range(-6, 12):
        dx, i = beside(x, 6)
        near = bv[x + 6, 8:32, :]
        left, right = zrb[0, dx + 1], zrb[1, dx + 1]
        for lead, ref in ((0, b1), (64, v1)):
            value = jnp.where(
                lane24 < 64, turn(near, -lead),
                jnp.where(lane24 < 72, turn(right, 64 - 8 * i - lead),
                          jnp.where(lane24 >= 120, turn(left, 120 - 8 * i - lead), 0.0)))
            if ref is v1:
                value = value + scaled(
                    up1[(x + 6) // 2, 0:24, :], mask, slab_weight(place, x, 6))
            ref[x + 6, 8:32, :] = value
    last_two1(4, 8, 24, mask)
    spread0(4, 16)
    for x in range(-7, BX + 7):
        weight = slab_weight(place, x, BX)
        for t in range(2):
            v0[t, x + 8, 8:40, :] += scaled(up0[t, (x + 8) // 2], mask32[t], weight)
    for x in range(-6, BX + 6):
        weight = slab_weight(place, x, BX)
        for t, (c, s) in enumerate(six0(v0, x + 8, 8, 32)):
            value = KEEP * c + SIXTH * s + c0 * b0[t, x + 8, 8:40, :]
            t0[t, x + 8, 8:40, :] = scaled(value, mask32[t], weight)
    for x in range(-5, BX + 5):
        weight = slab_weight(place, x, BX)
        for t, (c, s) in enumerate(six0(t0, x + 8, 8, 32)):
            value = KEEP * c + SIXTH * s + c0 * b0[t, x + 8, 8:40, :]
            v0[t, x + 8, 8:40, :] = scaled(value, mask32[t], weight)
    first = v0

    for x in range(-4, BX + 4):
        weight = slab_weight(place, x, BX)
        half = 0.5 if weight is None else 0.5 * weight
        i = x + 8
        a, h = first[0, i, 12:36, :], first[1, i, 12:36, :]
        ba, bh = z_back(a, h)
        na, nh = z_next(a, h)
        for t, (b, n) in enumerate(((ba, na), (bh, nh))):
            m = mask24[t] * half
            velocity[0, t, x + 4, 12:36, :] = (first[t, i + 1, 12:36, :] - first[t, i - 1, 12:36, :]) * m
            velocity[1, t, x + 4, 12:36, :] = (first[t, i, 13:37, :] - first[t, i, 11:35, :]) * m
            velocity[2, t, x + 4, 12:36, :] = (n - b) * m
    for x in range(-3, BX + 3):
        weight = slab_weight(place, x, BX)
        i = x + 4
        half_wind = [[0.5 * wind[e, t, x + 3, 4:28, :] for t in range(2)] for e in range(3)]
        for d in range(3):
            u = velocity.at[d]
            a, h = u[0, i, 12:36, :], u[1, i, 12:36, :]
            ba, bh = z_back(a, h)
            na, nh = z_next(a, h)
            for t, (c, b, n) in enumerate(((a, ba, na), (h, bh, nh))):
                x_low, x_high = u[t, i - 1, 12:36, :], u[t, i + 1, 12:36, :]
                y_low, y_high = u[t, i, 11:35, :], u[t, i, 13:37, :]
                value = (
                    7.0 * c
                    - ((x_low + x_high) + (y_low + y_high) + (b + n))
                    + half_wind[0][t] * (x_high - x_low)
                    + half_wind[1][t] * (y_high - y_low)
                    + half_wind[2][t] * (n - b)
                )
                flux[d, t, x + 3, 4:28, :] = scaled(value, mask24[t], weight)
    for x in range(-2, BX + 2):
        weight = slab_weight(place, x, BX)
        i = x + 3
        a, h = flux[2, 0, i, 4:28, :], flux[2, 1, i, 4:28, :]
        ba, bh = z_back(a, h)
        na, nh = z_next(a, h)
        for t, (b, n) in enumerate(((ba, na), (bh, nh))):
            value = (
                (flux[0, t, i + 1, 4:28, :] - flux[0, t, i - 1, 4:28, :])
                + (flux[1, t, i, 5:29, :] - flux[1, t, i, 3:27, :])
                + (n - b)
            ) * -0.5
            b0[t, x + 8, 12:36, :] = scaled(value, mask24[t], weight)

    first_two0(1, 12, 24, mask24)
    for i in range(6):
        pair = None
        for x in (2 * i, 2 * i + 1):
            ((c, s),) = six0(v0, x + 8, 16, 16, rim=False)
            res = b0[0, x + 8, 16:32, :] - (6.0 * c - s)
            pair = res if pair is None else pair + res
        rows0[0, i, 0:16, :] = pair
    cells = [rows0[0, i, pl.ds(0, 8, stride=2), :] + rows0[0, i, pl.ds(1, 8, stride=2), :] for i in range(6)]
    source = pick(jnp.concatenate(cells, axis=0), m_down0[0:128, :])
    low = jnp.zeros((8, 128), jnp.float32)
    high = jnp.zeros((8, 128), jnp.float32)
    for i in range(6):
        block = source[8 * i : 8 * i + 8, :]
        s1[i] = block
        l1[4 + i, 8:16, :] = block
        group = (lane8 >= 8 * i) & (lane8 < 8 * i + 8)
        low = jnp.where(group, turn(block, 8 * i), low)
        high = jnp.where(group, turn(block, 8 * i - 56), high)
    zs1[0] = high
    zs1[1] = low
    ex1.start()
    for x in range(BX):
        vp[x + 2, 16:32, :] = v0[0, x + 8, 16:32, :]
    pack0(lambda i: v0[0, 8 + i, 16:32, :], storer(zsv))
    exv.start()
    ex2[0].wait_send()
    exb.wait_send()
    ex1.wait_recv()
    for x in range(-4, 10):
        dx, i = beside(x, 6)
        b1[x + 6, 8:32, :] = jnp.where(
            lane24 < 64, l1[x + 4],
            jnp.where(lane24 < 72, turn(zr1[1, dx + 1], 64 - 8 * i),
                      jnp.where(lane24 >= 120, turn(zr1[0, dx + 1], 120 - 8 * i), 0.0)))
    mask = level1_mask(-4, 16)
    for x in range(-3, 9):
        c, s = six1(b1, x + 6, 12, 16)
        value = (1.0 + KEEP) * c1 * c + SIXTH * c1 * s
        v1[x + 6, 12:28, :] = scaled(value, mask, slab_weight(place, x, 6))
    down1_and_send(1, 12, 16)
    ex1.wait_send()
    exv.wait_send()
    exv.wait_recv()
    for x in range(-2, BX + 2):
        v0[0, x + 8, 12:36, :] = vp[x + 2, 12:36, :]
        v0[1, x + 8, 8:40, :] = unpack0(zrv, x, 32)
    ex2[1].wait_recv()
    here = coarse(1, 2)
    spread1(here, 2, -2, 8)
    for x in range(-3, 9):
        v1[x + 6, 12:28, :] += scaled(up1[(x + 4) // 2, 0:16, :], mask, slab_weight(place, x, 6))
    last_two1(1, 12, 16, mask)
    spread0(1, 12)
    for x in range(-2, BX + 2):
        weight = slab_weight(place, x, BX)
        for t in range(2):
            v0[t, x + 8, 12:36, :] += scaled(up0[t, (x + 2) // 2, 0:24, :], mask24[t], weight)
    for x in range(-1, BX + 1):
        weight = slab_weight(place, x, BX)
        for t, (c, s) in enumerate(six0(v0, x + 8, 12, 24)):
            value = KEEP * c + SIXTH * s + c0 * b0[t, x + 8, 12:36, :]
            t0[t, x + 8, 12:36, :] = scaled(value, mask24[t], weight)
    for x in range(BX):
        ((c, s),) = six0(t0, x + 8, 16, 16, rim=False)
        out_ref[x] = KEEP * c + SIXTH * s + c0 * b0[0, x + 8, 16:32, :]
    ex2[1].wait_send()


def solution(mesh):
    sizes = tuple(mesh.shape[a] for a in AXES)
    copies = 26 * 4 + len(NEAR) + len(COARSE[0]) + len(COARSE[1])
    f32 = jnp.float32
    bf16 = jnp.bfloat16

    def vmem(*shape, dtype=f32):
        return pltpu.VMEM(shape, dtype)

    def body(pressure, wind):
        return pl.pallas_call(
            functools.partial(kernel, sizes),
            out_shape=jax.ShapeDtypeStruct((BX, BY, BZ), f32),
            in_specs=[pl.BlockSpec(memory_space=pl.ANY)] * 2,
            out_specs=pl.BlockSpec(memory_space=pltpu.VMEM),
            scratch_shapes=[
                vmem(2, 28, 48, 128),
                vmem(2, 28, 48, 128),
                vmem(2, 28, 48, 128),
                vmem(2, 16, 128),
                vmem(2, 3, 32, 128),
                vmem(3, 2, 18, 32, 128),
                vmem(2, 3, 16, 128),
                vmem(2, 3, 3, 32, 128),
                vmem(3, 2, 20, 48, 128),
                vmem(3, 2, 18, 32, 128),
                vmem(16, 48, 128),
                vmem(2, 16, 128),
                vmem(2, 3, 32, 128),
                vmem(18, 40, 128),
                vmem(2, 8, 128),
                vmem(2, 3, 24, 128),
                vmem(6, 8, 128),
                vmem(14, 24, 128),
                vmem(2, 8, 128),
                vmem(2, 3, 24, 128),
                vmem(18, 40, 128),
                vmem(18, 40, 128),
                vmem(18, 40, 128),
                vmem(2, 5, 3, 5, 4, 128),
                vmem(3, 5, 24, 128),
                vmem(15, 24, 128),
                vmem(15, 24, 128),
                vmem(15, 24, 128),
                vmem(2, 10, 32, 128),
                vmem(8, 128),
                vmem(9, 32, 128),
                vmem(2, 14, 32, 128),
                vmem(256, 128, dtype=bf16),
                vmem(384, 128, dtype=bf16),
                vmem(128, 128, dtype=bf16),
                vmem(128, 256, dtype=bf16),
                pltpu.SemaphoreType.DMA((copies,)),
                pltpu.SemaphoreType.DMA((copies,)),
                pltpu.SemaphoreType.DMA((2,)),
            ],
            compiler_params=pltpu.CompilerParams(
                collective_id=0, has_side_effects=True, vmem_limit_bytes=67043328
            ),
            name="schur",
        )(pressure, wind)

    in_specs = (P("gx", "gy", "gz"), P(None, "gx", "gy", "gz"))
    return jax.shard_map(
        body, mesh=mesh, in_specs=in_specs, out_specs=P("gx", "gy", "gz"), check_vma=False
    )
```

```python
import functools

import jax
import jax.numpy as jnp
from jax import lax
from jax.experimental import pallas as pl
from jax.experimental.pallas import tpu as pltpu
from jax.sharding import PartitionSpec as P

MESH = pl.DeviceIdType.MESH
AXES = ("gx", "gy", "gz")
BX, BY, BZ = 12, 16, 128
OMEGA = 0.8
KEEP = 1.0 - OMEGA
SIXTH = OMEGA / 6.0

AROUND = [
    (dx, dy, dz)
    for dz in (0, 1, -1)
    for dx in (0, 1, -1)
    for dy in (0, 1, -1)
    if (dx, dy, dz) != (0, 0, 0)
]
AROUND.sort(key=lambda d: -(abs(d[0]) + abs(d[1]) + abs(d[2])))

NEAR = [d for d in AROUND if sum(map(abs, d)) <= 2]


def coarse_offsets(far_edges):
    out = []
    for dx in range(-2, 3):
        for dy in range(-2, 3):
            for dz in (-1, 0, 1):
                shape = (abs(dx), abs(dy), abs(dz))
                if shape[:2] in ((0, 0), (0, 1), (1, 0), (1, 1), (0, 2), (2, 0), (2, 1)):
                    keep = shape != (0, 0, 0)
                else:
                    keep = far_edges and shape[:2] == (1, 2)
                if keep:
                    out.append((dx, dy, dz))
    return sorted(out, key=lambda d: -sum(map(abs, d)))


COARSE = (coarse_offsets(True), coarse_offsets(False))
GREETED = coarse_offsets(True)


def part(delta, count, width):
    if delta == 0:
        return 0, 0, count
    if delta > 0:
        return count - width, -width, width
    return 0, count, width


class Place:
    def __init__(self, sizes):
        self.sizes = sizes
        self.at = [lax.axis_index(a) for a in AXES]
        self.has = []
        for g, n in zip(self.at, sizes):
            self.has.append({d: (g + d >= 0) & (g + d < n) for d in (-2, -1, 1, 2)})

        kinds = []
        for n in sizes:
            kinds.append(sorted({
                tuple(sum(0 <= g + d < n for d in (-k, k)) for k in (1, 2)) for g in range(n)
            }))
        self.profiles = [(a, b, c) for a in kinds[0] for b in kinds[1] for c in kinds[2]]
        self.kinds = kinds
        self.counts = [
            [t[-k].astype(jnp.int32) + t[k].astype(jnp.int32) for k in (1, 2)] for t in self.has
        ]

    def matches(self, profile):
        found = None
        for counts, wanted, kinds in zip(self.counts, profile, self.kinds):
            for c, v, seen in zip(counts, wanted, zip(*kinds)):
                if len(set(seen)) > 1:
                    found = (c == v) if found is None else found & (c == v)
        return True if found is None else found

    def exists(self, offset):
        found = None
        for table, d in zip(self.has, offset):
            if d:
                found = table[d] if found is None else found & table[d]
        return found

    def device(self, offset):
        return tuple(
            lax.rem(g + (d + n), n) if d else g for g, d, n in zip(self.at, offset, self.sizes)
        )


class Exchange:
    def __init__(self, place, copies, send_sem, recv_sem, ruler):
        self.place, self.items = place, []
        self.send_sem, self.recv_sem, self.ruler = send_sem, recv_sem, ruler
        self.weights = []
        for offset, src, dst in copies:
            copy = pltpu.make_async_remote_copy(
                src_ref=src,
                dst_ref=dst,
                send_sem=send_sem,
                recv_sem=recv_sem,
                device_id=place.device(offset),
                device_id_type=MESH,
            )
            self.items.append((offset, copy))
            units = 1
            for n in src.shape:
                units *= n
            self.weights.append((tuple(abs(d) for d in offset), units // 512))

    def start(self):
        for offset, copy in self.items:
            pl.when(self.place.exists(offset))(copy.start)

    def wait(self, sem):
        for profile in self.place.profiles:
            total = 0
            for shape, units in self.weights:
                share = 8 * units
                for counts, d in zip(profile, shape):
                    share = share * counts[d - 1] // 2 if d else share
                total += share
            total //= 8
            if total:
                rows = self.ruler.at[pl.ds(0, total)]
                pl.when(self.place.matches(profile))(pltpu.make_async_copy(rows, rows, sem).wait)

    def wait_recv(self):
        self.wait(self.recv_sem)

    def wait_send(self):
        self.wait(self.send_sem)


def lanes(rows):
    return lax.broadcasted_iota(jnp.int32, (rows, 128), 1)


def row_mask(place, first_row, rows, extent):
    y = first_row + lax.broadcasted_iota(jnp.int32, (rows, 128), 0)
    low = jnp.where(place.has[1][-1], -64, 0)
    high = jnp.where(place.has[1][1], 64, extent)
    return (y >= low) & (y < high)


def rim_lanes(place, rows, start, right_end):
    lane = lanes(rows)
    right_stop = jnp.where(place.has[2][1], right_end, 0)
    left_start = jnp.where(place.has[2][-1], 120, 128)
    return ((lane >= start) & (lane < right_stop)) | (lane >= left_start)


def slab_weight(place, x, extent):
    if x < 0:
        return place.has[0][-1].astype(jnp.float32)
    if x >= extent:
        return place.has[0][1].astype(jnp.float32)
    return None


def z_back(a, h):
    lane0 = lanes(a.shape[0]) == 0
    ra, rh = pltpu.roll(a, 1, 1), pltpu.roll(h, 1, 1)
    return jnp.where(lane0, rh, ra), jnp.where(lane0, ra, rh)


def z_next(a, h):
    lane127 = lanes(a.shape[0]) == 127
    ra, rh = pltpu.roll(a, 127, 1), pltpu.roll(h, 127, 1)
    return jnp.where(lane127, rh, ra), jnp.where(lane127, ra, rh)


def masks0(place, first_row, rows):
    inner = row_mask(place, first_row, rows, BY)
    rim = inner & rim_lanes(place, rows, 0, 8)
    return inner.astype(jnp.float32), rim.astype(jnp.float32)


def scaled(value, mask, weight):
    value = value * mask
    return value if weight is None else value * weight


def six0(ref, i, r, n, rim=True):
    a, h = ref[0, i, r : r + n, :], ref[1, i, r : r + n, :]
    ba, bh = z_back(a, h)
    na, nh = z_next(a, h)
    out = []
    for t, (c, b, f) in enumerate(((a, ba, na), (h, bh, nh))):
        if t and not rim:
            break
        s = (
            (ref[t, i - 1, r : r + n, :] + ref[t, i + 1, r : r + n, :])
            + (ref[t, i, r - 1 : r - 1 + n, :] + ref[t, i, r + 1 : r + 1 + n, :])
            + (b + f)
        )
        out.append((c, s))
    return out


def six1(ref, i, r, n):
    c = ref[i, r : r + n, :]
    s = (
        (ref[i - 1, r : r + n, :] + ref[i + 1, r : r + n, :])
        + (ref[i, r - 1 : r - 1 + n, :] + ref[i, r + 1 : r + 1 + n, :])
        + (pltpu.roll(c, 1, 1) + pltpu.roll(c, 127, 1))
    )
    return c, s


def pick(a, m):
    high = a.astype(jnp.bfloat16)
    low = (a - high.astype(jnp.float32)).astype(jnp.bfloat16)
    return jnp.dot(high, m, preferred_element_type=jnp.float32) + jnp.dot(
        low, m, preferred_element_type=jnp.float32
    )


def turn(value, shift):
    shift %= 128
    return pltpu.roll(value, shift, 1) if shift else value


def pack0(load, store, count=BX):
    lane = lanes(BY)
    first = jnp.zeros((BY, 128), jnp.float32)
    last = jnp.zeros((BY, 128), jnp.float32)
    for i in range(count):
        turned = turn(load(i), 8 * i)
        first = jnp.where((lane >= 8 * i) & (lane < 8 * i + 8), turned, first)
        at = (8 * i - 8) % 128
        last = jnp.where((lane >= at) & (lane < at + 8), turned, last)
    store(first, last)


def beside(x, count):
    return (0, x) if 0 <= x < count else ((-1, x + count) if x < 0 else (1, x - count))


def unpack0(land, x, rows):
    dx, i = beside(x, BX)
    return unpack_columns(land[0, dx + 1], land[1, dx + 1], i, rows)


def unpack_columns(left, right, i, rows):
    left, right = turn(left, -8 * i), turn(right, -8 * i)
    lane = lanes(rows)
    return jnp.where(lane < 8, right, jnp.where(lane >= 120, left, 0.0))


def rim_copies(source, land, offsets):
    out = []
    for offset in offsets:
        dx, dy, dz = offset
        if dz == 0:
            continue
        y0, yd, ny = part(dy, BY, 8)
        side = 0 if dz > 0 else 1
        out.append((offset, source(side, y0, ny), land(side, 1 - dx, yd, ny)))
    return out


def block_copies(source, land, reach, offsets, edge=None):
    out = []
    for offset in offsets:
        dx, dy, dz = offset
        if dz != 0:
            continue
        near, far = edge if edge and dy else reach
        if dx == 0:
            x0, xd, nx = 0, 0, BX
        elif dx > 0:
            x0, xd, nx = BX - far, -far, far - near + 1
        else:
            x0, xd, nx = near - 1, BX + near - 1, far - near + 1
        y0, yd, ny = part(dy, BY, 8)
        out.append((offset, source(x0, nx, y0, ny), land(xd, nx, yd, ny)))
    return out


def ordered(copies):
    return sorted(copies, key=lambda c: -sum(abs(d) for d in c[0]))


def clear_around(ref, lead_x, lead_y, count_y):
    nx, ny = ref.shape[0], ref.shape[1]
    ref[0:lead_x] = jnp.zeros((lead_x, ny, 128), jnp.float32)
    ref[lead_x + BX : nx] = jnp.zeros((nx - lead_x - BX, ny, 128), jnp.float32)
    ref[lead_x : lead_x + BX, 0:lead_y, :] = jnp.zeros((BX, lead_y, 128), jnp.float32)
    end = lead_y + count_y
    ref[lead_x : lead_x + BX, end:ny, :] = jnp.zeros((BX, ny - end, 128), jnp.float32)


def clear(*refs):
    for ref in refs:
        ref[...] = jnp.zeros(ref.shape, ref.dtype)


def kernel(
    sizes, p_ref, w_ref, out_ref,
    b0, far, sb, v0, t0, zs0, zr0, wind, zsw, zrw, zsx, zrx, coef, velocity, flux,
    vp, zsv, zrv,
    bv, zsb, zrb, s1, l1, zs1, zr1, b1, v1, t1,
    gathered, merged, c2, e2a, e2b,
    rows0, rows2, up1, up0, m_down0, m_down1, m_up1, m_up0,
    ruler, send_sems, recv_sems, load_sems,
):
    place = Place(sizes)
    load_p = pltpu.make_async_copy(
        p_ref, b0.at[0, pl.ds(8, BX), pl.ds(16, BY), :], load_sems.at[0])
    load_w = pltpu.make_async_copy(
        w_ref, wind.at[:, 0, pl.ds(3, BX), pl.ds(8, BY), :], load_sems.at[1])
    load_p.start()
    load_w.start()

    clear_around(b0.at[0], 8, 16, BY)
    for d in range(3):
        clear_around(wind.at[d, 0], 3, 8, BY)
    clear(far, zr0, zrw, zrx, vp, zrv, bv, zrb, l1, zr1, gathered)

    barrier = pltpu.get_barrier_semaphore()
    total = jnp.int32(0)
    for offset in GREETED:
        there = place.exists(offset)
        total = total + there.astype(jnp.int32)

        def greet(offset=offset):
            pl.semaphore_signal(
                barrier, inc=1, device_id=place.device(offset), device_id_type=MESH
            )

        pl.when(there)(greet)

    def storer(ref):
        def store(f, l):
            ref[0] = l
            ref[1] = f
        return store

    clear(b0.at[1], v0, t0, rows0)
    load_p.wait()
    pack0(lambda i: b0[0, 8 + i, 16:32, :], storer(zs0))

    used = [0]

    def exchange(copies):
        k = used[0]
        used[0] += 1
        return Exchange(place, ordered(copies), send_sems.at[k], recv_sems.at[k], ruler)

    def far_block(x, nx, y, ny):
        side, lead = (0, 8) if x < 0 else (1, -BX - 5)
        return far.at[side, pl.ds(x + lead, nx), pl.ds(y + 16, ny), :]

    def b0_block(x, nx, y, ny):
        return b0.at[0, pl.ds(x + 8, nx), pl.ds(y + 16, ny), :]

    def wind_block(x, nx, y, ny):
        return wind.at[:, 0, pl.ds(x + 3, nx), pl.ds(y + 8, ny), :]

    def vp_block(x, nx, y, ny):
        return vp.at[pl.ds(x + 2, nx), pl.ds(y + 16, ny), :]

    def wind_side_copies():
        out = []
        for offset in AROUND:
            dx, dy, dz = offset
            if dx and dz:
                y0, yd, ny = part(dy, BY, 8)
                side = 0 if dz > 0 else 1
                out.append((
                    offset, zsx.at[side, (dx + 1) // 2, pl.ds(y0, ny), :],
                    zrx.at[side, (1 - dx) // 2, pl.ds(yd + 8, ny), :]))
        return out

    ex0 = exchange(
        block_copies(b0_block, b0_block, (1, 6), AROUND, (1, 5))
        + rim_copies(
            lambda s, y, ny: zs0.at[s, pl.ds(y, ny), :],
            lambda s, dx, y, ny: zr0.at[s, dx, pl.ds(y + 8, ny), :], AROUND))
    sides = [d for d in AROUND if d[0]]
    ex_far = exchange(
        block_copies(b0_block, far_block, (7, 8), [d for d in sides if d[2] == 0], (6, 7)))
    exw = exchange(
        block_copies(wind_block, wind_block, (1, 3), AROUND, (1, 2))
        + rim_copies(
            lambda s, y, ny: zsw.at[s, :, pl.ds(y, ny), :],
            lambda s, dx, y, ny: zrw.at[s, :, pl.ds(y + 8, ny), :],
            [d for d in AROUND if not d[0]])
        + wind_side_copies())
    exv = exchange(
        block_copies(vp_block, vp_block, (1, 2), NEAR, (1, 1))
        + rim_copies(
            lambda s, y, ny: zsv.at[s, pl.ds(y, ny), :],
            lambda s, dx, y, ny: zrv.at[s, dx, pl.ds(y + 8, ny), :], NEAR))

    def bv_copies():
        out = []
        for offset in AROUND:
            dx, dy, dz = offset
            if dz == 0:
                out.append((
                    offset, bv.at[pl.ds(6, 6), pl.ds(16, 8), :],
                    bv.at[pl.ds(6 - 6 * dx, 6), pl.ds(16 - 8 * dy, 8), :]))
            else:
                side = 0 if dz > 0 else 1
                out.append((
                    offset, zsb.at[side], zrb.at[side, 1 - dx, pl.ds(8 - 8 * dy, 8), :]))
        return out

    def level1_copies():
        out = []
        for offset in AROUND:
            dx, dy, dz = offset
            if dz == 0:
                x0, xd, nx = part(dx, 6, 4)
                out.append((
                    offset, s1.at[pl.ds(x0, nx)],
                    l1.at[pl.ds(xd + 4, nx), pl.ds(8 - 8 * dy, 8), :]))
            else:
                side = 0 if dz > 0 else 1
                out.append((
                    offset, zs1.at[side], zr1.at[side, 1 - dx, pl.ds(8 - 8 * dy, 8), :]))
        return out

    def coarse_copies(number):
        return [
            (d, gathered.at[number, 2, 1, 2], gathered.at[number, 2 - d[1], 1 - d[2], 2 - d[0]])
            for d in COARSE[number]
        ]

    exb = exchange(bv_copies())
    ex1 = exchange(level1_copies())
    ex2 = [exchange(coarse_copies(0)), exchange(coarse_copies(1))]

    pl.semaphore_wait(barrier, total)
    ex0.start()
    ex_far.start()

    load_w.wait()
    for d in range(3):
        pack0(lambda i: wind[d, 0, 3 + i, 8:24, :], storer(zsw.at[:, d]))
    for high, lead in ((0, 3), (1, BX)):
        pack0(lambda i: wind[i // 3, 0, lead + i % 3, 8:24, :], storer(zsx.at[:, high]), 9)
    exw.start()

    clear(velocity, flux, sb, b1, v1, t1, merged, c2, e2a, e2b, rows2, up1, up0)

    bf16 = jnp.bfloat16
    k = lax.broadcasted_iota(jnp.int32, (128, 128), 0)
    l = lax.broadcasted_iota(jnp.int32, (128, 128), 1)
    eighth = jnp.float32(0.125)
    m_down0[0:128, :] = jnp.where(k // 2 == l, eighth, 0.0).astype(bf16)
    m_down0[128:256, :] = jnp.where(
        ((k < 8) | (k >= 120)) & (k // 2 + 64 == l), eighth, 0.0).astype(bf16)
    for i in range(3):
        m_down1[i * 128 : i * 128 + 128, :] = jnp.where(
            (l // 32 == i) & (k // 2 == l % 32), eighth, 0.0).astype(bf16)
    m_up1[...] = jnp.where(
        ((l < 72) & (k == l // 2)) | ((l >= 120) & (k == 64 + l // 2)), 1.0, 0.0).astype(bf16)
    m_up0[:, 0:128] = jnp.where(k == l // 2, 1.0, 0.0).astype(bf16)
    m_up0[:, 128:256] = jnp.where(
        ((l < 8) | (l >= 120)) & (k == 64 + l // 2), 1.0, 0.0).astype(bf16)

    c0 = OMEGA / 6.0
    w1 = 0.25
    c1 = OMEGA / (6.0 * w1)
    w2 = 0.0625
    c2s = OMEGA / (6.0 * w2)
    lane8, lane16, lane24, lane40 = lanes(8), lanes(16), lanes(24), lanes(40)
    m32a, m32h = masks0(place, -8, 32)
    m24a, m24h = masks0(place, -4, 24)
    mask32, mask24 = (m32a, m32h), (m24a, m24h)

    def level1_mask(first_row, rows):
        lane = lanes(rows)
        inside = row_mask(place, first_row, rows, 8)
        return (inside & ((lane < 64) | rim_lanes(place, rows, 64, 72))).astype(jnp.float32)

    def scaled_masks(masks, factor, weight):
        factor = factor if weight is None else factor * weight
        return [m * factor for m in masks]

    def sweep0(target, iterate, x, r, n, masks):
        weight = slab_weight(place, x, BX)
        keep, share = scaled_masks(masks, KEEP, weight), scaled_masks(masks, SIXTH, weight)
        for t, (c, s) in enumerate(six0(iterate, x + 8, r, n)):
            target[t, x + 8, r : r + n, :] = keep[t] * c + share[t] * s + sb[t, x + 8, r : r + n, :]

    def scale_source(x, r, n, masks):
        factor = scaled_masks(masks, c0, slab_weight(place, x, BX))
        for t in range(2):
            sb[t, x + 8, r : r + n, :] = factor[t] * b0[t, x + 8, r : r + n, :]

    def first_two0(slabs, r, n, masks):
        for x in slabs:
            weight = slab_weight(place, x, BX)
            for t, (c, s) in enumerate(six0(b0, x + 8, r, n)):
                value = (1.0 + KEEP) * c0 * c + SIXTH * c0 * s
                v0[t, x + 8, r : r + n, :] = scaled(value, masks[t], weight)

    def down1_and_send(number, r, n):
        pairs = []
        for i in range(3):
            pair = None
            for x in (2 * i, 2 * i + 1):
                c, s = six1(v1, x + 6, 16, 8)
                res = b1[x + 6, 16:24, :] - w1 * (6.0 * c - s)
                pair = res if pair is None else pair + res
            pairs.append(jnp.where(lane8 < 64, pair, 0.0))
        rows2[...] = pick(jnp.concatenate(pairs, axis=1), m_down1[...])
        gathered[number, 2, 1, 2] = (
            rows2[pl.ds(0, 4, stride=2), :] + rows2[pl.ds(1, 4, stride=2), :])
        ex2[number].start()

    def coarse(number, reach):
        for az in range(3):
            for ax in range(5):
                for ay in range(5):
                    merged[az, ax, 4 * ay : 4 * ay + 4, :] = gathered[number, ay, az, ax]
        for x in range(-reach - 3, 3 + reach + 3):
            ax, i = (x + 6) // 3, (x + 6) % 3
            left = turn(merged[0, ax], 96 - 32 * i)
            own = turn(merged[1, ax], -32 * i)
            right = turn(merged[2, ax], 32 - 32 * i)
            c2[x + 6] = jnp.where(
                lane24 < 32, own, jnp.where(lane24 < 40, right, jnp.where(lane24 >= 120, left, 0.0)))
        inside = row_mask(place, -6, 16, 4)
        mask2 = (inside & ((lane16 < 32) | rim_lanes(place, 16, 32, 40))).astype(jnp.float32)
        for x in range(-reach - 2, 3 + reach + 2):
            c, s = six1(c2, x + 6, 2, 16)
            value = (1.0 + KEEP) * c2s * c + SIXTH * c2s * s
            e2a[x + 6, 2:18, :] = scaled(value, mask2, slab_weight(place, x, 3))
        here, there = e2a, e2b
        for more in (1, 0):
            for x in range(-reach - more, 3 + reach + more):
                c, s = six1(here, x + 6, 2, 16)
                value = KEEP * c + SIXTH * s + c2s * c2[x + 6, 2:18, :]
                there[x + 6, 2:18, :] = scaled(value, mask2, slab_weight(place, x, 3))
            here, there = there, here
        return here

    def spread1(here, reach, y, n):
        slabs = 3 + 2 * reach
        spread = pick(
            jnp.concatenate([here[x - reach + 6, y + 8 : y + 8 + n, :] for x in range(slabs)], axis=0),
            m_up1[...])
        for j in range(slabs):
            value = spread[n * j : n * j + n, :]
            up1[j, pl.ds(0, n, stride=2), :] = value
            up1[j, pl.ds(1, n, stride=2), :] = value

    def last_two1(reach, r, n, mask):
        for x in range(-reach - 1, 6 + reach + 1):
            c, s = six1(v1, x + 6, r, n)
            value = KEEP * c + SIXTH * s + c1 * b1[x + 6, r : r + n, :]
            t1[x + 6, r : r + n, :] = scaled(value, mask, slab_weight(place, x, 6))
        for x in range(-reach, 6 + reach):
            c, s = six1(t1, x + 6, r, n)
            value = KEEP * c + SIXTH * s + c1 * b1[x + 6, r : r + n, :]
            v1[x + 6, r : r + n, :] = scaled(value, mask, slab_weight(place, x, 6))

    def spread0(reach, n):
        y = -(n - 8) // 2
        slabs = 6 + 2 * reach
        spread = pick(
            jnp.concatenate(
                [v1[x - reach + 6, y + 16 : y + 32, :] for x in range(slabs)], axis=0),
            m_up0[...])
        for j in range(slabs):
            for t in range(2):
                value = spread[16 * j : 16 * j + n, 128 * t : 128 * t + 128]
                up0[t, j, pl.ds(0, n, stride=2), :] = value
                up0[t, j, pl.ds(1, n, stride=2), :] = value

    ex0.wait_recv()
    for x in range(-8, BX + 8):
        b0[1, x + 8, 8:40, :] = unpack0(zr0, x, 32)
    first_two0(range(-5, BX + 5), 8, 32, mask32)
    for i in range(10):
        pair = [None, None]
        for x in (2 * i - 4, 2 * i - 3):
            for t, (c, s) in enumerate(six0(v0, x + 8, 12, 24)):
                res = b0[t, x + 8, 12:36, :] - (6.0 * c - s)
                pair[t] = res if pair[t] is None else pair[t] + res
        for t in range(2):
            rows0[t, i, 0:24, :] = pair[t]
    cells = [
        jnp.concatenate(
            [rows0[t, i, pl.ds(0, 16, stride=2), :] + rows0[t, i, pl.ds(1, 16, stride=2), :]
             for t in range(2)], axis=1)
        for i in range(10)
    ]
    source = pick(jnp.concatenate(cells, axis=0), m_down0[...])
    mask = level1_mask(-2, 16)
    for x in range(-2, 8):
        b1[x + 6, 14:30, :] = scaled(
            source[16 * (x + 2) : 16 * (x + 2) + 16, :], mask, slab_weight(place, x, 6))
    for x in range(-1, 7):
        c, s = six1(b1, x + 6, 14, 16)
        value = (1.0 + KEEP) * c1 * c + SIXTH * c1 * s
        v1[x + 6, 14:30, :] = scaled(value, mask, slab_weight(place, x, 6))
    down1_and_send(0, 14, 16)

    low = jnp.zeros((8, 128), jnp.float32)
    high = jnp.zeros((8, 128), jnp.float32)
    for i in range(6):
        block_b, block_v = b1[i + 6, 16:24, :], v1[i + 6, 16:24, :]
        bv[i + 6, 16:24, :] = jnp.where(lane8 < 64, block_b, pltpu.roll(block_v, 64, 1))
        for block, lead in ((block_b, 0), (block_v, 64)):
            group = (lane8 >= lead + 8 * i) & (lane8 < lead + 8 * i + 8)
            low = jnp.where(group, turn(block, lead + 8 * i), low)
            high = jnp.where(group, turn(block, lead + 8 * i - 56), high)
    zsb[0] = high
    zsb[1] = low
    exb.start()
    ex0.wait_send()
    ex_far.wait_recv()
    for side in range(2):
        for k in range(3):
            x = k - 8 if side == 0 else BX + 5 + k
            distance = -x if side == 0 else x - BX + 1
            if distance > 6:
                b0[0, x + 8, 16:32, :] = far[side, k, 16:32, :]
            if distance < 8:
                for r in (8, 32):
                    b0[0, x + 8, r : r + 8, :] = far[side, k, r : r + 8, :]
    first_two0((-7, -6, -5, BX + 4, BX + 5, BX + 6), 8, 32, mask32)
    for x in range(-6, BX + 6):
        scale_source(x, 8, 32, mask32)
    ex_far.wait_send()
    exw.wait_recv()
    for x in range(-3, BX + 3):
        ones = scaled_masks(mask24, 1.0, slab_weight(place, x, BX))
        halves = scaled_masks(mask24, 0.5, slab_weight(place, x, BX))
        for d in range(3):
            if 0 <= x < BX:
                rim = unpack_columns(zrw[0, d, 4:28, :], zrw[1, d, 4:28, :], x, 24)
            else:
                high, i = (0, x + 3) if x < 0 else (1, x - BX)
                rim = unpack_columns(
                    zrx[0, high, 4:28, :], zrx[1, high, 4:28, :], 3 * d + i, 24)
            for t, w in enumerate((wind[d, 0, x + 3, 4:28, :], rim)):
                half = halves[t] * w
                coef[d, 0, t, x + 3] = half - ones[t]
                coef[d, 1, t, x + 3] = -half - ones[t]
    exw.wait_send()
    ex2[0].wait_recv()
    here = coarse(0, 3)
    spread1(here, 3, -4, 16)
    exb.wait_recv()
    mask = level1_mask(-8, 24)
    for x in range(-6, 12):
        dx, i = beside(x, 6)
        near = bv[x + 6, 8:32, :]
        left, right = zrb[0, dx + 1], zrb[1, dx + 1]
        for lead, ref in ((0, b1), (64, v1)):
            value = jnp.where(
                lane24 < 64, turn(near, -lead),
                jnp.where(lane24 < 72, turn(right, 64 - 8 * i - lead),
                          jnp.where(lane24 >= 120, turn(left, 120 - 8 * i - lead), 0.0)))
            if ref is v1:
                value = value + scaled(
                    up1[(x + 6) // 2, 0:24, :], mask, slab_weight(place, x, 6))
            ref[x + 6, 8:32, :] = value
    last_two1(4, 8, 24, mask)
    spread0(4, 16)
    for x in range(-7, BX + 7):
        weight = slab_weight(place, x, BX)
        for t in range(2):
            v0[t, x + 8, 8:40, :] += scaled(up0[t, (x + 8) // 2], mask32[t], weight)
    for x in range(-6, BX + 6):
        sweep0(t0, v0, x, 8, 32, mask32)
    for x in range(-5, BX + 5):
        sweep0(v0, t0, x, 8, 32, mask32)
    first = v0

    for x in range(-4, BX + 4):
        weight = slab_weight(place, x, BX)
        half = 0.5 if weight is None else 0.5 * weight
        i = x + 8
        a, h = first[0, i, 12:36, :], first[1, i, 12:36, :]
        ba, bh = z_back(a, h)
        na, nh = z_next(a, h)
        for t, (b, n) in enumerate(((ba, na), (bh, nh))):
            m = mask24[t] * half
            velocity[0, t, x + 4, 12:36, :] = (first[t, i + 1, 12:36, :] - first[t, i - 1, 12:36, :]) * m
            velocity[1, t, x + 4, 12:36, :] = (first[t, i, 13:37, :] - first[t, i, 11:35, :]) * m
            velocity[2, t, x + 4, 12:36, :] = (n - b) * m
    for x in range(-3, BX + 3):
        weight = slab_weight(place, x, BX)
        i = x + 4
        sevens = scaled_masks(mask24, 7.0, weight)
        ways = [[[coef[e, k, t, x + 3] for k in range(2)] for e in range(3)] for t in range(2)]
        for d in range(3):
            u = velocity.at[d]
            a, h = u[0, i, 12:36, :], u[1, i, 12:36, :]
            ba, bh = z_back(a, h)
            na, nh = z_next(a, h)
            for t, (c, b, n) in enumerate(((a, ba, na), (h, bh, nh))):
                x_low, x_high = u[t, i - 1, 12:36, :], u[t, i + 1, 12:36, :]
                y_low, y_high = u[t, i, 11:35, :], u[t, i, 13:37, :]
                along_x, along_y, along_z = ways[t]
                flux[d, t, x + 3, 4:28, :] = (
                    sevens[t] * c
                    + (along_x[0] * x_high + along_x[1] * x_low)
                    + (along_y[0] * y_high + along_y[1] * y_low)
                    + (along_z[0] * n + along_z[1] * b)
                )
    for x in range(-2, BX + 2):
        weight = slab_weight(place, x, BX)
        i = x + 3
        a, h = flux[2, 0, i, 4:28, :], flux[2, 1, i, 4:28, :]
        ba, bh = z_back(a, h)
        na, nh = z_next(a, h)
        for t, (b, n) in enumerate(((ba, na), (bh, nh))):
            value = (
                (flux[0, t, i + 1, 4:28, :] - flux[0, t, i - 1, 4:28, :])
                + (flux[1, t, i, 5:29, :] - flux[1, t, i, 3:27, :])
                + (n - b)
            ) * -0.5
            b0[t, x + 8, 12:36, :] = scaled(value, mask24[t], weight)

    first_two0(range(-1, BX + 1), 12, 24, mask24)
    for i in range(6):
        pair = None
        for x in (2 * i, 2 * i + 1):
            ((c, s),) = six0(v0, x + 8, 16, 16, rim=False)
            res = b0[0, x + 8, 16:32, :] - (6.0 * c - s)
            pair = res if pair is None else pair + res
        rows0[0, i, 0:16, :] = pair
    cells = [rows0[0, i, pl.ds(0, 8, stride=2), :] + rows0[0, i, pl.ds(1, 8, stride=2), :] for i in range(6)]
    source = pick(jnp.concatenate(cells, axis=0), m_down0[0:128, :])
    low = jnp.zeros((8, 128), jnp.float32)
    high = jnp.zeros((8, 128), jnp.float32)
    for i in range(6):
        block = source[8 * i : 8 * i + 8, :]
        s1[i] = block
        l1[4 + i, 8:16, :] = block
        group = (lane8 >= 8 * i) & (lane8 < 8 * i + 8)
        low = jnp.where(group, turn(block, 8 * i), low)
        high = jnp.where(group, turn(block, 8 * i - 56), high)
    zs1[0] = high
    zs1[1] = low
    ex1.start()
    for x in range(BX):
        vp[x + 2, 16:32, :] = v0[0, x + 8, 16:32, :]
    pack0(lambda i: v0[0, 8 + i, 16:32, :], storer(zsv))
    exv.start()
    ex2[0].wait_send()
    exb.wait_send()
    ex1.wait_recv()
    for x in range(-4, 10):
        dx, i = beside(x, 6)
        b1[x + 6, 8:32, :] = jnp.where(
            lane24 < 64, l1[x + 4],
            jnp.where(lane24 < 72, turn(zr1[1, dx + 1], 64 - 8 * i),
                      jnp.where(lane24 >= 120, turn(zr1[0, dx + 1], 120 - 8 * i), 0.0)))
    mask = level1_mask(-4, 16)
    for x in range(-3, 9):
        c, s = six1(b1, x + 6, 12, 16)
        value = (1.0 + KEEP) * c1 * c + SIXTH * c1 * s
        v1[x + 6, 12:28, :] = scaled(value, mask, slab_weight(place, x, 6))
    down1_and_send(1, 12, 16)
    ex1.wait_send()
    exv.wait_send()
    exv.wait_recv()
    for x in range(-1, BX + 1):
        scale_source(x, 12, 24, mask24)
    for x in range(-2, BX + 2):
        v0[0, x + 8, 12:36, :] = vp[x + 2, 12:36, :]
        v0[1, x + 8, 8:40, :] = unpack0(zrv, x, 32)
    ex2[1].wait_recv()
    here = coarse(1, 2)
    spread1(here, 2, -2, 8)
    for x in range(-3, 9):
        v1[x + 6, 12:28, :] += scaled(up1[(x + 4) // 2, 0:16, :], mask, slab_weight(place, x, 6))
    last_two1(1, 12, 16, mask)
    spread0(1, 12)
    for x in range(-2, BX + 2):
        weight = slab_weight(place, x, BX)
        for t in range(2):
            v0[t, x + 8, 12:36, :] += scaled(up0[t, (x + 2) // 2, 0:24, :], mask24[t], weight)
    for x in range(-1, BX + 1):
        sweep0(t0, v0, x, 12, 24, mask24)
    for x in range(BX):
        ((c, s),) = six0(t0, x + 8, 16, 16, rim=False)
        out_ref[x] = KEEP * c + SIXTH * s + sb[0, x + 8, 16:32, :]
    ex2[1].wait_send()


def solution(mesh):
    sizes = tuple(mesh.shape[a] for a in AXES)
    exchanges = 8
    f32 = jnp.float32
    bf16 = jnp.bfloat16

    def vmem(*shape, dtype=f32):
        return pltpu.VMEM(shape, dtype)

    def body(pressure, wind):
        return pl.pallas_call(
            functools.partial(kernel, sizes),
            out_shape=jax.ShapeDtypeStruct((BX, BY, BZ), f32),
            in_specs=[pl.BlockSpec(memory_space=pl.ANY)] * 2,
            out_specs=pl.BlockSpec(memory_space=pltpu.VMEM),
            scratch_shapes=[
                vmem(2, 28, 48, 128),
                vmem(2, 3, 48, 128),
                vmem(2, 28, 48, 128),
                vmem(2, 28, 48, 128),
                vmem(2, 28, 48, 128),
                vmem(2, 16, 128),
                vmem(2, 3, 32, 128),
                vmem(3, 1, 18, 32, 128),
                vmem(2, 3, 16, 128),
                vmem(2, 3, 32, 128),
                vmem(2, 2, 16, 128),
                vmem(2, 2, 32, 128),
                vmem(3, 2, 2, 18, 24, 128),
                vmem(3, 2, 20, 48, 128),
                vmem(3, 2, 18, 32, 128),
                vmem(16, 48, 128),
                vmem(2, 16, 128),
                vmem(2, 3, 32, 128),
                vmem(18, 40, 128),
                vmem(2, 8, 128),
                vmem(2, 3, 24, 128),
                vmem(6, 8, 128),
                vmem(14, 24, 128),
                vmem(2, 8, 128),
                vmem(2, 3, 24, 128),
                vmem(18, 40, 128),
                vmem(18, 40, 128),
                vmem(18, 40, 128),
                vmem(2, 5, 3, 5, 4, 128),
                vmem(3, 5, 24, 128),
                vmem(15, 24, 128),
                vmem(15, 24, 128),
                vmem(15, 24, 128),
                vmem(2, 10, 32, 128),
                vmem(8, 128),
                vmem(9, 32, 128),
                vmem(2, 14, 32, 128),
                vmem(256, 128, dtype=bf16),
                vmem(384, 128, dtype=bf16),
                vmem(128, 128, dtype=bf16),
                vmem(128, 256, dtype=bf16),
                vmem(512, 4, 128),
                pltpu.SemaphoreType.DMA((exchanges,)),
                pltpu.SemaphoreType.DMA((exchanges,)),
                pltpu.SemaphoreType.DMA((2,)),
            ],
            compiler_params=pltpu.CompilerParams(
                collective_id=0, has_side_effects=True, vmem_limit_bytes=67043328
            ),
            name="schur",
        )(pressure, wind)

    in_specs = (P("gx", "gy", "gz"), P(None, "gx", "gy", "gz"))
    return jax.shard_map(
        body, mesh=mesh, in_specs=in_specs, out_specs=P("gx", "gy", "gz"), check_vma=False
    )
```

```python
import functools

import jax
import jax.numpy as jnp
from jax import lax
from jax.experimental import pallas as pl
from jax.experimental.pallas import tpu as pltpu
from jax.sharding import PartitionSpec as P

MESH = pl.DeviceIdType.MESH
AXES = ("gx", "gy", "gz")
BX, BY, BZ = 12, 16, 128
OMEGA = 0.8
KEEP = 1.0 - OMEGA
SIXTH = OMEGA / 6.0

AROUND = [
    (dx, dy, dz)
    for dz in (0, 1, -1)
    for dx in (0, 1, -1)
    for dy in (0, 1, -1)
    if (dx, dy, dz) != (0, 0, 0)
]
AROUND.sort(key=lambda d: -(abs(d[0]) + abs(d[1]) + abs(d[2])))

NEAR = [d for d in AROUND if sum(map(abs, d)) <= 2]


def coarse_offsets(far_edges):
    out = []
    for dx in range(-2, 3):
        for dy in range(-2, 3):
            for dz in (-1, 0, 1):
                shape = (abs(dx), abs(dy), abs(dz))
                if shape[:2] in ((0, 0), (0, 1), (1, 0), (1, 1), (0, 2), (2, 0), (2, 1)):
                    keep = shape != (0, 0, 0)
                else:
                    keep = far_edges and shape[:2] == (1, 2)
                if keep:
                    out.append((dx, dy, dz))
    return sorted(out, key=lambda d: -sum(map(abs, d)))


COARSE = (coarse_offsets(True), coarse_offsets(False))
GREETED = AROUND


def part(delta, count, width):
    if delta == 0:
        return 0, 0, count
    if delta > 0:
        return count - width, -width, width
    return 0, count, width


class Place:
    def __init__(self, sizes):
        self.sizes = sizes
        self.at = [lax.axis_index(a) for a in AXES]
        self.has = []
        for g, n in zip(self.at, sizes):
            self.has.append({d: (g + d >= 0) & (g + d < n) for d in (-2, -1, 1, 2)})

        kinds = []
        for n in sizes:
            kinds.append(sorted({
                tuple(sum(0 <= g + d < n for d in (-k, k)) for k in (1, 2)) for g in range(n)
            }))
        self.profiles = [(a, b, c) for a in kinds[0] for b in kinds[1] for c in kinds[2]]
        self.kinds = kinds
        self.counts = [
            [t[-k].astype(jnp.int32) + t[k].astype(jnp.int32) for k in (1, 2)] for t in self.has
        ]

    def matches(self, profile):
        found = None
        for counts, wanted, kinds in zip(self.counts, profile, self.kinds):
            for c, v, seen in zip(counts, wanted, zip(*kinds)):
                if len(set(seen)) > 1:
                    found = (c == v) if found is None else found & (c == v)
        return True if found is None else found

    def exists(self, offset):
        found = None
        for table, d in zip(self.has, offset):
            if d:
                found = table[d] if found is None else found & table[d]
        return found

    def device(self, offset):
        return tuple(
            lax.rem(g + (d + n), n) if d else g for g, d, n in zip(self.at, offset, self.sizes)
        )


class Exchange:
    def __init__(self, place, copies, send_sem, recv_sem, ruler):
        self.place, self.items = place, []
        self.send_sem, self.recv_sem, self.ruler = send_sem, recv_sem, ruler
        self.weights = []
        for offset, src, dst in copies:
            copy = pltpu.make_async_remote_copy(
                src_ref=src,
                dst_ref=dst,
                send_sem=send_sem,
                recv_sem=recv_sem,
                device_id=place.device(offset),
                device_id_type=MESH,
            )
            self.items.append((offset, copy))
            units = 1
            for n in src.shape:
                units *= n
            self.weights.append((tuple(abs(d) for d in offset), units // 512))

    def start(self):
        for offset, copy in self.items:
            pl.when(self.place.exists(offset))(copy.start)

    def wait(self, sem):
        for profile in self.place.profiles:
            total = 0
            for shape, units in self.weights:
                share = 8 * units
                for counts, d in zip(profile, shape):
                    share = share * counts[d - 1] // 2 if d else share
                total += share
            total //= 8
            if total:
                rows = self.ruler.at[pl.ds(0, total)]
                pl.when(self.place.matches(profile))(pltpu.make_async_copy(rows, rows, sem).wait)

    def wait_recv(self):
        self.wait(self.recv_sem)

    def wait_send(self):
        self.wait(self.send_sem)


def lanes(rows):
    return lax.broadcasted_iota(jnp.int32, (rows, 128), 1)


def row_mask(place, first_row, rows, extent):
    y = first_row + lax.broadcasted_iota(jnp.int32, (rows, 128), 0)
    low = jnp.where(place.has[1][-1], -64, 0)
    high = jnp.where(place.has[1][1], 64, extent)
    return (y >= low) & (y < high)


def rim_lanes(place, rows, start, right_end):
    lane = lanes(rows)
    right_stop = jnp.where(place.has[2][1], right_end, 0)
    left_start = jnp.where(place.has[2][-1], 120, 128)
    return ((lane >= start) & (lane < right_stop)) | (lane >= left_start)


def slab_weight(place, x, extent):
    if x < 0:
        return place.has[0][-1].astype(jnp.float32)
    if x >= extent:
        return place.has[0][1].astype(jnp.float32)
    return None


def z_back(a, h):
    lane0 = lanes(a.shape[0]) == 0
    ra, rh = pltpu.roll(a, 1, 1), pltpu.roll(h, 1, 1)
    return jnp.where(lane0, rh, ra), jnp.where(lane0, ra, rh)


def z_next(a, h):
    lane127 = lanes(a.shape[0]) == 127
    ra, rh = pltpu.roll(a, 127, 1), pltpu.roll(h, 127, 1)
    return jnp.where(lane127, rh, ra), jnp.where(lane127, ra, rh)


def masks0(place, first_row, rows):
    inner = row_mask(place, first_row, rows, BY)
    rim = inner & rim_lanes(place, rows, 0, 8)
    return inner.astype(jnp.float32), rim.astype(jnp.float32)


def scaled(value, mask, weight):
    value = value * mask
    return value if weight is None else value * weight


def six0(ref, i, r, n, rim=True):
    a, h = ref[0, i, r : r + n, :], ref[1, i, r : r + n, :]
    ba, bh = z_back(a, h)
    na, nh = z_next(a, h)
    out = []
    for t, (c, b, f) in enumerate(((a, ba, na), (h, bh, nh))):
        if t and not rim:
            break
        s = (
            (ref[t, i - 1, r : r + n, :] + ref[t, i + 1, r : r + n, :])
            + (ref[t, i, r - 1 : r - 1 + n, :] + ref[t, i, r + 1 : r + 1 + n, :])
            + (b + f)
        )
        out.append((c, s))
    return out


def six1(ref, i, r, n):
    c = ref[i, r : r + n, :]
    s = (
        (ref[i - 1, r : r + n, :] + ref[i + 1, r : r + n, :])
        + (ref[i, r - 1 : r - 1 + n, :] + ref[i, r + 1 : r + 1 + n, :])
        + (pltpu.roll(c, 1, 1) + pltpu.roll(c, 127, 1))
    )
    return c, s


def pick(a, m):
    high = a.astype(jnp.bfloat16)
    low = (a - high.astype(jnp.float32)).astype(jnp.bfloat16)
    return jnp.dot(high, m, preferred_element_type=jnp.float32) + jnp.dot(
        low, m, preferred_element_type=jnp.float32
    )


def turn(value, shift):
    shift %= 128
    return pltpu.roll(value, shift, 1) if shift else value


def pack0(load, store, count=BX):
    lane = lanes(BY)
    first = jnp.zeros((BY, 128), jnp.float32)
    last = jnp.zeros((BY, 128), jnp.float32)
    for i in range(count):
        turned = turn(load(i), 8 * i)
        first = jnp.where((lane >= 8 * i) & (lane < 8 * i + 8), turned, first)
        at = (8 * i - 8) % 128
        last = jnp.where((lane >= at) & (lane < at + 8), turned, last)
    store(first, last)


def beside(x, count):
    return (0, x) if 0 <= x < count else ((-1, x + count) if x < 0 else (1, x - count))


def unpack0(land, x, rows):
    dx, i = beside(x, BX)
    return unpack_columns(land[0, dx + 1], land[1, dx + 1], i, rows)


def unpack_columns(left, right, i, rows):
    left, right = turn(left, -8 * i), turn(right, -8 * i)
    lane = lanes(rows)
    return jnp.where(lane < 8, right, jnp.where(lane >= 120, left, 0.0))


def rim_copies(source, land, offsets):
    out = []
    for offset in offsets:
        dx, dy, dz = offset
        if dz == 0:
            continue
        y0, yd, ny = part(dy, BY, 8)
        side = 0 if dz > 0 else 1
        out.append((offset, source(side, y0, ny), land(side, 1 - dx, yd, ny)))
    return out


def block_copies(source, land, reach, offsets, edge=None):
    out = []
    for offset in offsets:
        dx, dy, dz = offset
        if dz != 0:
            continue
        near, far = edge if edge and dy else reach
        if dx == 0:
            x0, xd, nx = 0, 0, BX
        elif dx > 0:
            x0, xd, nx = BX - far, -far, far - near + 1
        else:
            x0, xd, nx = near - 1, BX + near - 1, far - near + 1
        y0, yd, ny = part(dy, BY, 8)
        out.append((offset, source(x0, nx, y0, ny), land(xd, nx, yd, ny)))
    return out


def ordered(copies):
    return sorted(copies, key=lambda c: -sum(abs(d) for d in c[0]))


def clear_around(ref, lead_x, lead_y, count_y):
    nx, ny = ref.shape[0], ref.shape[1]
    ref[0:lead_x] = jnp.zeros((lead_x, ny, 128), jnp.float32)
    ref[lead_x + BX : nx] = jnp.zeros((nx - lead_x - BX, ny, 128), jnp.float32)
    ref[lead_x : lead_x + BX, 0:lead_y, :] = jnp.zeros((BX, lead_y, 128), jnp.float32)
    end = lead_y + count_y
    ref[lead_x : lead_x + BX, end:ny, :] = jnp.zeros((BX, ny - end, 128), jnp.float32)


def clear(*refs):
    for ref in refs:
        ref[...] = jnp.zeros(ref.shape, ref.dtype)


def kernel(
    sizes, p_ref, w_ref, out_ref,
    b0, far, sb, v0, t0, zs0, zr0, wind, zsw, zrw, zsx, zrx, coef, velocity, flux,
    vp, zsv, zrv,
    bv, zsb, zrb, s1, l1, zs1, zr1, b1, v1, t1,
    gathered, merged, c2, e2a, e2b,
    rows0, rows2, up1, up0, m_down0, m_down1, m_up1, m_up0,
    ruler, send_sems, recv_sems, load_sems,
):
    place = Place(sizes)
    load_p = pltpu.make_async_copy(
        p_ref, b0.at[0, pl.ds(8, BX), pl.ds(16, BY), :], load_sems.at[0])
    load_w = pltpu.make_async_copy(
        w_ref, wind.at[:, 0, pl.ds(3, BX), pl.ds(8, BY), :], load_sems.at[1])
    load_p.start()
    load_w.start()

    clear_around(b0.at[0], 8, 16, BY)
    for d in range(3):
        clear_around(wind.at[d, 0], 3, 8, BY)
    clear(far, zr0, zrw, zrx, vp, zrv, bv, zrb, l1, zr1, gathered)

    barrier = pltpu.get_barrier_semaphore()
    total = jnp.int32(0)
    for offset in GREETED:
        there = place.exists(offset)
        total = total + there.astype(jnp.int32)

        def greet(offset=offset):
            pl.semaphore_signal(
                barrier, inc=1, device_id=place.device(offset), device_id_type=MESH
            )

        pl.when(there)(greet)

    def storer(ref):
        def store(f, l):
            ref[0] = l
            ref[1] = f
        return store

    clear(b0.at[1], v0, t0, rows0)
    load_p.wait()
    pack0(lambda i: b0[0, 8 + i, 16:32, :], storer(zs0))

    used = [0]

    def exchange(copies):
        k = used[0]
        used[0] += 1
        return Exchange(place, ordered(copies), send_sems.at[k], recv_sems.at[k], ruler)

    def far_block(x, nx, y, ny):
        side, lead = (0, 8) if x < 0 else (1, -BX - 5)
        return far.at[side, pl.ds(x + lead, nx), pl.ds(y + 16, ny), :]

    def b0_block(x, nx, y, ny):
        return b0.at[0, pl.ds(x + 8, nx), pl.ds(y + 16, ny), :]

    def wind_block(x, nx, y, ny):
        return wind.at[:, 0, pl.ds(x + 3, nx), pl.ds(y + 8, ny), :]

    def vp_block(x, nx, y, ny):
        return vp.at[pl.ds(x + 2, nx), pl.ds(y + 16, ny), :]

    def wind_side_copies():
        out = []
        for offset in AROUND:
            dx, dy, dz = offset
            if dx and dz:
                y0, yd, ny = part(dy, BY, 8)
                side = 0 if dz > 0 else 1
                out.append((
                    offset, zsx.at[side, (dx + 1) // 2, pl.ds(y0, ny), :],
                    zrx.at[side, (1 - dx) // 2, pl.ds(yd + 8, ny), :]))
        return out

    ex0 = exchange(
        block_copies(b0_block, b0_block, (1, 6), AROUND, (1, 5))
        + rim_copies(
            lambda s, y, ny: zs0.at[s, pl.ds(y, ny), :],
            lambda s, dx, y, ny: zr0.at[s, dx, pl.ds(y + 8, ny), :], AROUND))
    sides = [d for d in AROUND if d[0]]
    ex_far = exchange(
        block_copies(b0_block, far_block, (7, 8), [d for d in sides if d[2] == 0], (6, 7)))
    exw = exchange(
        block_copies(wind_block, wind_block, (1, 3), AROUND, (1, 2))
        + rim_copies(
            lambda s, y, ny: zsw.at[s, :, pl.ds(y, ny), :],
            lambda s, dx, y, ny: zrw.at[s, :, pl.ds(y + 8, ny), :],
            [d for d in AROUND if not d[0]])
        + wind_side_copies())
    exv = exchange(
        block_copies(vp_block, vp_block, (1, 2), NEAR, (1, 1))
        + rim_copies(
            lambda s, y, ny: zsv.at[s, pl.ds(y, ny), :],
            lambda s, dx, y, ny: zrv.at[s, dx, pl.ds(y + 8, ny), :], NEAR))

    def bv_copies():
        out = []
        for offset in AROUND:
            dx, dy, dz = offset
            if dz == 0:
                out.append((
                    offset, bv.at[pl.ds(6, 6), pl.ds(16, 8), :],
                    bv.at[pl.ds(6 - 6 * dx, 6), pl.ds(16 - 8 * dy, 8), :]))
            else:
                side = 0 if dz > 0 else 1
                out.append((
                    offset, zsb.at[side], zrb.at[side, 1 - dx, pl.ds(8 - 8 * dy, 8), :]))
        return out

    def level1_copies():
        out = []
        for offset in AROUND:
            dx, dy, dz = offset
            if dz == 0:
                x0, xd, nx = part(dx, 6, 4)
                out.append((
                    offset, s1.at[pl.ds(x0, nx)],
                    l1.at[pl.ds(xd + 4, nx), pl.ds(8 - 8 * dy, 8), :]))
            else:
                side = 0 if dz > 0 else 1
                out.append((
                    offset, zs1.at[side], zr1.at[side, 1 - dx, pl.ds(8 - 8 * dy, 8), :]))
        return out

    def coarse_copies(number):
        return [
            (d, gathered.at[number, 2, 1, 2], gathered.at[number, 2 - d[1], 1 - d[2], 2 - d[0]])
            for d in COARSE[number]
        ]

    exb = exchange(bv_copies())
    ex1 = exchange(level1_copies())
    ex2 = [exchange(coarse_copies(0)), exchange(coarse_copies(1))]

    pl.semaphore_wait(barrier, total)
    ex0.start()
    ex_far.start()

    load_w.wait()
    for d in range(3):
        pack0(lambda i: wind[d, 0, 3 + i, 8:24, :], storer(zsw.at[:, d]))
    for high, lead in ((0, 3), (1, BX)):
        pack0(lambda i: wind[i // 3, 0, lead + i % 3, 8:24, :], storer(zsx.at[:, high]), 9)
    exw.start()

    clear(velocity, flux, sb, b1, v1, t1, merged, c2, e2a, e2b, rows2, up1, up0)

    bf16 = jnp.bfloat16
    k = lax.broadcasted_iota(jnp.int32, (128, 128), 0)
    l = lax.broadcasted_iota(jnp.int32, (128, 128), 1)
    eighth = jnp.float32(0.125)
    m_down0[0:128, :] = jnp.where(k // 2 == l, eighth, 0.0).astype(bf16)
    m_down0[128:256, :] = jnp.where(
        ((k < 8) | (k >= 120)) & (k // 2 + 64 == l), eighth, 0.0).astype(bf16)
    for i in range(3):
        m_down1[i * 128 : i * 128 + 128, :] = jnp.where(
            (l // 32 == i) & (k // 2 == l % 32), eighth, 0.0).astype(bf16)
    m_up1[...] = jnp.where(
        ((l < 72) & (k == l // 2)) | ((l >= 120) & (k == 64 + l // 2)), 1.0, 0.0).astype(bf16)
    m_up0[:, 0:128] = jnp.where(k == l // 2, 1.0, 0.0).astype(bf16)
    m_up0[:, 128:256] = jnp.where(
        ((l < 8) | (l >= 120)) & (k == 64 + l // 2), 1.0, 0.0).astype(bf16)

    c0 = OMEGA / 6.0
    w1 = 0.25
    c1 = OMEGA / (6.0 * w1)
    w2 = 0.0625
    c2s = OMEGA / (6.0 * w2)
    lane8, lane16, lane24, lane40 = lanes(8), lanes(16), lanes(24), lanes(40)
    m32a, m32h = masks0(place, -8, 32)
    m24a, m24h = masks0(place, -4, 24)
    mask32, mask24 = (m32a, m32h), (m24a, m24h)

    def level1_mask(first_row, rows):
        lane = lanes(rows)
        inside = row_mask(place, first_row, rows, 8)
        return (inside & ((lane < 64) | rim_lanes(place, rows, 64, 72))).astype(jnp.float32)

    def scaled_masks(masks, factor, weight):
        factor = factor if weight is None else factor * weight
        return [m * factor for m in masks]

    def sweep0(target, iterate, x, r, n, masks):
        weight = slab_weight(place, x, BX)
        keep, share = scaled_masks(masks, KEEP, weight), scaled_masks(masks, SIXTH, weight)
        for t, (c, s) in enumerate(six0(iterate, x + 8, r, n)):
            target[t, x + 8, r : r + n, :] = keep[t] * c + share[t] * s + sb[t, x + 8, r : r + n, :]

    def scale_source(x, r, n, masks):
        factor = scaled_masks(masks, c0, slab_weight(place, x, BX))
        for t in range(2):
            sb[t, x + 8, r : r + n, :] = factor[t] * b0[t, x + 8, r : r + n, :]

    def first_two0(slabs, r, n, masks):
        for x in slabs:
            weight = slab_weight(place, x, BX)
            for t, (c, s) in enumerate(six0(b0, x + 8, r, n)):
                value = (1.0 + KEEP) * c0 * c + SIXTH * c0 * s
                v0[t, x + 8, r : r + n, :] = scaled(value, masks[t], weight)

    def down1_and_send(number, r, n):
        pairs = []
        for i in range(3):
            pair = None
            for x in (2 * i, 2 * i + 1):
                c, s = six1(v1, x + 6, 16, 8)
                res = b1[x + 6, 16:24, :] - w1 * (6.0 * c - s)
                pair = res if pair is None else pair + res
            pairs.append(jnp.where(lane8 < 64, pair, 0.0))
        rows2[...] = pick(jnp.concatenate(pairs, axis=1), m_down1[...])
        gathered[number, 2, 1, 2] = (
            rows2[pl.ds(0, 4, stride=2), :] + rows2[pl.ds(1, 4, stride=2), :])
        ex2[number].start()

    def coarse(number, reach):
        for az in range(3):
            for ax in range(5):
                for ay in range(5):
                    merged[az, ax, 4 * ay : 4 * ay + 4, :] = gathered[number, ay, az, ax]
        for x in range(-reach - 3, 3 + reach + 3):
            ax, i = (x + 6) // 3, (x + 6) % 3
            left = turn(merged[0, ax], 96 - 32 * i)
            own = turn(merged[1, ax], -32 * i)
            right = turn(merged[2, ax], 32 - 32 * i)
            c2[x + 6] = jnp.where(
                lane24 < 32, own, jnp.where(lane24 < 40, right, jnp.where(lane24 >= 120, left, 0.0)))
        inside = row_mask(place, -6, 16, 4)
        mask2 = (inside & ((lane16 < 32) | rim_lanes(place, 16, 32, 40))).astype(jnp.float32)
        for x in range(-reach - 2, 3 + reach + 2):
            c, s = six1(c2, x + 6, 2, 16)
            value = (1.0 + KEEP) * c2s * c + SIXTH * c2s * s
            e2a[x + 6, 2:18, :] = scaled(value, mask2, slab_weight(place, x, 3))
        here, there = e2a, e2b
        for more in (1, 0):
            for x in range(-reach - more, 3 + reach + more):
                c, s = six1(here, x + 6, 2, 16)
                value = KEEP * c + SIXTH * s + c2s * c2[x + 6, 2:18, :]
                there[x + 6, 2:18, :] = scaled(value, mask2, slab_weight(place, x, 3))
            here, there = there, here
        return here

    def spread1(here, reach, y, n):
        slabs = 3 + 2 * reach
        spread = pick(
            jnp.concatenate([here[x - reach + 6, y + 8 : y + 8 + n, :] for x in range(slabs)], axis=0),
            m_up1[...])
        for j in range(slabs):
            value = spread[n * j : n * j + n, :]
            up1[j, pl.ds(0, n, stride=2), :] = value
            up1[j, pl.ds(1, n, stride=2), :] = value

    def last_two1(reach, r, n, mask):
        for x in range(-reach - 1, 6 + reach + 1):
            c, s = six1(v1, x + 6, r, n)
            value = KEEP * c + SIXTH * s + c1 * b1[x + 6, r : r + n, :]
            t1[x + 6, r : r + n, :] = scaled(value, mask, slab_weight(place, x, 6))
        for x in range(-reach, 6 + reach):
            c, s = six1(t1, x + 6, r, n)
            value = KEEP * c + SIXTH * s + c1 * b1[x + 6, r : r + n, :]
            v1[x + 6, r : r + n, :] = scaled(value, mask, slab_weight(place, x, 6))

    def spread0(reach, n):
        y = -(n - 8) // 2
        slabs = 6 + 2 * reach
        spread = pick(
            jnp.concatenate(
                [v1[x - reach + 6, y + 16 : y + 32, :] for x in range(slabs)], axis=0),
            m_up0[...])
        for j in range(slabs):
            for t in range(2):
                value = spread[16 * j : 16 * j + n, 128 * t : 128 * t + 128]
                up0[t, j, pl.ds(0, n, stride=2), :] = value
                up0[t, j, pl.ds(1, n, stride=2), :] = value

    ex0.wait_recv()
    for x in range(-8, BX + 8):
        b0[1, x + 8, 8:40, :] = unpack0(zr0, x, 32)
    first_two0(range(-5, BX + 5), 8, 32, mask32)
    for i in range(10):
        pair = [None, None]
        for x in (2 * i - 4, 2 * i - 3):
            for t, (c, s) in enumerate(six0(v0, x + 8, 12, 24)):
                res = b0[t, x + 8, 12:36, :] - (6.0 * c - s)
                pair[t] = res if pair[t] is None else pair[t] + res
        for t in range(2):
            rows0[t, i, 0:24, :] = pair[t]
    cells = [
        jnp.concatenate(
            [rows0[t, i, pl.ds(0, 16, stride=2), :] + rows0[t, i, pl.ds(1, 16, stride=2), :]
             for t in range(2)], axis=1)
        for i in range(10)
    ]
    source = pick(jnp.concatenate(cells, axis=0), m_down0[...])
    mask = level1_mask(-2, 16)
    for x in range(-2, 8):
        b1[x + 6, 14:30, :] = scaled(
            source[16 * (x + 2) : 16 * (x + 2) + 16, :], mask, slab_weight(place, x, 6))
    for x in range(-1, 7):
        c, s = six1(b1, x + 6, 14, 16)
        value = (1.0 + KEEP) * c1 * c + SIXTH * c1 * s
        v1[x + 6, 14:30, :] = scaled(value, mask, slab_weight(place, x, 6))
    down1_and_send(0, 14, 16)

    low = jnp.zeros((8, 128), jnp.float32)
    high = jnp.zeros((8, 128), jnp.float32)
    for i in range(6):
        block_b, block_v = b1[i + 6, 16:24, :], v1[i + 6, 16:24, :]
        bv[i + 6, 16:24, :] = jnp.where(lane8 < 64, block_b, pltpu.roll(block_v, 64, 1))
        for block, lead in ((block_b, 0), (block_v, 64)):
            group = (lane8 >= lead + 8 * i) & (lane8 < lead + 8 * i + 8)
            low = jnp.where(group, turn(block, lead + 8 * i), low)
            high = jnp.where(group, turn(block, lead + 8 * i - 56), high)
    zsb[0] = high
    zsb[1] = low
    exb.start()
    ex0.wait_send()
    ex_far.wait_recv()
    for side in range(2):
        for k in range(3):
            x = k - 8 if side == 0 else BX + 5 + k
            distance = -x if side == 0 else x - BX + 1
            if distance > 6:
                b0[0, x + 8, 16:32, :] = far[side, k, 16:32, :]
            if distance < 8:
                for r in (8, 32):
                    b0[0, x + 8, r : r + 8, :] = far[side, k, r : r + 8, :]
    first_two0((-7, -6, -5, BX + 4, BX + 5, BX + 6), 8, 32, mask32)
    for x in range(-6, BX + 6):
        scale_source(x, 8, 32, mask32)
    ex_far.wait_send()
    exw.wait_recv()
    for x in range(-3, BX + 3):
        ones = scaled_masks(mask24, 1.0, slab_weight(place, x, BX))
        halves = scaled_masks(mask24, 0.5, slab_weight(place, x, BX))
        for d in range(3):
            if 0 <= x < BX:
                rim = unpack_columns(zrw[0, d, 4:28, :], zrw[1, d, 4:28, :], x, 24)
            else:
                high, i = (0, x + 3) if x < 0 else (1, x - BX)
                rim = unpack_columns(
                    zrx[0, high, 4:28, :], zrx[1, high, 4:28, :], 3 * d + i, 24)
            for t, w in enumerate((wind[d, 0, x + 3, 4:28, :], rim)):
                half = halves[t] * w
                coef[d, 0, t, x + 3] = half - ones[t]
                coef[d, 1, t, x + 3] = -half - ones[t]
    exw.wait_send()
    ex2[0].wait_recv()
    here = coarse(0, 3)
    spread1(here, 3, -4, 16)
    exb.wait_recv()
    mask = level1_mask(-8, 24)
    for x in range(-6, 12):
        dx, i = beside(x, 6)
        near = bv[x + 6, 8:32, :]
        left, right = zrb[0, dx + 1], zrb[1, dx + 1]
        for lead, ref in ((0, b1), (64, v1)):
            value = jnp.where(
                lane24 < 64, turn(near, -lead),
                jnp.where(lane24 < 72, turn(right, 64 - 8 * i - lead),
                          jnp.where(lane24 >= 120, turn(left, 120 - 8 * i - lead), 0.0)))
            if ref is v1:
                value = value + scaled(
                    up1[(x + 6) // 2, 0:24, :], mask, slab_weight(place, x, 6))
            ref[x + 6, 8:32, :] = value
    last_two1(4, 8, 24, mask)
    spread0(4, 16)
    for x in range(-7, BX + 7):
        weight = slab_weight(place, x, BX)
        for t in range(2):
            v0[t, x + 8, 8:40, :] += scaled(up0[t, (x + 8) // 2], mask32[t], weight)
    for x in range(-6, BX + 6):
        sweep0(t0, v0, x, 8, 32, mask32)
    for x in range(-5, BX + 5):
        sweep0(v0, t0, x, 8, 32, mask32)
    first = v0

    for x in range(-4, BX + 4):
        weight = slab_weight(place, x, BX)
        half = 0.5 if weight is None else 0.5 * weight
        i = x + 8
        a, h = first[0, i, 12:36, :], first[1, i, 12:36, :]
        ba, bh = z_back(a, h)
        na, nh = z_next(a, h)
        for t, (b, n) in enumerate(((ba, na), (bh, nh))):
            m = mask24[t] * half
            velocity[0, t, x + 4, 12:36, :] = (first[t, i + 1, 12:36, :] - first[t, i - 1, 12:36, :]) * m
            velocity[1, t, x + 4, 12:36, :] = (first[t, i, 13:37, :] - first[t, i, 11:35, :]) * m
            velocity[2, t, x + 4, 12:36, :] = (n - b) * m
    for x in range(-3, BX + 3):
        weight = slab_weight(place, x, BX)
        i = x + 4
        sevens = scaled_masks(mask24, 7.0, weight)
        ways = [[[coef[e, k, t, x + 3] for k in range(2)] for e in range(3)] for t in range(2)]
        for d in range(3):
            u = velocity.at[d]
            a, h = u[0, i, 12:36, :], u[1, i, 12:36, :]
            ba, bh = z_back(a, h)
            na, nh = z_next(a, h)
            for t, (c, b, n) in enumerate(((a, ba, na), (h, bh, nh))):
                x_low, x_high = u[t, i - 1, 12:36, :], u[t, i + 1, 12:36, :]
                y_low, y_high = u[t, i, 11:35, :], u[t, i, 13:37, :]
                along_x, along_y, along_z = ways[t]
                flux[d, t, x + 3, 4:28, :] = (
                    sevens[t] * c
                    + (along_x[0] * x_high + along_x[1] * x_low)
                    + (along_y[0] * y_high + along_y[1] * y_low)
                    + (along_z[0] * n + along_z[1] * b)
                )
    for x in range(-2, BX + 2):
        weight = slab_weight(place, x, BX)
        i = x + 3
        a, h = flux[2, 0, i, 4:28, :], flux[2, 1, i, 4:28, :]
        ba, bh = z_back(a, h)
        na, nh = z_next(a, h)
        for t, (b, n) in enumerate(((ba, na), (bh, nh))):
            value = (
                (flux[0, t, i + 1, 4:28, :] - flux[0, t, i - 1, 4:28, :])
                + (flux[1, t, i, 5:29, :] - flux[1, t, i, 3:27, :])
                + (n - b)
            ) * -0.5
            b0[t, x + 8, 12:36, :] = scaled(value, mask24[t], weight)

    first_two0(range(-1, BX + 1), 12, 24, mask24)
    for i in range(6):
        pair = None
        for x in (2 * i, 2 * i + 1):
            ((c, s),) = six0(v0, x + 8, 16, 16, rim=False)
            res = b0[0, x + 8, 16:32, :] - (6.0 * c - s)
            pair = res if pair is None else pair + res
        rows0[0, i, 0:16, :] = pair
    cells = [rows0[0, i, pl.ds(0, 8, stride=2), :] + rows0[0, i, pl.ds(1, 8, stride=2), :] for i in range(6)]
    source = pick(jnp.concatenate(cells, axis=0), m_down0[0:128, :])
    low = jnp.zeros((8, 128), jnp.float32)
    high = jnp.zeros((8, 128), jnp.float32)
    for i in range(6):
        block = source[8 * i : 8 * i + 8, :]
        s1[i] = block
        l1[4 + i, 8:16, :] = block
        group = (lane8 >= 8 * i) & (lane8 < 8 * i + 8)
        low = jnp.where(group, turn(block, 8 * i), low)
        high = jnp.where(group, turn(block, 8 * i - 56), high)
    zs1[0] = high
    zs1[1] = low
    ex1.start()
    for x in range(BX):
        vp[x + 2, 16:32, :] = v0[0, x + 8, 16:32, :]
    pack0(lambda i: v0[0, 8 + i, 16:32, :], storer(zsv))
    exv.start()
    ex2[0].wait_send()
    exb.wait_send()
    ex1.wait_recv()
    for x in range(-4, 10):
        dx, i = beside(x, 6)
        b1[x + 6, 8:32, :] = jnp.where(
            lane24 < 64, l1[x + 4],
            jnp.where(lane24 < 72, turn(zr1[1, dx + 1], 64 - 8 * i),
                      jnp.where(lane24 >= 120, turn(zr1[0, dx + 1], 120 - 8 * i), 0.0)))
    mask = level1_mask(-4, 16)
    for x in range(-3, 9):
        c, s = six1(b1, x + 6, 12, 16)
        value = (1.0 + KEEP) * c1 * c + SIXTH * c1 * s
        v1[x + 6, 12:28, :] = scaled(value, mask, slab_weight(place, x, 6))
    down1_and_send(1, 12, 16)
    ex1.wait_send()
    exv.wait_send()
    exv.wait_recv()
    for x in range(-1, BX + 1):
        scale_source(x, 12, 24, mask24)
    for x in range(-2, BX + 2):
        v0[0, x + 8, 12:36, :] = vp[x + 2, 12:36, :]
        v0[1, x + 8, 8:40, :] = unpack0(zrv, x, 32)
    ex2[1].wait_recv()
    here = coarse(1, 2)
    spread1(here, 2, -2, 8)
    for x in range(-3, 9):
        v1[x + 6, 12:28, :] += scaled(up1[(x + 4) // 2, 0:16, :], mask, slab_weight(place, x, 6))
    last_two1(1, 12, 16, mask)
    spread0(1, 12)
    for x in range(-2, BX + 2):
        weight = slab_weight(place, x, BX)
        for t in range(2):
            v0[t, x + 8, 12:36, :] += scaled(up0[t, (x + 2) // 2, 0:24, :], mask24[t], weight)
    for x in range(-1, BX + 1):
        sweep0(t0, v0, x, 12, 24, mask24)
    for x in range(BX):
        ((c, s),) = six0(t0, x + 8, 16, 16, rim=False)
        out_ref[x] = KEEP * c + SIXTH * s + sb[0, x + 8, 16:32, :]
    ex2[1].wait_send()


def solution(mesh):
    sizes = tuple(mesh.shape[a] for a in AXES)
    exchanges = 8
    f32 = jnp.float32
    bf16 = jnp.bfloat16

    def vmem(*shape, dtype=f32):
        return pltpu.VMEM(shape, dtype)

    def body(pressure, wind):
        return pl.pallas_call(
            functools.partial(kernel, sizes),
            out_shape=jax.ShapeDtypeStruct((BX, BY, BZ), f32),
            in_specs=[pl.BlockSpec(memory_space=pl.ANY)] * 2,
            out_specs=pl.BlockSpec(memory_space=pltpu.VMEM),
            scratch_shapes=[
                vmem(2, 28, 48, 128),
                vmem(2, 3, 48, 128),
                vmem(2, 28, 48, 128),
                vmem(2, 28, 48, 128),
                vmem(2, 28, 48, 128),
                vmem(2, 16, 128),
                vmem(2, 3, 32, 128),
                vmem(3, 1, 18, 32, 128),
                vmem(2, 3, 16, 128),
                vmem(2, 3, 32, 128),
                vmem(2, 2, 16, 128),
                vmem(2, 2, 32, 128),
                vmem(3, 2, 2, 18, 24, 128),
                vmem(3, 2, 20, 48, 128),
                vmem(3, 2, 18, 32, 128),
                vmem(16, 48, 128),
                vmem(2, 16, 128),
                vmem(2, 3, 32, 128),
                vmem(18, 40, 128),
                vmem(2, 8, 128),
                vmem(2, 3, 24, 128),
                vmem(6, 8, 128),
                vmem(14, 24, 128),
                vmem(2, 8, 128),
                vmem(2, 3, 24, 128),
                vmem(18, 40, 128),
                vmem(18, 40, 128),
                vmem(18, 40, 128),
                vmem(2, 5, 3, 5, 4, 128),
                vmem(3, 5, 24, 128),
                vmem(15, 24, 128),
                vmem(15, 24, 128),
                vmem(15, 24, 128),
                vmem(2, 10, 32, 128),
                vmem(8, 128),
                vmem(9, 32, 128),
                vmem(2, 14, 32, 128),
                vmem(256, 128, dtype=bf16),
                vmem(384, 128, dtype=bf16),
                vmem(128, 128, dtype=bf16),
                vmem(128, 256, dtype=bf16),
                vmem(512, 4, 128),
                pltpu.SemaphoreType.DMA((exchanges,)),
                pltpu.SemaphoreType.DMA((exchanges,)),
                pltpu.SemaphoreType.DMA((2,)),
            ],
            compiler_params=pltpu.CompilerParams(
                collective_id=0, has_side_effects=True, vmem_limit_bytes=67043328
            ),
            name="schur",
        )(pressure, wind)

    in_specs = (P("gx", "gy", "gz"), P(None, "gx", "gy", "gz"))
    return jax.shard_map(
        body, mesh=mesh, in_specs=in_specs, out_specs=P("gx", "gy", "gz"), check_vma=False
    )
```

```python
import functools

import jax
import jax.numpy as jnp
from jax import lax
from jax.experimental import pallas as pl
from jax.experimental.pallas import tpu as pltpu
from jax.sharding import PartitionSpec as P

MESH = pl.DeviceIdType.MESH
AXES = ("gx", "gy", "gz")
BX, BY, BZ = 12, 16, 128
OMEGA = 0.8
KEEP = 1.0 - OMEGA
SIXTH = OMEGA / 6.0

AROUND = [
    (dx, dy, dz)
    for dz in (0, 1, -1)
    for dx in (0, 1, -1)
    for dy in (0, 1, -1)
    if (dx, dy, dz) != (0, 0, 0)
]
AROUND.sort(key=lambda d: -(abs(d[0]) + abs(d[1]) + abs(d[2])))

NEAR = [d for d in AROUND if sum(map(abs, d)) <= 2]


def coarse_offsets(far_edges):
    out = []
    for dx in range(-2, 3):
        for dy in range(-2, 3):
            for dz in (-1, 0, 1):
                shape = (abs(dx), abs(dy), abs(dz))
                if shape[:2] in ((0, 0), (0, 1), (1, 0), (1, 1), (0, 2), (2, 0), (2, 1)):
                    keep = shape != (0, 0, 0)
                else:
                    keep = far_edges and shape[:2] == (1, 2)
                if keep:
                    out.append((dx, dy, dz))
    return sorted(out, key=lambda d: -sum(map(abs, d)))


COARSE = (coarse_offsets(True), coarse_offsets(False))
GREETED = AROUND


def part(delta, count, width):
    if delta == 0:
        return 0, 0, count
    if delta > 0:
        return count - width, -width, width
    return 0, count, width


class Place:
    def __init__(self, sizes):
        self.sizes = sizes
        self.at = [lax.axis_index(a) for a in AXES]
        self.has = []
        for g, n in zip(self.at, sizes):
            self.has.append({d: (g + d >= 0) & (g + d < n) for d in (-2, -1, 1, 2)})

        kinds = []
        for n in sizes:
            kinds.append(sorted({
                tuple(sum(0 <= g + d < n for d in (-k, k)) for k in (1, 2)) for g in range(n)
            }))
        self.profiles = [(a, b, c) for a in kinds[0] for b in kinds[1] for c in kinds[2]]
        self.kinds = kinds
        self.counts = [
            [t[-k].astype(jnp.int32) + t[k].astype(jnp.int32) for k in (1, 2)] for t in self.has
        ]

    def matches(self, profile):
        found = None
        for counts, wanted, kinds in zip(self.counts, profile, self.kinds):
            for c, v, seen in zip(counts, wanted, zip(*kinds)):
                if len(set(seen)) > 1:
                    found = (c == v) if found is None else found & (c == v)
        return True if found is None else found

    def exists(self, offset):
        found = None
        for table, d in zip(self.has, offset):
            if d:
                found = table[d] if found is None else found & table[d]
        return found

    def device(self, offset):
        return tuple(
            lax.rem(g + (d + n), n) if d else g for g, d, n in zip(self.at, offset, self.sizes)
        )


class Exchange:
    def __init__(self, place, copies, send_sem, recv_sem, ruler):
        self.place, self.items = place, []
        self.send_sem, self.recv_sem, self.ruler = send_sem, recv_sem, ruler
        self.weights = []
        for offset, src, dst in copies:
            copy = pltpu.make_async_remote_copy(
                src_ref=src,
                dst_ref=dst,
                send_sem=send_sem,
                recv_sem=recv_sem,
                device_id=place.device(offset),
                device_id_type=MESH,
            )
            self.items.append((offset, copy))
            units = 1
            for n in src.shape:
                units *= n
            self.weights.append((tuple(abs(d) for d in offset), units // 512))

    def start(self):
        for offset, copy in self.items:
            pl.when(self.place.exists(offset))(copy.start)

    def wait(self, sem):
        for profile in self.place.profiles:
            total = 0
            for shape, units in self.weights:
                share = 8 * units
                for counts, d in zip(profile, shape):
                    share = share * counts[d - 1] // 2 if d else share
                total += share
            total //= 8
            if total:
                rows = self.ruler.at[pl.ds(0, total)]
                pl.when(self.place.matches(profile))(pltpu.make_async_copy(rows, rows, sem).wait)

    def wait_recv(self):
        self.wait(self.recv_sem)

    def wait_send(self):
        self.wait(self.send_sem)


def lanes(rows):
    return lax.broadcasted_iota(jnp.int32, (rows, 128), 1)


def row_mask(place, first_row, rows, extent):
    y = first_row + lax.broadcasted_iota(jnp.int32, (rows, 128), 0)
    low = jnp.where(place.has[1][-1], -64, 0)
    high = jnp.where(place.has[1][1], 64, extent)
    return (y >= low) & (y < high)


def rim_lanes(place, rows, start, right_end):
    lane = lanes(rows)
    right_stop = jnp.where(place.has[2][1], right_end, 0)
    left_start = jnp.where(place.has[2][-1], 120, 128)
    return ((lane >= start) & (lane < right_stop)) | (lane >= left_start)


def slab_weight(place, x, extent):
    if x < 0:
        return place.has[0][-1].astype(jnp.float32)
    if x >= extent:
        return place.has[0][1].astype(jnp.float32)
    return None


def z_back(a, h):
    lane0 = lanes(a.shape[0]) == 0
    ra, rh = pltpu.roll(a, 1, 1), pltpu.roll(h, 1, 1)
    return jnp.where(lane0, rh, ra), jnp.where(lane0, ra, rh)


def z_next(a, h):
    lane127 = lanes(a.shape[0]) == 127
    ra, rh = pltpu.roll(a, 127, 1), pltpu.roll(h, 127, 1)
    return jnp.where(lane127, rh, ra), jnp.where(lane127, ra, rh)


def masks0(place, first_row, rows):
    inner = row_mask(place, first_row, rows, BY)
    rim = inner & rim_lanes(place, rows, 0, 8)
    return inner.astype(jnp.float32), rim.astype(jnp.float32)


def scaled(value, mask, weight):
    value = value * mask
    return value if weight is None else value * weight


def six0(ref, i, r, n, rim=True):
    a, h = ref[0, i, r : r + n, :], ref[1, i, r : r + n, :]
    ba, bh = z_back(a, h)
    na, nh = z_next(a, h)
    out = []
    for t, (c, b, f) in enumerate(((a, ba, na), (h, bh, nh))):
        if t and not rim:
            break
        s = (
            (ref[t, i - 1, r : r + n, :] + ref[t, i + 1, r : r + n, :])
            + (ref[t, i, r - 1 : r - 1 + n, :] + ref[t, i, r + 1 : r + 1 + n, :])
            + (b + f)
        )
        out.append((c, s))
    return out


def six1(ref, i, r, n):
    c = ref[i, r : r + n, :]
    s = (
        (ref[i - 1, r : r + n, :] + ref[i + 1, r : r + n, :])
        + (ref[i, r - 1 : r - 1 + n, :] + ref[i, r + 1 : r + 1 + n, :])
        + (pltpu.roll(c, 1, 1) + pltpu.roll(c, 127, 1))
    )
    return c, s


def pick(a, m):
    high = a.astype(jnp.bfloat16)
    low = (a - high.astype(jnp.float32)).astype(jnp.bfloat16)
    return jnp.dot(high, m, preferred_element_type=jnp.float32) + jnp.dot(
        low, m, preferred_element_type=jnp.float32
    )


def turn(value, shift):
    shift %= 128
    return pltpu.roll(value, shift, 1) if shift else value


def pack0(load, store, count=BX):
    lane = lanes(BY)
    first = jnp.zeros((BY, 128), jnp.float32)
    last = jnp.zeros((BY, 128), jnp.float32)
    for i in range(count):
        turned = turn(load(i), 8 * i)
        first = jnp.where((lane >= 8 * i) & (lane < 8 * i + 8), turned, first)
        at = (8 * i - 8) % 128
        last = jnp.where((lane >= at) & (lane < at + 8), turned, last)
    store(first, last)


def beside(x, count):
    return (0, x) if 0 <= x < count else ((-1, x + count) if x < 0 else (1, x - count))


def unpack0(land, x, rows):
    dx, i = beside(x, BX)
    return unpack_columns(land[0, dx + 1], land[1, dx + 1], i, rows)


def unpack_columns(left, right, i, rows):
    left, right = turn(left, -8 * i), turn(right, -8 * i)
    lane = lanes(rows)
    return jnp.where(lane < 8, right, jnp.where(lane >= 120, left, 0.0))


def rim_copies(source, land, offsets):
    out = []
    for offset in offsets:
        dx, dy, dz = offset
        if dz == 0:
            continue
        y0, yd, ny = part(dy, BY, 8)
        side = 0 if dz > 0 else 1
        out.append((offset, source(side, y0, ny), land(side, 1 - dx, yd, ny)))
    return out


def block_copies(source, land, reach, offsets, edge=None):
    out = []
    for offset in offsets:
        dx, dy, dz = offset
        if dz != 0:
            continue
        near, far = edge if edge and dy else reach
        if dx == 0:
            x0, xd, nx = 0, 0, BX
        elif dx > 0:
            x0, xd, nx = BX - far, -far, far - near + 1
        else:
            x0, xd, nx = near - 1, BX + near - 1, far - near + 1
        y0, yd, ny = part(dy, BY, 8)
        out.append((offset, source(x0, nx, y0, ny), land(xd, nx, yd, ny)))
    return out


def ordered(copies):
    return sorted(copies, key=lambda c: -sum(abs(d) for d in c[0]))


def clear_around(ref, lead_x, lead_y, count_y):
    nx, ny = ref.shape[0], ref.shape[1]
    ref[0:lead_x] = jnp.zeros((lead_x, ny, 128), jnp.float32)
    ref[lead_x + BX : nx] = jnp.zeros((nx - lead_x - BX, ny, 128), jnp.float32)
    ref[lead_x : lead_x + BX, 0:lead_y, :] = jnp.zeros((BX, lead_y, 128), jnp.float32)
    end = lead_y + count_y
    ref[lead_x : lead_x + BX, end:ny, :] = jnp.zeros((BX, ny - end, 128), jnp.float32)


def clear(*refs):
    for ref in refs:
        ref[...] = jnp.zeros(ref.shape, ref.dtype)


def kernel(
    sizes, p_ref, w_ref, out_ref,
    b0, far, sb, v0, t0, zs0, zr0, wind, zsw, zrw, zsx, zrx, coef, velocity, flux,
    vp, zsv, zrv,
    bv, zsb, zrb, s1, l1, l1_far, zs1, zr1, zr1_far, b1, v1, t1,
    gathered, merged, c2, e2a, e2b,
    rows0, rows2, up1, up0, m_down0, m_down1, m_up1, m_up0,
    ruler, send_sems, recv_sems, load_sems,
):
    place = Place(sizes)
    load_p = pltpu.make_async_copy(
        p_ref, b0.at[0, pl.ds(8, BX), pl.ds(16, BY), :], load_sems.at[0])
    load_w = pltpu.make_async_copy(
        w_ref, wind.at[:, 0, pl.ds(3, BX), pl.ds(8, BY), :], load_sems.at[1])
    load_p.start()
    load_w.start()

    clear_around(b0.at[0], 8, 16, BY)
    for d in range(3):
        clear_around(wind.at[d, 0], 3, 8, BY)
    clear(far, zr0, zrw, zrx, vp, zrv, bv, zrb, l1, l1_far, zr1, zr1_far, gathered)

    barrier = pltpu.get_barrier_semaphore()
    total = jnp.int32(0)
    for offset in GREETED:
        there = place.exists(offset)
        total = total + there.astype(jnp.int32)

        def greet(offset=offset):
            pl.semaphore_signal(
                barrier, inc=1, device_id=place.device(offset), device_id_type=MESH
            )

        pl.when(there)(greet)

    def storer(ref):
        def store(f, l):
            ref[0] = l
            ref[1] = f
        return store

    clear(b0.at[1], v0, t0, rows0)
    load_p.wait()
    pack0(lambda i: b0[0, 8 + i, 16:32, :], storer(zs0))

    used = [0]

    def exchange(copies):
        k = used[0]
        used[0] += 1
        return Exchange(place, ordered(copies), send_sems.at[k], recv_sems.at[k], ruler)

    def far_block(x, nx, y, ny):
        side, lead = (0, 8) if x < 0 else (1, -BX - 5)
        return far.at[side, pl.ds(x + lead, nx), pl.ds(y + 16, ny), :]

    def b0_block(x, nx, y, ny):
        return b0.at[0, pl.ds(x + 8, nx), pl.ds(y + 16, ny), :]

    def wind_block(x, nx, y, ny):
        return wind.at[:, 0, pl.ds(x + 3, nx), pl.ds(y + 8, ny), :]

    def vp_block(x, nx, y, ny):
        return vp.at[pl.ds(x + 2, nx), pl.ds(y + 16, ny), :]

    def wind_side_copies():
        out = []
        for offset in AROUND:
            dx, dy, dz = offset
            if dx and dz:
                y0, yd, ny = part(dy, BY, 8)
                side = 0 if dz > 0 else 1
                out.append((
                    offset, zsx.at[side, (dx + 1) // 2, pl.ds(y0, ny), :],
                    zrx.at[side, (1 - dx) // 2, pl.ds(yd + 8, ny), :]))
        return out

    ex0 = exchange(
        block_copies(b0_block, b0_block, (1, 6), AROUND, (1, 5))
        + rim_copies(
            lambda s, y, ny: zs0.at[s, pl.ds(y, ny), :],
            lambda s, dx, y, ny: zr0.at[s, dx, pl.ds(y + 8, ny), :], AROUND))
    sides = [d for d in AROUND if d[0]]
    ex_far = exchange(
        block_copies(b0_block, far_block, (7, 8), [d for d in sides if d[2] == 0], (6, 7)))
    exw = exchange(
        block_copies(wind_block, wind_block, (1, 3), AROUND, (1, 2))
        + rim_copies(
            lambda s, y, ny: zsw.at[s, :, pl.ds(y, ny), :],
            lambda s, dx, y, ny: zrw.at[s, :, pl.ds(y + 8, ny), :],
            [d for d in AROUND if not d[0]])
        + wind_side_copies())
    exv = exchange(
        block_copies(vp_block, vp_block, (1, 2), NEAR, (1, 1))
        + rim_copies(
            lambda s, y, ny: zsv.at[s, pl.ds(y, ny), :],
            lambda s, dx, y, ny: zrv.at[s, dx, pl.ds(y + 8, ny), :], NEAR))

    def bv_copies():
        out = []
        for offset in AROUND:
            dx, dy, dz = offset
            if dz == 0:
                out.append((
                    offset, bv.at[pl.ds(6, 6), pl.ds(16, 8), :],
                    bv.at[pl.ds(6 - 6 * dx, 6), pl.ds(16 - 8 * dy, 8), :]))
            else:
                side = 0 if dz > 0 else 1
                out.append((
                    offset, zsb.at[side], zrb.at[side, 1 - dx, pl.ds(8 - 8 * dy, 8), :]))
        return out

    def level1_copies(reach, edge, offsets, blocks, rims):
        out = []
        for offset in offsets:
            dx, dy, dz = offset
            if dz == 0:
                near, far_end = edge if dx and dy else reach
                if dx == 0:
                    x0, xd, nx = 0, 0, 6
                elif dx > 0:
                    x0, xd, nx = 6 - far_end, -far_end, far_end - near + 1
                else:
                    x0, xd, nx = near - 1, 5 + near, far_end - near + 1
                out.append((
                    offset, s1.at[pl.ds(x0, nx)],
                    blocks.at[pl.ds(xd + 4, nx), pl.ds(8 - 8 * dy, 8), :]))
            else:
                side = 0 if dz > 0 else 1
                out.append((
                    offset, zs1.at[side], rims.at[side, 1 - dx, pl.ds(8 - 8 * dy, 8), :]))
        return out

    def coarse_copies(number):
        return [
            (d, gathered.at[number, 2, 1, 2], gathered.at[number, 2 - d[1], 1 - d[2], 2 - d[0]])
            for d in COARSE[number]
        ]

    exb = exchange(bv_copies())
    ex1 = exchange(level1_copies((1, 2), (1, 1), NEAR, l1, zr1))
    ex1_far = exchange(level1_copies(
        (3, 4), (2, 3), [d for d in AROUND if d[0] and (d[2] == 0 or d[1])], l1_far, zr1_far))
    ex2 = [exchange(coarse_copies(0)), exchange(coarse_copies(1))]

    pl.semaphore_wait(barrier, total)
    ex0.start()
    ex_far.start()

    load_w.wait()
    for d in range(3):
        pack0(lambda i: wind[d, 0, 3 + i, 8:24, :], storer(zsw.at[:, d]))
    for high, lead in ((0, 3), (1, BX)):
        pack0(lambda i: wind[i // 3, 0, lead + i % 3, 8:24, :], storer(zsx.at[:, high]), 9)
    exw.start()

    clear(velocity, flux, sb, b1, v1, t1, merged, c2, e2a, e2b, rows2, up1, up0)

    bf16 = jnp.bfloat16
    k = lax.broadcasted_iota(jnp.int32, (128, 128), 0)
    l = lax.broadcasted_iota(jnp.int32, (128, 128), 1)
    eighth = jnp.float32(0.125)
    m_down0[0:128, :] = jnp.where(k // 2 == l, eighth, 0.0).astype(bf16)
    m_down0[128:256, :] = jnp.where(
        ((k < 8) | (k >= 120)) & (k // 2 + 64 == l), eighth, 0.0).astype(bf16)
    for i in range(3):
        m_down1[i * 128 : i * 128 + 128, :] = jnp.where(
            (l // 32 == i) & (k // 2 == l % 32), eighth, 0.0).astype(bf16)
    m_up1[...] = jnp.where(
        ((l < 72) & (k == l // 2)) | ((l >= 120) & (k == 64 + l // 2)), 1.0, 0.0).astype(bf16)
    m_up0[:, 0:128] = jnp.where(k == l // 2, 1.0, 0.0).astype(bf16)
    m_up0[:, 128:256] = jnp.where(
        ((l < 8) | (l >= 120)) & (k == 64 + l // 2), 1.0, 0.0).astype(bf16)

    c0 = OMEGA / 6.0
    w1 = 0.25
    c1 = OMEGA / (6.0 * w1)
    w2 = 0.0625
    c2s = OMEGA / (6.0 * w2)
    lane8, lane16, lane24, lane40 = lanes(8), lanes(16), lanes(24), lanes(40)
    m32a, m32h = masks0(place, -8, 32)
    m24a, m24h = masks0(place, -4, 24)
    mask32, mask24 = (m32a, m32h), (m24a, m24h)

    def level1_mask(first_row, rows):
        lane = lanes(rows)
        inside = row_mask(place, first_row, rows, 8)
        return (inside & ((lane < 64) | rim_lanes(place, rows, 64, 72))).astype(jnp.float32)

    def scaled_masks(masks, factor, weight):
        factor = factor if weight is None else factor * weight
        return [m * factor for m in masks]

    def sweep0(target, iterate, x, r, n, masks):
        weight = slab_weight(place, x, BX)
        keep, share = scaled_masks(masks, KEEP, weight), scaled_masks(masks, SIXTH, weight)
        for t, (c, s) in enumerate(six0(iterate, x + 8, r, n)):
            target[t, x + 8, r : r + n, :] = keep[t] * c + share[t] * s + sb[t, x + 8, r : r + n, :]

    def scale_source(x, r, n, masks):
        factor = scaled_masks(masks, c0, slab_weight(place, x, BX))
        for t in range(2):
            sb[t, x + 8, r : r + n, :] = factor[t] * b0[t, x + 8, r : r + n, :]

    def first_two0(slabs, r, n, masks):
        for x in slabs:
            factors = scaled_masks(masks, c0, slab_weight(place, x, BX))
            for t, (c, s) in enumerate(six0(b0, x + 8, r, n)):
                v0[t, x + 8, r : r + n, :] = factors[t] * ((1.0 + KEEP) * c + SIXTH * s)

    def down1_and_send(number, r, n):
        pairs = []
        for i in range(3):
            pair = None
            for x in (2 * i, 2 * i + 1):
                c, s = six1(v1, x + 6, 16, 8)
                res = b1[x + 6, 16:24, :] - w1 * (6.0 * c - s)
                pair = res if pair is None else pair + res
            pairs.append(jnp.where(lane8 < 64, pair, 0.0))
        rows2[...] = pick(jnp.concatenate(pairs, axis=1), m_down1[...])
        gathered[number, 2, 1, 2] = (
            rows2[pl.ds(0, 4, stride=2), :] + rows2[pl.ds(1, 4, stride=2), :])
        ex2[number].start()

    def coarse(number, reach):
        for az in range(3):
            for ax in range(5):
                for ay in range(5):
                    merged[az, ax, 4 * ay : 4 * ay + 4, :] = gathered[number, ay, az, ax]
        for x in range(-reach - 3, 3 + reach + 3):
            ax, i = (x + 6) // 3, (x + 6) % 3
            left = turn(merged[0, ax], 96 - 32 * i)
            own = turn(merged[1, ax], -32 * i)
            right = turn(merged[2, ax], 32 - 32 * i)
            c2[x + 6] = jnp.where(
                lane24 < 32, own, jnp.where(lane24 < 40, right, jnp.where(lane24 >= 120, left, 0.0)))
        inside = row_mask(place, -6, 16, 4)
        mask2 = (inside & ((lane16 < 32) | rim_lanes(place, 16, 32, 40))).astype(jnp.float32)
        for x in range(-reach - 2, 3 + reach + 2):
            c, s = six1(c2, x + 6, 2, 16)
            value = (1.0 + KEEP) * c2s * c + SIXTH * c2s * s
            e2a[x + 6, 2:18, :] = scaled(value, mask2, slab_weight(place, x, 3))
        here, there = e2a, e2b
        for more in (1, 0):
            for x in range(-reach - more, 3 + reach + more):
                c, s = six1(here, x + 6, 2, 16)
                value = KEEP * c + SIXTH * s + c2s * c2[x + 6, 2:18, :]
                there[x + 6, 2:18, :] = scaled(value, mask2, slab_weight(place, x, 3))
            here, there = there, here
        return here

    def spread1(here, reach, y, n):
        slabs = 3 + 2 * reach
        spread = pick(
            jnp.concatenate([here[x - reach + 6, y + 8 : y + 8 + n, :] for x in range(slabs)], axis=0),
            m_up1[...])
        for j in range(slabs):
            value = spread[n * j : n * j + n, :]
            up1[j, pl.ds(0, n, stride=2), :] = value
            up1[j, pl.ds(1, n, stride=2), :] = value

    def last_two1(reach, r, n, mask):
        for x in range(-reach - 1, 6 + reach + 1):
            c, s = six1(v1, x + 6, r, n)
            value = KEEP * c + SIXTH * s + c1 * b1[x + 6, r : r + n, :]
            t1[x + 6, r : r + n, :] = scaled(value, mask, slab_weight(place, x, 6))
        for x in range(-reach, 6 + reach):
            c, s = six1(t1, x + 6, r, n)
            value = KEEP * c + SIXTH * s + c1 * b1[x + 6, r : r + n, :]
            v1[x + 6, r : r + n, :] = scaled(value, mask, slab_weight(place, x, 6))

    def spread0(reach, n):
        y = -(n - 8) // 2
        slabs = 6 + 2 * reach
        spread = pick(
            jnp.concatenate(
                [v1[x - reach + 6, y + 16 : y + 32, :] for x in range(slabs)], axis=0),
            m_up0[...])
        for j in range(slabs):
            for t in range(2):
                value = spread[16 * j : 16 * j + n, 128 * t : 128 * t + 128]
                up0[t, j, pl.ds(0, n, stride=2), :] = value
                up0[t, j, pl.ds(1, n, stride=2), :] = value

    ex0.wait_recv()
    for x in range(-8, BX + 8):
        b0[1, x + 8, 8:40, :] = unpack0(zr0, x, 32)
    first_two0(range(-5, BX + 5), 8, 32, mask32)
    for i in range(10):
        pair = [None, None]
        for x in (2 * i - 4, 2 * i - 3):
            for t, (c, s) in enumerate(six0(v0, x + 8, 12, 24)):
                res = b0[t, x + 8, 12:36, :] - (6.0 * c - s)
                pair[t] = res if pair[t] is None else pair[t] + res
        for t in range(2):
            rows0[t, i, 0:24, :] = pair[t]
    cells = [
        jnp.concatenate(
            [rows0[t, i, pl.ds(0, 16, stride=2), :] + rows0[t, i, pl.ds(1, 16, stride=2), :]
             for t in range(2)], axis=1)
        for i in range(10)
    ]
    source = pick(jnp.concatenate(cells, axis=0), m_down0[...])
    mask = level1_mask(-2, 16)
    for x in range(-2, 8):
        b1[x + 6, 14:30, :] = scaled(
            source[16 * (x + 2) : 16 * (x + 2) + 16, :], mask, slab_weight(place, x, 6))
    for x in range(-1, 7):
        c, s = six1(b1, x + 6, 14, 16)
        value = (1.0 + KEEP) * c1 * c + SIXTH * c1 * s
        v1[x + 6, 14:30, :] = scaled(value, mask, slab_weight(place, x, 6))
    down1_and_send(0, 14, 16)

    low = jnp.zeros((8, 128), jnp.float32)
    high = jnp.zeros((8, 128), jnp.float32)
    for i in range(6):
        block_b, block_v = b1[i + 6, 16:24, :], v1[i + 6, 16:24, :]
        bv[i + 6, 16:24, :] = jnp.where(lane8 < 64, block_b, pltpu.roll(block_v, 64, 1))
        for block, lead in ((block_b, 0), (block_v, 64)):
            group = (lane8 >= lead + 8 * i) & (lane8 < lead + 8 * i + 8)
            low = jnp.where(group, turn(block, lead + 8 * i), low)
            high = jnp.where(group, turn(block, lead + 8 * i - 56), high)
    zsb[0] = high
    zsb[1] = low
    exb.start()
    ex0.wait_send()
    ex_far.wait_recv()
    for side in range(2):
        for k in range(3):
            x = k - 8 if side == 0 else BX + 5 + k
            distance = -x if side == 0 else x - BX + 1
            if distance > 6:
                b0[0, x + 8, 16:32, :] = far[side, k, 16:32, :]
            if distance < 8:
                for r in (8, 32):
                    b0[0, x + 8, r : r + 8, :] = far[side, k, r : r + 8, :]
    first_two0((-7, -6, -5, BX + 4, BX + 5, BX + 6), 8, 32, mask32)
    for x in range(-6, BX + 6):
        scale_source(x, 8, 32, mask32)
    ex_far.wait_send()
    exw.wait_recv()
    for x in range(-3, BX + 3):
        ones = scaled_masks(mask24, 1.0, slab_weight(place, x, BX))
        halves = scaled_masks(mask24, 0.5, slab_weight(place, x, BX))
        for d in range(3):
            if 0 <= x < BX:
                rim = unpack_columns(zrw[0, d, 4:28, :], zrw[1, d, 4:28, :], x, 24)
            else:
                high, i = (0, x + 3) if x < 0 else (1, x - BX)
                rim = unpack_columns(
                    zrx[0, high, 4:28, :], zrx[1, high, 4:28, :], 3 * d + i, 24)
            for t, w in enumerate((wind[d, 0, x + 3, 4:28, :], rim)):
                half = halves[t] * w
                coef[d, 0, t, x + 3] = half - ones[t]
                coef[d, 1, t, x + 3] = -half - ones[t]
    exw.wait_send()
    ex2[0].wait_recv()
    here = coarse(0, 3)
    spread1(here, 3, -4, 16)
    exb.wait_recv()
    mask = level1_mask(-8, 24)
    for x in range(-6, 12):
        dx, i = beside(x, 6)
        near = bv[x + 6, 8:32, :]
        left, right = zrb[0, dx + 1], zrb[1, dx + 1]
        for lead, ref in ((0, b1), (64, v1)):
            value = jnp.where(
                lane24 < 64, turn(near, -lead),
                jnp.where(lane24 < 72, turn(right, 64 - 8 * i - lead),
                          jnp.where(lane24 >= 120, turn(left, 120 - 8 * i - lead), 0.0)))
            if ref is v1:
                value = value + up1[(x + 6) // 2, 0:24, :]
            ref[x + 6, 8:32, :] = value
    last_two1(4, 8, 24, mask)
    spread0(4, 16)
    for x in range(-7, BX + 7):
        for t in range(2):
            v0[t, x + 8, 8:40, :] += up0[t, (x + 8) // 2]
    for reach, target, iterate in ((6, t0, v0), (5, v0, t0)):
        for x in range(-reach, BX + reach):
            away = max(-x, x - BX + 1, 0)
            if reach - away <= 4:
                sweep0(target, iterate, x, 12, 24, mask24)
            else:
                sweep0(target, iterate, x, 8, 32, mask32)
    first = v0

    for x in range(-4, BX + 4):
        weight = slab_weight(place, x, BX)
        half = 0.5 if weight is None else 0.5 * weight
        i = x + 8
        a, h = first[0, i, 12:36, :], first[1, i, 12:36, :]
        ba, bh = z_back(a, h)
        na, nh = z_next(a, h)
        for t, (b, n) in enumerate(((ba, na), (bh, nh))):
            m = mask24[t] * half
            velocity[0, t, x + 4, 12:36, :] = (first[t, i + 1, 12:36, :] - first[t, i - 1, 12:36, :]) * m
            velocity[1, t, x + 4, 12:36, :] = (first[t, i, 13:37, :] - first[t, i, 11:35, :]) * m
            velocity[2, t, x + 4, 12:36, :] = (n - b) * m
    for x in range(-3, BX + 3):
        weight = slab_weight(place, x, BX)
        i = x + 4
        sevens = scaled_masks(mask24, 7.0, weight)
        ways = [[[coef[e, k, t, x + 3] for k in range(2)] for e in range(3)] for t in range(2)]
        for d in range(3):
            u = velocity.at[d]
            a, h = u[0, i, 12:36, :], u[1, i, 12:36, :]
            ba, bh = z_back(a, h)
            na, nh = z_next(a, h)
            for t, (c, b, n) in enumerate(((a, ba, na), (h, bh, nh))):
                x_low, x_high = u[t, i - 1, 12:36, :], u[t, i + 1, 12:36, :]
                y_low, y_high = u[t, i, 11:35, :], u[t, i, 13:37, :]
                along_x, along_y, along_z = ways[t]
                flux[d, t, x + 3, 4:28, :] = (
                    sevens[t] * c
                    + (along_x[0] * x_high + along_x[1] * x_low)
                    + (along_y[0] * y_high + along_y[1] * y_low)
                    + (along_z[0] * n + along_z[1] * b)
                )
    for x in range(-2, BX + 2):
        halves = scaled_masks(mask24, -0.5, slab_weight(place, x, BX))
        i = x + 3
        a, h = flux[2, 0, i, 4:28, :], flux[2, 1, i, 4:28, :]
        ba, bh = z_back(a, h)
        na, nh = z_next(a, h)
        for t, (b, n) in enumerate(((ba, na), (bh, nh))):
            value = (
                (flux[0, t, i + 1, 4:28, :] - flux[0, t, i - 1, 4:28, :])
                + (flux[1, t, i, 5:29, :] - flux[1, t, i, 3:27, :])
                + (n - b)
            )
            b0[t, x + 8, 12:36, :] = value * halves[t]

    first_two0(range(-1, BX + 1), 12, 24, mask24)
    for i in range(6):
        pair = None
        for x in (2 * i, 2 * i + 1):
            ((c, s),) = six0(v0, x + 8, 16, 16, rim=False)
            res = b0[0, x + 8, 16:32, :] - (6.0 * c - s)
            pair = res if pair is None else pair + res
        rows0[0, i, 0:16, :] = pair
    cells = [rows0[0, i, pl.ds(0, 8, stride=2), :] + rows0[0, i, pl.ds(1, 8, stride=2), :] for i in range(6)]
    source = pick(jnp.concatenate(cells, axis=0), m_down0[0:128, :])
    low = jnp.zeros((8, 128), jnp.float32)
    high = jnp.zeros((8, 128), jnp.float32)
    for i in range(6):
        block = source[8 * i : 8 * i + 8, :]
        s1[i] = block
        l1[4 + i, 8:16, :] = block
        group = (lane8 >= 8 * i) & (lane8 < 8 * i + 8)
        low = jnp.where(group, turn(block, 8 * i), low)
        high = jnp.where(group, turn(block, 8 * i - 56), high)
    zs1[0] = high
    zs1[1] = low
    ex1.start()
    ex1_far.start()
    for x in range(BX):
        vp[x + 2, 16:32, :] = v0[0, x + 8, 16:32, :]
    pack0(lambda i: v0[0, 8 + i, 16:32, :], storer(zsv))
    exv.start()
    ex2[0].wait_send()
    exb.wait_send()
    ex1.wait_recv()
    mask = level1_mask(-4, 16)

    def source1(slabs, block, rim):
        for x in slabs:
            dx, i = beside(x, 6)
            b1[x + 6, 8:32, :] = jnp.where(
                lane24 < 64, block(x + 4),
                jnp.where(lane24 < 72, turn(rim(1, dx + 1), 64 - 8 * i),
                          jnp.where(lane24 >= 120, turn(rim(0, dx + 1), 120 - 8 * i), 0.0)))

    def first_two1(reach):
        for x in range(-reach, 6 + reach):
            factors = scaled_masks((mask,), c1, slab_weight(place, x, 6))
            c, s = six1(b1, x + 6, 12, 16)
            v1[x + 6, 12:28, :] = factors[0] * ((1.0 + KEEP) * c + SIXTH * s)

    source1(range(-2, 8), lambda k: l1[k], lambda side, k: zr1[side, k])
    first_two1(1)
    down1_and_send(1, 12, 16)
    ex1_far.wait_recv()
    source1(
        range(-4, 10), lambda k: l1[k] + l1_far[k],
        lambda side, k: zr1[side, k] + zr1_far[side, k])
    first_two1(3)
    ex1.wait_send()
    ex1_far.wait_send()
    exv.wait_send()
    exv.wait_recv()
    for x in range(-1, BX + 1):
        scale_source(x, 12, 24, mask24)
    for x in range(-2, BX + 2):
        v0[0, x + 8, 12:36, :] = vp[x + 2, 12:36, :]
        v0[1, x + 8, 8:40, :] = unpack0(zrv, x, 32)
    ex2[1].wait_recv()
    here = coarse(1, 2)
    spread1(here, 2, -2, 8)
    for x in range(-3, 9):
        v1[x + 6, 12:28, :] += up1[(x + 4) // 2, 0:16, :]
    last_two1(1, 12, 16, mask)
    spread0(1, 12)
    for x in range(-2, BX + 2):
        for t in range(2):
            v0[t, x + 8, 12:36, :] += up0[t, (x + 2) // 2, 0:24, :]
    for x in range(-1, BX + 1):
        sweep0(t0, v0, x, 12, 24, mask24)
    for x in range(BX):
        ((c, s),) = six0(t0, x + 8, 16, 16, rim=False)
        out_ref[x] = KEEP * c + SIXTH * s + sb[0, x + 8, 16:32, :]
    ex2[1].wait_send()


def solution(mesh):
    sizes = tuple(mesh.shape[a] for a in AXES)
    exchanges = 9
    f32 = jnp.float32
    bf16 = jnp.bfloat16

    def vmem(*shape, dtype=f32):
        return pltpu.VMEM(shape, dtype)

    def body(pressure, wind):
        return pl.pallas_call(
            functools.partial(kernel, sizes),
            out_shape=jax.ShapeDtypeStruct((BX, BY, BZ), f32),
            in_specs=[pl.BlockSpec(memory_space=pl.ANY)] * 2,
            out_specs=pl.BlockSpec(memory_space=pltpu.VMEM),
            scratch_shapes=[
                vmem(2, 28, 48, 128),
                vmem(2, 3, 48, 128),
                vmem(2, 28, 48, 128),
                vmem(2, 28, 48, 128),
                vmem(2, 28, 48, 128),
                vmem(2, 16, 128),
                vmem(2, 3, 32, 128),
                vmem(3, 1, 18, 32, 128),
                vmem(2, 3, 16, 128),
                vmem(2, 3, 32, 128),
                vmem(2, 2, 16, 128),
                vmem(2, 2, 32, 128),
                vmem(3, 2, 2, 18, 24, 128),
                vmem(3, 2, 20, 48, 128),
                vmem(3, 2, 18, 32, 128),
                vmem(16, 48, 128),
                vmem(2, 16, 128),
                vmem(2, 3, 32, 128),
                vmem(18, 40, 128),
                vmem(2, 8, 128),
                vmem(2, 3, 24, 128),
                vmem(6, 8, 128),
                vmem(14, 24, 128),
                vmem(14, 24, 128),
                vmem(2, 8, 128),
                vmem(2, 3, 24, 128),
                vmem(2, 3, 24, 128),
                vmem(18, 40, 128),
                vmem(18, 40, 128),
                vmem(18, 40, 128),
                vmem(2, 5, 3, 5, 4, 128),
                vmem(3, 5, 24, 128),
                vmem(15, 24, 128),
                vmem(15, 24, 128),
                vmem(15, 24, 128),
                vmem(2, 10, 32, 128),
                vmem(8, 128),
                vmem(9, 32, 128),
                vmem(2, 14, 32, 128),
                vmem(256, 128, dtype=bf16),
                vmem(384, 128, dtype=bf16),
                vmem(128, 128, dtype=bf16),
                vmem(128, 256, dtype=bf16),
                vmem(512, 4, 128),
                pltpu.SemaphoreType.DMA((exchanges,)),
                pltpu.SemaphoreType.DMA((exchanges,)),
                pltpu.SemaphoreType.DMA((2,)),
            ],
            compiler_params=pltpu.CompilerParams(
                collective_id=0, has_side_effects=True, vmem_limit_bytes=56400000
            ),
            name="schur",
        )(pressure, wind)

    in_specs = (P("gx", "gy", "gz"), P(None, "gx", "gy", "gz"))
    return jax.shard_map(
        body, mesh=mesh, in_specs=in_specs, out_specs=P("gx", "gy", "gz"), check_vma=False
    )
```

```python
import functools

import jax
import jax.numpy as jnp
from jax import lax
from jax.experimental import pallas as pl
from jax.experimental.pallas import tpu as pltpu
from jax.sharding import PartitionSpec as P

MESH = pl.DeviceIdType.MESH
AXES = ("gx", "gy", "gz")
BX, BY, BZ = 12, 16, 128
OMEGA = 0.8
KEEP = 1.0 - OMEGA
SIXTH = OMEGA / 6.0

AROUND = [
    (dx, dy, dz)
    for dz in (0, 1, -1)
    for dx in (0, 1, -1)
    for dy in (0, 1, -1)
    if (dx, dy, dz) != (0, 0, 0)
]
AROUND.sort(key=lambda d: -(abs(d[0]) + abs(d[1]) + abs(d[2])))

NEAR = [d for d in AROUND if sum(map(abs, d)) <= 2]


def coarse_offsets(far_edges):
    out = []
    for dx in range(-2, 3):
        for dy in range(-2, 3):
            for dz in (-1, 0, 1):
                shape = (abs(dx), abs(dy), abs(dz))
                if shape[:2] in ((0, 0), (0, 1), (1, 0), (1, 1), (0, 2), (2, 0), (2, 1)):
                    keep = shape != (0, 0, 0)
                else:
                    keep = far_edges and shape[:2] == (1, 2)
                if keep:
                    out.append((dx, dy, dz))
    return sorted(out, key=lambda d: -sum(map(abs, d)))


COARSE = (coarse_offsets(True), coarse_offsets(False))
GREETED = AROUND


def part(delta, count, width):
    if delta == 0:
        return 0, 0, count
    if delta > 0:
        return count - width, -width, width
    return 0, count, width


class Place:
    def __init__(self, sizes):
        self.sizes = sizes
        self.at = [lax.axis_index(a) for a in AXES]
        self.has = []
        for g, n in zip(self.at, sizes):
            self.has.append({d: (g + d >= 0) & (g + d < n) for d in (-2, -1, 1, 2)})

        kinds = []
        for n in sizes:
            kinds.append(sorted({
                tuple(sum(0 <= g + d < n for d in (-k, k)) for k in (1, 2)) for g in range(n)
            }))
        self.profiles = [(a, b, c) for a in kinds[0] for b in kinds[1] for c in kinds[2]]
        self.kinds = kinds
        self.counts = [
            [t[-k].astype(jnp.int32) + t[k].astype(jnp.int32) for k in (1, 2)] for t in self.has
        ]

    def matches(self, profile):
        found = None
        for counts, wanted, kinds in zip(self.counts, profile, self.kinds):
            for c, v, seen in zip(counts, wanted, zip(*kinds)):
                if len(set(seen)) > 1:
                    found = (c == v) if found is None else found & (c == v)
        return True if found is None else found

    def exists(self, offset):
        found = None
        for table, d in zip(self.has, offset):
            if d:
                found = table[d] if found is None else found & table[d]
        return found

    def device(self, offset):
        return tuple(
            lax.rem(g + (d + n), n) if d else g for g, d, n in zip(self.at, offset, self.sizes)
        )


class Exchange:
    def __init__(self, place, copies, send_sem, recv_sem, ruler):
        self.place, self.items = place, []
        self.send_sem, self.recv_sem, self.ruler = send_sem, recv_sem, ruler
        self.weights = []
        for offset, src, dst in copies:
            copy = pltpu.make_async_remote_copy(
                src_ref=src,
                dst_ref=dst,
                send_sem=send_sem,
                recv_sem=recv_sem,
                device_id=place.device(offset),
                device_id_type=MESH,
            )
            self.items.append((offset, copy))
            units = 1
            for n in src.shape:
                units *= n
            self.weights.append((tuple(abs(d) for d in offset), units // 512))

    def start(self):
        for offset, copy in self.items:
            pl.when(self.place.exists(offset))(copy.start)

    def wait(self, sem):
        for profile in self.place.profiles:
            total = 0
            for shape, units in self.weights:
                share = 8 * units
                for counts, d in zip(profile, shape):
                    share = share * counts[d - 1] // 2 if d else share
                total += share
            total //= 8
            if total:
                rows = self.ruler.at[pl.ds(0, total)]
                pl.when(self.place.matches(profile))(pltpu.make_async_copy(rows, rows, sem).wait)

    def wait_recv(self):
        self.wait(self.recv_sem)

    def wait_send(self):
        self.wait(self.send_sem)


def lanes(rows):
    return lax.broadcasted_iota(jnp.int32, (rows, 128), 1)


def row_mask(place, first_row, rows, extent):
    y = first_row + lax.broadcasted_iota(jnp.int32, (rows, 128), 0)
    has = place.has[1]
    low = jnp.where(has[-2], -64, jnp.where(has[-1], -extent, 0))
    high = jnp.where(has[2], 64, jnp.where(has[1], 2 * extent, extent))
    return (y >= low) & (y < high)


def rim_lanes(place, rows, start, right_end):
    lane = lanes(rows)
    right_stop = jnp.where(place.has[2][1], right_end, 0)
    left_start = jnp.where(place.has[2][-1], 120, 128)
    return ((lane >= start) & (lane < right_stop)) | (lane >= left_start)


def slab_weight(place, x, extent):
    if 0 <= x < extent:
        return None
    return place.has[0][x // extent].astype(jnp.float32)


def z_back(a, h):
    lane0 = lanes(a.shape[0]) == 0
    ra, rh = pltpu.roll(a, 1, 1), pltpu.roll(h, 1, 1)
    return jnp.where(lane0, rh, ra), jnp.where(lane0, ra, rh)


def z_next(a, h):
    lane127 = lanes(a.shape[0]) == 127
    ra, rh = pltpu.roll(a, 127, 1), pltpu.roll(h, 127, 1)
    return jnp.where(lane127, rh, ra), jnp.where(lane127, ra, rh)


def masks0(place, first_row, rows):
    inner = row_mask(place, first_row, rows, BY)
    rim = inner & rim_lanes(place, rows, 0, 8)
    return inner.astype(jnp.float32), rim.astype(jnp.float32)


def scaled(value, mask, weight):
    value = value * mask
    return value if weight is None else value * weight


def six0(ref, i, r, n, rim=True):
    a, h = ref[0, i, r : r + n, :], ref[1, i, r : r + n, :]
    ba, bh = z_back(a, h)
    na, nh = z_next(a, h)
    out = []
    for t, (c, b, f) in enumerate(((a, ba, na), (h, bh, nh))):
        if t and not rim:
            break
        s = (
            (ref[t, i - 1, r : r + n, :] + ref[t, i + 1, r : r + n, :])
            + (ref[t, i, r - 1 : r - 1 + n, :] + ref[t, i, r + 1 : r + 1 + n, :])
            + (b + f)
        )
        out.append((c, s))
    return out


def six1(ref, i, r, n):
    c = ref[i, r : r + n, :]
    s = (
        (ref[i - 1, r : r + n, :] + ref[i + 1, r : r + n, :])
        + (ref[i, r - 1 : r - 1 + n, :] + ref[i, r + 1 : r + 1 + n, :])
        + (pltpu.roll(c, 1, 1) + pltpu.roll(c, 127, 1))
    )
    return c, s


def pick(a, m):
    high = a.astype(jnp.bfloat16)
    low = (a - high.astype(jnp.float32)).astype(jnp.bfloat16)
    return jnp.dot(high, m, preferred_element_type=jnp.float32) + jnp.dot(
        low, m, preferred_element_type=jnp.float32
    )


def turn(value, shift):
    shift %= 128
    return pltpu.roll(value, shift, 1) if shift else value


def pack0(load, store, count=BX):
    lane = lanes(BY)
    first = jnp.zeros((BY, 128), jnp.float32)
    last = jnp.zeros((BY, 128), jnp.float32)
    for i in range(count):
        turned = turn(load(i), 8 * i)
        first = jnp.where((lane >= 8 * i) & (lane < 8 * i + 8), turned, first)
        at = (8 * i - 8) % 128
        last = jnp.where((lane >= at) & (lane < at + 8), turned, last)
    store(first, last)


def beside(x, count):
    return (0, x) if 0 <= x < count else ((-1, x + count) if x < 0 else (1, x - count))


def unpack0(land, x, rows):
    dx, i = beside(x, BX)
    return unpack_columns(land[0, dx + 1], land[1, dx + 1], i, rows)


def unpack_columns(left, right, i, rows):
    left, right = turn(left, -8 * i), turn(right, -8 * i)
    lane = lanes(rows)
    return jnp.where(lane < 8, right, jnp.where(lane >= 120, left, 0.0))


def rim_copies(source, land, offsets):
    out = []
    for offset in offsets:
        dx, dy, dz = offset
        if dz == 0:
            continue
        y0, yd, ny = part(dy, BY, 8)
        side = 0 if dz > 0 else 1
        out.append((offset, source(side, y0, ny), land(side, 1 - dx, yd, ny)))
    return out


def block_copies(source, land, reach, offsets, edge=None):
    out = []
    for offset in offsets:
        dx, dy, dz = offset
        if dz != 0:
            continue
        near, far = edge if edge and dy else reach
        if dx == 0:
            x0, xd, nx = 0, 0, BX
        elif dx > 0:
            x0, xd, nx = BX - far, -far, far - near + 1
        else:
            x0, xd, nx = near - 1, BX + near - 1, far - near + 1
        y0, yd, ny = part(dy, BY, 8)
        out.append((offset, source(x0, nx, y0, ny), land(xd, nx, yd, ny)))
    return out


def ordered(copies):
    return sorted(copies, key=lambda c: -sum(abs(d) for d in c[0]))


def clear_around(ref, lead_x, lead_y, count_y):
    nx, ny = ref.shape[0], ref.shape[1]
    ref[0:lead_x] = jnp.zeros((lead_x, ny, 128), jnp.float32)
    ref[lead_x + BX : nx] = jnp.zeros((nx - lead_x - BX, ny, 128), jnp.float32)
    ref[lead_x : lead_x + BX, 0:lead_y, :] = jnp.zeros((BX, lead_y, 128), jnp.float32)
    end = lead_y + count_y
    ref[lead_x : lead_x + BX, end:ny, :] = jnp.zeros((BX, ny - end, 128), jnp.float32)


def clear(*refs):
    for ref in refs:
        ref[...] = jnp.zeros(ref.shape, ref.dtype)


def kernel(
    sizes, p_ref, w_ref, out_ref,
    b0, far, sb, v0, t0, zs0, zr0, wind, zsw, zrw, zsx, zrx, coef, velocity, flux,
    vp, zsv, zrv,
    bv, zsb, zrb, s1, l1, l1_far, zs1, zr1, zr1_far, b1, v1, t1,
    gathered, merged, c2, e2a, e2b,
    rows0, rows2, up1, up0, m_down0, m_down1, m_up1, m_up0,
    ruler, send_sems, recv_sems, load_sems,
):
    place = Place(sizes)
    load_p = pltpu.make_async_copy(
        p_ref, b0.at[0, pl.ds(8, BX), pl.ds(16, BY), :], load_sems.at[0])
    load_w = pltpu.make_async_copy(
        w_ref, wind.at[:, 0, pl.ds(3, BX), pl.ds(8, BY), :], load_sems.at[1])
    load_p.start()
    load_w.start()

    clear_around(b0.at[0], 8, 16, BY)
    for d in range(3):
        clear_around(wind.at[d, 0], 3, 8, BY)
    clear(far, zr0, zrw, zrx, vp, zrv, bv, zrb, l1, l1_far, zr1, zr1_far, gathered)

    barrier = pltpu.get_barrier_semaphore()
    total = jnp.int32(0)
    for offset in GREETED:
        there = place.exists(offset)
        total = total + there.astype(jnp.int32)

        def greet(offset=offset):
            pl.semaphore_signal(
                barrier, inc=1, device_id=place.device(offset), device_id_type=MESH
            )

        pl.when(there)(greet)

    def storer(ref):
        def store(f, l):
            ref[0] = l
            ref[1] = f
        return store

    clear(b0.at[1], v0, t0, rows0)
    load_p.wait()
    pack0(lambda i: b0[0, 8 + i, 16:32, :], storer(zs0))

    used = [0]

    def exchange(copies):
        k = used[0]
        used[0] += 1
        return Exchange(place, ordered(copies), send_sems.at[k], recv_sems.at[k], ruler)

    def far_block(x, nx, y, ny):
        side, lead = (0, 8) if x < 0 else (1, -BX - 5)
        return far.at[side, pl.ds(x + lead, nx), pl.ds(y + 16, ny), :]

    def b0_block(x, nx, y, ny):
        return b0.at[0, pl.ds(x + 8, nx), pl.ds(y + 16, ny), :]

    def wind_block(x, nx, y, ny):
        return wind.at[:, 0, pl.ds(x + 3, nx), pl.ds(y + 8, ny), :]

    def vp_block(x, nx, y, ny):
        return vp.at[pl.ds(x + 2, nx), pl.ds(y + 16, ny), :]

    def wind_side_copies():
        out = []
        for offset in AROUND:
            dx, dy, dz = offset
            if dx and dz:
                y0, yd, ny = part(dy, BY, 8)
                side = 0 if dz > 0 else 1
                out.append((
                    offset, zsx.at[side, (dx + 1) // 2, pl.ds(y0, ny), :],
                    zrx.at[side, (1 - dx) // 2, pl.ds(yd + 8, ny), :]))
        return out

    ex0 = exchange(
        block_copies(b0_block, b0_block, (1, 6), AROUND, (1, 5))
        + rim_copies(
            lambda s, y, ny: zs0.at[s, pl.ds(y, ny), :],
            lambda s, dx, y, ny: zr0.at[s, dx, pl.ds(y + 8, ny), :], AROUND))
    sides = [d for d in AROUND if d[0]]
    ex_far = exchange(
        block_copies(b0_block, far_block, (7, 8), [d for d in sides if d[2] == 0], (6, 7)))
    exw = exchange(
        block_copies(wind_block, wind_block, (1, 3), AROUND, (1, 2))
        + rim_copies(
            lambda s, y, ny: zsw.at[s, :, pl.ds(y, ny), :],
            lambda s, dx, y, ny: zrw.at[s, :, pl.ds(y + 8, ny), :],
            [d for d in AROUND if not d[0]])
        + wind_side_copies())
    exv = exchange(
        block_copies(vp_block, vp_block, (1, 2), NEAR, (1, 1))
        + rim_copies(
            lambda s, y, ny: zsv.at[s, pl.ds(y, ny), :],
            lambda s, dx, y, ny: zrv.at[s, dx, pl.ds(y + 8, ny), :], NEAR))

    def bv_copies():
        out = []
        for offset in AROUND:
            dx, dy, dz = offset
            if dz == 0:
                out.append((
                    offset, bv.at[pl.ds(6, 6), pl.ds(16, 8), :],
                    bv.at[pl.ds(6 - 6 * dx, 6), pl.ds(16 - 8 * dy, 8), :]))
            else:
                side = 0 if dz > 0 else 1
                out.append((
                    offset, zsb.at[side], zrb.at[side, 1 - dx, pl.ds(8 - 8 * dy, 8), :]))
        return out

    def level1_copies(reach, edge, offsets, blocks, rims):
        out = []
        for offset in offsets:
            dx, dy, dz = offset
            if dz == 0:
                near, far_end = edge if dx and dy else reach
                if dx == 0:
                    x0, xd, nx = 0, 0, 6
                elif dx > 0:
                    x0, xd, nx = 6 - far_end, -far_end, far_end - near + 1
                else:
                    x0, xd, nx = near - 1, 5 + near, far_end - near + 1
                out.append((
                    offset, s1.at[pl.ds(x0, nx)],
                    blocks.at[pl.ds(xd + 4, nx), pl.ds(8 - 8 * dy, 8), :]))
            else:
                side = 0 if dz > 0 else 1
                out.append((
                    offset, zs1.at[side], rims.at[side, 1 - dx, pl.ds(8 - 8 * dy, 8), :]))
        return out

    def coarse_copies(number):
        return [
            (d, gathered.at[number, 2, 1, 2], gathered.at[number, 2 - d[1], 1 - d[2], 2 - d[0]])
            for d in COARSE[number]
        ]

    exb = exchange(bv_copies())
    ex1 = exchange(level1_copies((1, 2), (1, 1), NEAR, l1, zr1))
    ex1_far = exchange(level1_copies(
        (3, 4), (2, 4), [d for d in AROUND if d[0] and (d[2] == 0 or d[1])], l1_far, zr1_far))
    ex2 = [exchange(coarse_copies(0)), exchange(coarse_copies(1))]

    pl.semaphore_wait(barrier, total)
    ex0.start()
    ex_far.start()

    load_w.wait()
    for d in range(3):
        pack0(lambda i: wind[d, 0, 3 + i, 8:24, :], storer(zsw.at[:, d]))
    for high, lead in ((0, 3), (1, BX)):
        pack0(lambda i: wind[i // 3, 0, lead + i % 3, 8:24, :], storer(zsx.at[:, high]), 9)
    exw.start()

    clear(velocity, flux, sb, b1, v1, t1, merged, c2, e2a, e2b, rows2, up1, up0)

    bf16 = jnp.bfloat16
    k = lax.broadcasted_iota(jnp.int32, (128, 128), 0)
    l = lax.broadcasted_iota(jnp.int32, (128, 128), 1)
    eighth = jnp.float32(0.125)
    m_down0[0:128, :] = jnp.where(k // 2 == l, eighth, 0.0).astype(bf16)
    m_down0[128:256, :] = jnp.where(
        ((k < 8) | (k >= 120)) & (k // 2 + 64 == l), eighth, 0.0).astype(bf16)
    for i in range(3):
        m_down1[i * 128 : i * 128 + 128, :] = jnp.where(
            (l // 32 == i) & (k // 2 == l % 32), eighth, 0.0).astype(bf16)
    m_up1[...] = jnp.where(
        ((l < 72) & (k == l // 2)) | ((l >= 120) & (k == 64 + l // 2)), 1.0, 0.0).astype(bf16)
    m_up0[:, 0:128] = jnp.where(k == l // 2, 1.0, 0.0).astype(bf16)
    m_up0[:, 128:256] = jnp.where(
        ((l < 8) | (l >= 120)) & (k == 64 + l // 2), 1.0, 0.0).astype(bf16)

    c0 = OMEGA / 6.0
    w1 = 0.25
    c1 = OMEGA / (6.0 * w1)
    w2 = 0.0625
    c2s = OMEGA / (6.0 * w2)
    lane8, lane16, lane24, lane40 = lanes(8), lanes(16), lanes(24), lanes(40)
    m32a, m32h = masks0(place, -8, 32)
    m24a, m24h = masks0(place, -4, 24)
    mask32, mask24 = (m32a, m32h), (m24a, m24h)

    def level1_mask(first_row, rows):
        lane = lanes(rows)
        inside = row_mask(place, first_row, rows, 8)
        return (inside & ((lane < 64) | rim_lanes(place, rows, 64, 72))).astype(jnp.float32)

    def scaled_masks(masks, factor, weight):
        factor = factor if weight is None else factor * weight
        return [m * factor for m in masks]

    def sweep0(target, iterate, x, r, n, masks):
        weight = slab_weight(place, x, BX)
        keep, share = scaled_masks(masks, KEEP, weight), scaled_masks(masks, SIXTH, weight)
        for t, (c, s) in enumerate(six0(iterate, x + 8, r, n)):
            target[t, x + 8, r : r + n, :] = keep[t] * c + share[t] * s + sb[t, x + 8, r : r + n, :]

    def scale_source(x, r, n, masks):
        factor = scaled_masks(masks, c0, slab_weight(place, x, BX))
        for t in range(2):
            sb[t, x + 8, r : r + n, :] = factor[t] * b0[t, x + 8, r : r + n, :]

    def first_two0(slabs, r, n, masks):
        for x in slabs:
            factors = scaled_masks(masks, c0, slab_weight(place, x, BX))
            for t, (c, s) in enumerate(six0(b0, x + 8, r, n)):
                v0[t, x + 8, r : r + n, :] = factors[t] * ((1.0 + KEEP) * c + SIXTH * s)

    def down1_and_send(number, r, n):
        pairs = []
        for i in range(3):
            pair = None
            for x in (2 * i, 2 * i + 1):
                c, s = six1(v1, x + 6, 16, 8)
                res = b1[x + 6, 16:24, :] - w1 * (6.0 * c - s)
                pair = res if pair is None else pair + res
            pairs.append(jnp.where(lane8 < 64, pair, 0.0))
        rows2[...] = pick(jnp.concatenate(pairs, axis=1), m_down1[...])
        gathered[number, 2, 1, 2] = (
            rows2[pl.ds(0, 4, stride=2), :] + rows2[pl.ds(1, 4, stride=2), :])
        ex2[number].start()

    def coarse(number, reach):
        for az in range(3):
            for ax in range(5):
                for ay in range(5):
                    merged[az, ax, 4 * ay : 4 * ay + 4, :] = gathered[number, ay, az, ax]
        for x in range(-reach - 3, 3 + reach + 3):
            ax, i = (x + 6) // 3, (x + 6) % 3
            left = turn(merged[0, ax], 96 - 32 * i)
            own = turn(merged[1, ax], -32 * i)
            right = turn(merged[2, ax], 32 - 32 * i)
            c2[x + 6] = jnp.where(
                lane24 < 32, own, jnp.where(lane24 < 40, right, jnp.where(lane24 >= 120, left, 0.0)))
        inside = row_mask(place, -6, 16, 4)
        mask2 = (inside & ((lane16 < 32) | rim_lanes(place, 16, 32, 40))).astype(jnp.float32)
        for x in range(-reach - 2, 3 + reach + 2):
            c, s = six1(c2, x + 6, 2, 16)
            value = (1.0 + KEEP) * c2s * c + SIXTH * c2s * s
            e2a[x + 6, 2:18, :] = scaled(value, mask2, slab_weight(place, x, 3))
        here, there = e2a, e2b
        for more in (1, 0):
            for x in range(-reach - more, 3 + reach + more):
                c, s = six1(here, x + 6, 2, 16)
                value = KEEP * c + SIXTH * s + c2s * c2[x + 6, 2:18, :]
                there[x + 6, 2:18, :] = scaled(value, mask2, slab_weight(place, x, 3))
            here, there = there, here
        return here

    def spread1(here, reach, y, n):
        slabs = 3 + 2 * reach
        spread = pick(
            jnp.concatenate([here[x - reach + 6, y + 8 : y + 8 + n, :] for x in range(slabs)], axis=0),
            m_up1[...])
        for j in range(slabs):
            value = spread[n * j : n * j + n, :]
            up1[j, pl.ds(0, n, stride=2), :] = value
            up1[j, pl.ds(1, n, stride=2), :] = value

    def last_two1(reach, r, n, mask):
        for x in range(-reach - 1, 6 + reach + 1):
            c, s = six1(v1, x + 6, r, n)
            value = KEEP * c + SIXTH * s + c1 * b1[x + 6, r : r + n, :]
            t1[x + 6, r : r + n, :] = scaled(value, mask, slab_weight(place, x, 6))
        for x in range(-reach, 6 + reach):
            c, s = six1(t1, x + 6, r, n)
            value = KEEP * c + SIXTH * s + c1 * b1[x + 6, r : r + n, :]
            v1[x + 6, r : r + n, :] = scaled(value, mask, slab_weight(place, x, 6))

    def spread0(reach, n):
        y = -(n - 8) // 2
        slabs = 6 + 2 * reach
        spread = pick(
            jnp.concatenate(
                [v1[x - reach + 6, y + 16 : y + 32, :] for x in range(slabs)], axis=0),
            m_up0[...])
        for j in range(slabs):
            for t in range(2):
                value = spread[16 * j : 16 * j + n, 128 * t : 128 * t + 128]
                up0[t, j, pl.ds(0, n, stride=2), :] = value
                up0[t, j, pl.ds(1, n, stride=2), :] = value

    ex0.wait_recv()
    for x in range(-8, BX + 8):
        b0[1, x + 8, 8:40, :] = unpack0(zr0, x, 32)
    first_two0(range(-5, BX + 5), 8, 32, mask32)
    for i in range(10):
        pair = [None, None]
        for x in (2 * i - 4, 2 * i - 3):
            for t, (c, s) in enumerate(six0(v0, x + 8, 12, 24)):
                res = b0[t, x + 8, 12:36, :] - (6.0 * c - s)
                pair[t] = res if pair[t] is None else pair[t] + res
        for t in range(2):
            rows0[t, i, 0:24, :] = pair[t]
    cells = [
        jnp.concatenate(
            [rows0[t, i, pl.ds(0, 16, stride=2), :] + rows0[t, i, pl.ds(1, 16, stride=2), :]
             for t in range(2)], axis=1)
        for i in range(10)
    ]
    source = pick(jnp.concatenate(cells, axis=0), m_down0[...])
    mask = level1_mask(-2, 16)
    for x in range(-2, 8):
        b1[x + 6, 14:30, :] = scaled(
            source[16 * (x + 2) : 16 * (x + 2) + 16, :], mask, slab_weight(place, x, 6))
    for x in range(-1, 7):
        c, s = six1(b1, x + 6, 14, 16)
        value = (1.0 + KEEP) * c1 * c + SIXTH * c1 * s
        v1[x + 6, 14:30, :] = scaled(value, mask, slab_weight(place, x, 6))
    down1_and_send(0, 14, 16)

    low = jnp.zeros((8, 128), jnp.float32)
    high = jnp.zeros((8, 128), jnp.float32)
    for i in range(6):
        block_b, block_v = b1[i + 6, 16:24, :], v1[i + 6, 16:24, :]
        bv[i + 6, 16:24, :] = jnp.where(lane8 < 64, block_b, pltpu.roll(block_v, 64, 1))
        for block, lead in ((block_b, 0), (block_v, 64)):
            group = (lane8 >= lead + 8 * i) & (lane8 < lead + 8 * i + 8)
            low = jnp.where(group, turn(block, lead + 8 * i), low)
            high = jnp.where(group, turn(block, lead + 8 * i - 56), high)
    zsb[0] = high
    zsb[1] = low
    exb.start()
    ex0.wait_send()
    ex_far.wait_recv()
    for side in range(2):
        for k in range(3):
            x = k - 8 if side == 0 else BX + 5 + k
            distance = -x if side == 0 else x - BX + 1
            if distance > 6:
                b0[0, x + 8, 16:32, :] = far[side, k, 16:32, :]
            if distance < 8:
                for r in (8, 32):
                    b0[0, x + 8, r : r + 8, :] = far[side, k, r : r + 8, :]
    first_two0((-7, -6, -5, BX + 4, BX + 5, BX + 6), 8, 32, mask32)
    for x in range(-6, BX + 6):
        scale_source(x, 8, 32, mask32)
    ex_far.wait_send()
    exw.wait_recv()
    for x in range(-3, BX + 3):
        ones = scaled_masks(mask24, 1.0, slab_weight(place, x, BX))
        halves = scaled_masks(mask24, 0.5, slab_weight(place, x, BX))
        for d in range(3):
            if 0 <= x < BX:
                rim = unpack_columns(zrw[0, d, 4:28, :], zrw[1, d, 4:28, :], x, 24)
            else:
                high, i = (0, x + 3) if x < 0 else (1, x - BX)
                rim = unpack_columns(
                    zrx[0, high, 4:28, :], zrx[1, high, 4:28, :], 3 * d + i, 24)
            for t, w in enumerate((wind[d, 0, x + 3, 4:28, :], rim)):
                half = halves[t] * w
                coef[d, 0, t, x + 3] = half - ones[t]
                coef[d, 1, t, x + 3] = -half - ones[t]
    exw.wait_send()
    ex2[0].wait_recv()
    here = coarse(0, 3)
    spread1(here, 3, -4, 16)
    exb.wait_recv()
    mask = level1_mask(-8, 24)
    for x in range(-6, 12):
        dx, i = beside(x, 6)
        near = bv[x + 6, 8:32, :]
        left, right = zrb[0, dx + 1], zrb[1, dx + 1]
        for lead, ref in ((0, b1), (64, v1)):
            value = jnp.where(
                lane24 < 64, turn(near, -lead),
                jnp.where(lane24 < 72, turn(right, 64 - 8 * i - lead),
                          jnp.where(lane24 >= 120, turn(left, 120 - 8 * i - lead), 0.0)))
            if ref is v1:
                value = value + up1[(x + 6) // 2, 0:24, :]
            ref[x + 6, 8:32, :] = value
    last_two1(4, 8, 24, mask)
    spread0(4, 16)
    for x in range(-7, BX + 7):
        for t in range(2):
            v0[t, x + 8, 8:40, :] += up0[t, (x + 8) // 2]
    for reach, target, iterate in ((6, t0, v0), (5, v0, t0)):
        for x in range(-reach, BX + reach):
            away = max(-x, x - BX + 1, 0)
            if reach - away <= 4:
                sweep0(target, iterate, x, 12, 24, mask24)
            else:
                sweep0(target, iterate, x, 8, 32, mask32)
    first = v0

    for x in range(-4, BX + 4):
        weight = slab_weight(place, x, BX)
        half = 0.5 if weight is None else 0.5 * weight
        i = x + 8
        a, h = first[0, i, 12:36, :], first[1, i, 12:36, :]
        ba, bh = z_back(a, h)
        na, nh = z_next(a, h)
        for t, (b, n) in enumerate(((ba, na), (bh, nh))):
            m = mask24[t] * half
            velocity[0, t, x + 4, 12:36, :] = (first[t, i + 1, 12:36, :] - first[t, i - 1, 12:36, :]) * m
            velocity[1, t, x + 4, 12:36, :] = (first[t, i, 13:37, :] - first[t, i, 11:35, :]) * m
            velocity[2, t, x + 4, 12:36, :] = (n - b) * m
    for x in range(-3, BX + 3):
        weight = slab_weight(place, x, BX)
        i = x + 4
        sevens = scaled_masks(mask24, 7.0, weight)
        ways = [[[coef[e, k, t, x + 3] for k in range(2)] for e in range(3)] for t in range(2)]
        for d in range(3):
            u = velocity.at[d]
            a, h = u[0, i, 12:36, :], u[1, i, 12:36, :]
            ba, bh = z_back(a, h)
            na, nh = z_next(a, h)
            for t, (c, b, n) in enumerate(((a, ba, na), (h, bh, nh))):
                x_low, x_high = u[t, i - 1, 12:36, :], u[t, i + 1, 12:36, :]
                y_low, y_high = u[t, i, 11:35, :], u[t, i, 13:37, :]
                along_x, along_y, along_z = ways[t]
                flux[d, t, x + 3, 4:28, :] = (
                    sevens[t] * c
                    + (along_x[0] * x_high + along_x[1] * x_low)
                    + (along_y[0] * y_high + along_y[1] * y_low)
                    + (along_z[0] * n + along_z[1] * b)
                )
    for x in range(-2, BX + 2):
        halves = scaled_masks(mask24, -0.5, slab_weight(place, x, BX))
        i = x + 3
        a, h = flux[2, 0, i, 4:28, :], flux[2, 1, i, 4:28, :]
        ba, bh = z_back(a, h)
        na, nh = z_next(a, h)
        for t, (b, n) in enumerate(((ba, na), (bh, nh))):
            value = (
                (flux[0, t, i + 1, 4:28, :] - flux[0, t, i - 1, 4:28, :])
                + (flux[1, t, i, 5:29, :] - flux[1, t, i, 3:27, :])
                + (n - b)
            )
            b0[t, x + 8, 12:36, :] = value * halves[t]

    first_two0(range(-1, BX + 1), 12, 24, mask24)
    for i in range(6):
        pair = None
        for x in (2 * i, 2 * i + 1):
            ((c, s),) = six0(v0, x + 8, 16, 16, rim=False)
            res = b0[0, x + 8, 16:32, :] - (6.0 * c - s)
            pair = res if pair is None else pair + res
        rows0[0, i, 0:16, :] = pair
    cells = [rows0[0, i, pl.ds(0, 8, stride=2), :] + rows0[0, i, pl.ds(1, 8, stride=2), :] for i in range(6)]
    source = pick(jnp.concatenate(cells, axis=0), m_down0[0:128, :])
    low = jnp.zeros((8, 128), jnp.float32)
    high = jnp.zeros((8, 128), jnp.float32)
    for i in range(6):
        block = source[8 * i : 8 * i + 8, :]
        s1[i] = block
        l1[4 + i, 8:16, :] = block
        group = (lane8 >= 8 * i) & (lane8 < 8 * i + 8)
        low = jnp.where(group, turn(block, 8 * i), low)
        high = jnp.where(group, turn(block, 8 * i - 56), high)
    zs1[0] = high
    zs1[1] = low
    ex1.start()
    ex1_far.start()
    for x in range(BX):
        vp[x + 2, 16:32, :] = v0[0, x + 8, 16:32, :]
    pack0(lambda i: v0[0, 8 + i, 16:32, :], storer(zsv))
    exv.start()
    ex2[0].wait_send()
    exb.wait_send()
    ex1.wait_recv()
    mask = level1_mask(-4, 16)

    def source1(slabs, block, rim):
        for x in slabs:
            dx, i = beside(x, 6)
            b1[x + 6, 8:32, :] = jnp.where(
                lane24 < 64, block(x + 4),
                jnp.where(lane24 < 72, turn(rim(1, dx + 1), 64 - 8 * i),
                          jnp.where(lane24 >= 120, turn(rim(0, dx + 1), 120 - 8 * i), 0.0)))

    def first_two1(reach):
        for x in range(-reach, 6 + reach):
            factors = scaled_masks((mask,), c1, slab_weight(place, x, 6))
            c, s = six1(b1, x + 6, 12, 16)
            v1[x + 6, 12:28, :] = factors[0] * ((1.0 + KEEP) * c + SIXTH * s)

    source1(range(-2, 8), lambda k: l1[k], lambda side, k: zr1[side, k])
    first_two1(1)
    down1_and_send(1, 12, 16)
    ex1_far.wait_recv()
    source1(
        range(-4, 10), lambda k: l1[k] + l1_far[k],
        lambda side, k: zr1[side, k] + zr1_far[side, k])
    first_two1(3)
    ex1.wait_send()
    ex1_far.wait_send()
    exv.wait_send()
    exv.wait_recv()
    for x in range(-1, BX + 1):
        scale_source(x, 12, 24, mask24)
    for x in range(-2, BX + 2):
        v0[0, x + 8, 12:36, :] = vp[x + 2, 12:36, :]
        v0[1, x + 8, 8:40, :] = unpack0(zrv, x, 32)
    ex2[1].wait_recv()
    here = coarse(1, 2)
    spread1(here, 2, -2, 8)
    for x in range(-3, 9):
        v1[x + 6, 12:28, :] += up1[(x + 4) // 2, 0:16, :]
    last_two1(1, 12, 16, mask)
    spread0(1, 12)
    for x in range(-2, BX + 2):
        for t in range(2):
            v0[t, x + 8, 12:36, :] += up0[t, (x + 2) // 2, 0:24, :]
    for x in range(-1, BX + 1):
        sweep0(t0, v0, x, 12, 24, mask24)
    for x in range(BX):
        ((c, s),) = six0(t0, x + 8, 16, 16, rim=False)
        out_ref[x] = KEEP * c + SIXTH * s + sb[0, x + 8, 16:32, :]
    ex2[1].wait_send()


def solution(mesh):
    sizes = tuple(mesh.shape[a] for a in AXES)
    exchanges = 9
    f32 = jnp.float32
    bf16 = jnp.bfloat16

    def vmem(*shape, dtype=f32):
        return pltpu.VMEM(shape, dtype)

    def body(pressure, wind):
        return pl.pallas_call(
            functools.partial(kernel, sizes),
            out_shape=jax.ShapeDtypeStruct((BX, BY, BZ), f32),
            in_specs=[pl.BlockSpec(memory_space=pl.ANY)] * 2,
            out_specs=pl.BlockSpec(memory_space=pltpu.VMEM),
            scratch_shapes=[
                vmem(2, 28, 48, 128),
                vmem(2, 3, 48, 128),
                vmem(2, 28, 48, 128),
                vmem(2, 28, 48, 128),
                vmem(2, 28, 48, 128),
                vmem(2, 16, 128),
                vmem(2, 3, 32, 128),
                vmem(3, 1, 18, 32, 128),
                vmem(2, 3, 16, 128),
                vmem(2, 3, 32, 128),
                vmem(2, 2, 16, 128),
                vmem(2, 2, 32, 128),
                vmem(3, 2, 2, 18, 24, 128),
                vmem(3, 2, 20, 48, 128),
                vmem(3, 2, 18, 32, 128),
                vmem(16, 48, 128),
                vmem(2, 16, 128),
                vmem(2, 3, 32, 128),
                vmem(18, 40, 128),
                vmem(2, 8, 128),
                vmem(2, 3, 24, 128),
                vmem(6, 8, 128),
                vmem(14, 24, 128),
                vmem(14, 24, 128),
                vmem(2, 8, 128),
                vmem(2, 3, 24, 128),
                vmem(2, 3, 24, 128),
                vmem(18, 40, 128),
                vmem(18, 40, 128),
                vmem(18, 40, 128),
                vmem(2, 5, 3, 5, 4, 128),
                vmem(3, 5, 24, 128),
                vmem(15, 24, 128),
                vmem(15, 24, 128),
                vmem(15, 24, 128),
                vmem(2, 10, 32, 128),
                vmem(8, 128),
                vmem(9, 32, 128),
                vmem(2, 14, 32, 128),
                vmem(256, 128, dtype=bf16),
                vmem(384, 128, dtype=bf16),
                vmem(128, 128, dtype=bf16),
                vmem(128, 256, dtype=bf16),
                vmem(512, 4, 128),
                pltpu.SemaphoreType.DMA((exchanges,)),
                pltpu.SemaphoreType.DMA((exchanges,)),
                pltpu.SemaphoreType.DMA((2,)),
            ],
            compiler_params=pltpu.CompilerParams(
                collective_id=0, has_side_effects=True, vmem_limit_bytes=56400000
            ),
            name="schur",
        )(pressure, wind)

    in_specs = (P("gx", "gy", "gz"), P(None, "gx", "gy", "gz"))
    return jax.shard_map(
        body, mesh=mesh, in_specs=in_specs, out_specs=P("gx", "gy", "gz"), check_vma=False
    )
```

```python
import functools

import jax
import jax.numpy as jnp
from jax import lax
from jax.experimental import pallas as pl
from jax.experimental.pallas import tpu as pltpu
from jax.sharding import PartitionSpec as P

MESH = pl.DeviceIdType.MESH
AXES = ("gx", "gy", "gz")
BX, BY, BZ = 12, 16, 128
OMEGA = 0.8
KEEP = 1.0 - OMEGA
SIXTH = OMEGA / 6.0

AROUND = [
    (dx, dy, dz)
    for dz in (0, 1, -1)
    for dx in (0, 1, -1)
    for dy in (0, 1, -1)
    if (dx, dy, dz) != (0, 0, 0)
]
AROUND.sort(key=lambda d: -(abs(d[0]) + abs(d[1]) + abs(d[2])))

NEAR = [d for d in AROUND if sum(map(abs, d)) <= 2]


def coarse_offsets(far_edges):
    out = []
    for dx in range(-2, 3):
        for dy in range(-2, 3):
            for dz in (-1, 0, 1):
                shape = (abs(dx), abs(dy), abs(dz))
                if shape[:2] in ((0, 0), (0, 1), (1, 0), (1, 1), (0, 2), (2, 0), (2, 1)):
                    keep = shape != (0, 0, 0)
                else:
                    keep = far_edges and shape[:2] == (1, 2)
                if keep:
                    out.append((dx, dy, dz))
    return sorted(out, key=lambda d: -sum(map(abs, d)))


COARSE = (coarse_offsets(True), coarse_offsets(False))
GREETED = AROUND


def part(delta, count, width):
    if delta == 0:
        return 0, 0, count
    if delta > 0:
        return count - width, -width, width
    return 0, count, width


class Place:
    def __init__(self, sizes):
        self.sizes = sizes
        self.at = [lax.axis_index(a) for a in AXES]
        self.has = []
        for g, n in zip(self.at, sizes):
            self.has.append({d: (g + d >= 0) & (g + d < n) for d in (-2, -1, 1, 2)})

        kinds = []
        for n in sizes:
            kinds.append(sorted({
                tuple(sum(0 <= g + d < n for d in (-k, k)) for k in (1, 2)) for g in range(n)
            }))
        self.profiles = [(a, b, c) for a in kinds[0] for b in kinds[1] for c in kinds[2]]
        self.kinds = kinds
        self.counts = [
            [t[-k].astype(jnp.int32) + t[k].astype(jnp.int32) for k in (1, 2)] for t in self.has
        ]

    def matches(self, profile):
        found = None
        for counts, wanted, kinds in zip(self.counts, profile, self.kinds):
            for c, v, seen in zip(counts, wanted, zip(*kinds)):
                if len(set(seen)) > 1:
                    found = (c == v) if found is None else found & (c == v)
        return True if found is None else found

    def exists(self, offset):
        found = None
        for table, d in zip(self.has, offset):
            if d:
                found = table[d] if found is None else found & table[d]
        return found

    def device(self, offset):
        return tuple(
            lax.rem(g + (d + n), n) if d else g for g, d, n in zip(self.at, offset, self.sizes)
        )


class Exchange:
    def __init__(self, place, copies, send_sem, recv_sem, ruler):
        self.place, self.items = place, []
        self.send_sem, self.recv_sem, self.ruler = send_sem, recv_sem, ruler
        self.weights = []
        for offset, src, dst in copies:
            copy = pltpu.make_async_remote_copy(
                src_ref=src,
                dst_ref=dst,
                send_sem=send_sem,
                recv_sem=recv_sem,
                device_id=place.device(offset),
                device_id_type=MESH,
            )
            self.items.append((offset, copy))
            units = 1
            for n in src.shape:
                units *= n
            self.weights.append((tuple(abs(d) for d in offset), units // 512))

    def start(self):
        for offset, copy in self.items:
            pl.when(self.place.exists(offset))(copy.start)

    def wait(self, sem):
        for profile in self.place.profiles:
            total = 0
            for shape, units in self.weights:
                share = 8 * units
                for counts, d in zip(profile, shape):
                    share = share * counts[d - 1] // 2 if d else share
                total += share
            total //= 8
            if total:
                rows = self.ruler.at[pl.ds(0, total)]
                pl.when(self.place.matches(profile))(pltpu.make_async_copy(rows, rows, sem).wait)

    def wait_recv(self):
        self.wait(self.recv_sem)

    def wait_send(self):
        self.wait(self.send_sem)


def lanes(rows):
    return lax.broadcasted_iota(jnp.int32, (rows, 128), 1)


def row_mask(place, first_row, rows, extent):
    y = first_row + lax.broadcasted_iota(jnp.int32, (rows, 128), 0)
    has = place.has[1]
    low = jnp.where(has[-2], -64, jnp.where(has[-1], -extent, 0))
    high = jnp.where(has[2], 64, jnp.where(has[1], 2 * extent, extent))
    return (y >= low) & (y < high)


def rim_lanes(place, rows, start, right_end):
    lane = lanes(rows)
    right_stop = jnp.where(place.has[2][1], right_end, 0)
    left_start = jnp.where(place.has[2][-1], 120, 128)
    return ((lane >= start) & (lane < right_stop)) | (lane >= left_start)


def slab_weight(place, x, extent):
    if 0 <= x < extent:
        return None
    return place.has[0][x // extent].astype(jnp.float32)


def z_back(a, h):
    lane0 = lanes(a.shape[0]) == 0
    ra, rh = pltpu.roll(a, 1, 1), pltpu.roll(h, 1, 1)
    return jnp.where(lane0, rh, ra), jnp.where(lane0, ra, rh)


def z_next(a, h):
    lane127 = lanes(a.shape[0]) == 127
    ra, rh = pltpu.roll(a, 127, 1), pltpu.roll(h, 127, 1)
    return jnp.where(lane127, rh, ra), jnp.where(lane127, ra, rh)


def masks0(place, first_row, rows):
    inner = row_mask(place, first_row, rows, BY)
    rim = inner & rim_lanes(place, rows, 0, 8)
    return inner.astype(jnp.float32), rim.astype(jnp.float32)


def scaled(value, mask, weight):
    value = value * mask
    return value if weight is None else value * weight


def six0(ref, i, r, n, rim=True):
    a, h = ref[0, i, r : r + n, :], ref[1, i, r : r + n, :]
    ba, bh = z_back(a, h)
    na, nh = z_next(a, h)
    out = []
    for t, (c, b, f) in enumerate(((a, ba, na), (h, bh, nh))):
        if t and not rim:
            break
        s = (
            (ref[t, i - 1, r : r + n, :] + ref[t, i + 1, r : r + n, :])
            + (ref[t, i, r - 1 : r - 1 + n, :] + ref[t, i, r + 1 : r + 1 + n, :])
            + (b + f)
        )
        out.append((c, s))
    return out


def six1(ref, i, r, n):
    c = ref[i, r : r + n, :]
    s = (
        (ref[i - 1, r : r + n, :] + ref[i + 1, r : r + n, :])
        + (ref[i, r - 1 : r - 1 + n, :] + ref[i, r + 1 : r + 1 + n, :])
        + (pltpu.roll(c, 1, 1) + pltpu.roll(c, 127, 1))
    )
    return c, s


def pick(a, m):
    high = a.astype(jnp.bfloat16)
    low = (a - high.astype(jnp.float32)).astype(jnp.bfloat16)
    return jnp.dot(high, m, preferred_element_type=jnp.float32) + jnp.dot(
        low, m, preferred_element_type=jnp.float32
    )


def turn(value, shift):
    shift %= 128
    return pltpu.roll(value, shift, 1) if shift else value


def pack0(load, store, count=BX):
    lane = lanes(BY)
    first = jnp.zeros((BY, 128), jnp.float32)
    last = jnp.zeros((BY, 128), jnp.float32)
    for i in range(count):
        turned = turn(load(i), 8 * i)
        first = jnp.where((lane >= 8 * i) & (lane < 8 * i + 8), turned, first)
        at = (8 * i - 8) % 128
        last = jnp.where((lane >= at) & (lane < at + 8), turned, last)
    store(first, last)


def beside(x, count):
    return (0, x) if 0 <= x < count else ((-1, x + count) if x < 0 else (1, x - count))


def unpack0(land, x, rows):
    dx, i = beside(x, BX)
    return unpack_columns(land[0, dx + 1], land[1, dx + 1], i, rows)


def unpack_columns(left, right, i, rows):
    left, right = turn(left, -8 * i), turn(right, -8 * i)
    lane = lanes(rows)
    return jnp.where(lane < 8, right, jnp.where(lane >= 120, left, 0.0))


def rim_copies(source, land, offsets):
    out = []
    for offset in offsets:
        dx, dy, dz = offset
        if dz == 0:
            continue
        y0, yd, ny = part(dy, BY, 8)
        side = 0 if dz > 0 else 1
        out.append((offset, source(side, y0, ny), land(side, 1 - dx, yd, ny)))
    return out


def block_copies(source, land, reach, offsets, edge=None):
    out = []
    for offset in offsets:
        dx, dy, dz = offset
        if dz != 0:
            continue
        near, far = edge if edge and dy else reach
        if dx == 0:
            x0, xd, nx = 0, 0, BX
        elif dx > 0:
            x0, xd, nx = BX - far, -far, far - near + 1
        else:
            x0, xd, nx = near - 1, BX + near - 1, far - near + 1
        y0, yd, ny = part(dy, BY, 8)
        out.append((offset, source(x0, nx, y0, ny), land(xd, nx, yd, ny)))
    return out


def ordered(copies):
    return sorted(copies, key=lambda c: -sum(abs(d) for d in c[0]))


def clear_around(ref, lead_x, lead_y, count_y):
    nx, ny = ref.shape[0], ref.shape[1]
    ref[0:lead_x] = jnp.zeros((lead_x, ny, 128), jnp.float32)
    ref[lead_x + BX : nx] = jnp.zeros((nx - lead_x - BX, ny, 128), jnp.float32)
    ref[lead_x : lead_x + BX, 0:lead_y, :] = jnp.zeros((BX, lead_y, 128), jnp.float32)
    end = lead_y + count_y
    ref[lead_x : lead_x + BX, end:ny, :] = jnp.zeros((BX, ny - end, 128), jnp.float32)


def clear(*refs):
    for ref in refs:
        ref[...] = jnp.zeros(ref.shape, ref.dtype)


def kernel(
    sizes, p_ref, w_ref, out_ref,
    b0, far, sb, v0, t0, zs0, zr0, wind, zsw, zrw, zsx, zrx, coef, velocity, flux,
    vp, zsv, zrv,
    bv, zsb, zrb, s1, l1, l1_far, zs1, zr1, zr1_far, b1, v1, t1,
    gathered, merged, c2, e2a, e2b,
    rows0, rows2, up1, up0, m_down0, m_down1, m_up1, m_up0,
    ruler, send_sems, recv_sems, load_sems,
):
    place = Place(sizes)
    load_p = pltpu.make_async_copy(
        p_ref, b0.at[0, pl.ds(8, BX), pl.ds(16, BY), :], load_sems.at[0])
    load_w = pltpu.make_async_copy(
        w_ref, wind.at[:, 0, pl.ds(3, BX), pl.ds(8, BY), :], load_sems.at[1])
    load_p.start()
    load_w.start()

    clear_around(b0.at[0], 8, 16, BY)
    for d in range(3):
        clear_around(wind.at[d, 0], 3, 8, BY)
    clear(far, zr0, zrw, zrx, gathered)

    barrier = pltpu.get_barrier_semaphore()
    total = jnp.int32(0)
    for offset in GREETED:
        there = place.exists(offset)
        total = total + there.astype(jnp.int32)

        def greet(offset=offset):
            pl.semaphore_signal(
                barrier, inc=1, device_id=place.device(offset), device_id_type=MESH
            )

        pl.when(there)(greet)

    def storer(ref):
        def store(f, l):
            ref[0] = l
            ref[1] = f
        return store

    clear(vp, zrv, bv, zrb, l1, l1_far, zr1, zr1_far)
    clear(b0.at[1], v0, t0, rows0)
    load_p.wait()
    pack0(lambda i: b0[0, 8 + i, 16:32, :], storer(zs0))

    used = [0]

    def exchange(copies):
        k = used[0]
        used[0] += 1
        return Exchange(place, ordered(copies), send_sems.at[k], recv_sems.at[k], ruler)

    def far_block(x, nx, y, ny):
        side, lead = (0, 8) if x < 0 else (1, -BX - 5)
        return far.at[side, pl.ds(x + lead, nx), pl.ds(y + 16, ny), :]

    def b0_block(x, nx, y, ny):
        return b0.at[0, pl.ds(x + 8, nx), pl.ds(y + 16, ny), :]

    def wind_block(x, nx, y, ny):
        return wind.at[:, 0, pl.ds(x + 3, nx), pl.ds(y + 8, ny), :]

    def vp_block(x, nx, y, ny):
        return vp.at[pl.ds(x + 2, nx), pl.ds(y + 16, ny), :]

    def wind_side_copies():
        out = []
        for offset in AROUND:
            dx, dy, dz = offset
            if dx and dz:
                y0, yd, ny = part(dy, BY, 8)
                side = 0 if dz > 0 else 1
                out.append((
                    offset, zsx.at[side, (dx + 1) // 2, pl.ds(y0, ny), :],
                    zrx.at[side, (1 - dx) // 2, pl.ds(yd + 8, ny), :]))
        return out

    ex0 = exchange(
        block_copies(b0_block, b0_block, (1, 6), AROUND, (1, 5))
        + rim_copies(
            lambda s, y, ny: zs0.at[s, pl.ds(y, ny), :],
            lambda s, dx, y, ny: zr0.at[s, dx, pl.ds(y + 8, ny), :], AROUND))
    sides = [d for d in AROUND if d[0]]
    ex_far = exchange(
        block_copies(b0_block, far_block, (7, 8), [d for d in sides if d[2] == 0], (6, 7)))
    exw = exchange(
        block_copies(wind_block, wind_block, (1, 3), AROUND, (1, 2))
        + rim_copies(
            lambda s, y, ny: zsw.at[s, :, pl.ds(y, ny), :],
            lambda s, dx, y, ny: zrw.at[s, :, pl.ds(y + 8, ny), :],
            [d for d in AROUND if not d[0]])
        + wind_side_copies())
    exv = exchange(
        block_copies(vp_block, vp_block, (1, 2), NEAR, (1, 1))
        + rim_copies(
            lambda s, y, ny: zsv.at[s, pl.ds(y, ny), :],
            lambda s, dx, y, ny: zrv.at[s, dx, pl.ds(y + 8, ny), :], NEAR))

    def bv_copies():
        out = []
        for offset in AROUND:
            dx, dy, dz = offset
            if dz == 0:
                out.append((
                    offset, bv.at[pl.ds(6, 6), pl.ds(16, 8), :],
                    bv.at[pl.ds(6 - 6 * dx, 6), pl.ds(16 - 8 * dy, 8), :]))
            else:
                side = 0 if dz > 0 else 1
                out.append((
                    offset, zsb.at[side], zrb.at[side, 1 - dx, pl.ds(8 - 8 * dy, 8), :]))
        return out

    def level1_copies(reach, edge, offsets, blocks, rims):
        out = []
        for offset in offsets:
            dx, dy, dz = offset
            if dz == 0:
                near, far_end = edge if dx and dy else reach
                if dx == 0:
                    x0, xd, nx = 0, 0, 6
                elif dx > 0:
                    x0, xd, nx = 6 - far_end, -far_end, far_end - near + 1
                else:
                    x0, xd, nx = near - 1, 5 + near, far_end - near + 1
                out.append((
                    offset, s1.at[pl.ds(x0, nx)],
                    blocks.at[pl.ds(xd + 4, nx), pl.ds(8 - 8 * dy, 8), :]))
            else:
                side = 0 if dz > 0 else 1
                out.append((
                    offset, zs1.at[side], rims.at[side, 1 - dx, pl.ds(8 - 8 * dy, 8), :]))
        return out

    def coarse_copies(number):
        return [
            (d, gathered.at[number, 2, 1, 2], gathered.at[number, 2 - d[1], 1 - d[2], 2 - d[0]])
            for d in COARSE[number]
        ]

    exb = exchange(bv_copies())
    ex1 = exchange(level1_copies((1, 2), (1, 1), NEAR, l1, zr1))
    ex1_far = exchange(level1_copies(
        (3, 4), (2, 4), [d for d in AROUND if d[0] and (d[2] == 0 or d[1])], l1_far, zr1_far))
    ex2 = [exchange(coarse_copies(0)), exchange(coarse_copies(1))]

    pl.semaphore_wait(barrier, total)
    ex0.start()
    ex_far.start()

    load_w.wait()
    for d in range(3):
        pack0(lambda i: wind[d, 0, 3 + i, 8:24, :], storer(zsw.at[:, d]))
    for high, lead in ((0, 3), (1, BX)):
        pack0(lambda i: wind[i // 3, 0, lead + i % 3, 8:24, :], storer(zsx.at[:, high]), 9)
    exw.start()

    clear(velocity, flux, sb, b1, v1, t1, merged, c2, e2a, e2b, rows2, up1, up0)

    bf16 = jnp.bfloat16
    k = lax.broadcasted_iota(jnp.int32, (128, 128), 0)
    l = lax.broadcasted_iota(jnp.int32, (128, 128), 1)
    eighth = jnp.float32(0.125)
    m_down0[0:128, :] = jnp.where(k // 2 == l, eighth, 0.0).astype(bf16)
    m_down0[128:256, :] = jnp.where(
        ((k < 8) | (k >= 120)) & (k // 2 + 64 == l), eighth, 0.0).astype(bf16)
    for i in range(3):
        m_down1[i * 128 : i * 128 + 128, :] = jnp.where(
            (l // 32 == i) & (k // 2 == l % 32), eighth, 0.0).astype(bf16)
    m_up1[...] = jnp.where(
        ((l < 72) & (k == l // 2)) | ((l >= 120) & (k == 64 + l // 2)), 1.0, 0.0).astype(bf16)
    m_up0[:, 0:128] = jnp.where(k == l // 2, 1.0, 0.0).astype(bf16)
    m_up0[:, 128:256] = jnp.where(
        ((l < 8) | (l >= 120)) & (k == 64 + l // 2), 1.0, 0.0).astype(bf16)

    c0 = OMEGA / 6.0
    w1 = 0.25
    c1 = OMEGA / (6.0 * w1)
    w2 = 0.0625
    c2s = OMEGA / (6.0 * w2)
    lane8, lane16, lane24, lane40 = lanes(8), lanes(16), lanes(24), lanes(40)
    m32a, m32h = masks0(place, -8, 32)
    m24a, m24h = masks0(place, -4, 24)
    mask32, mask24 = (m32a, m32h), (m24a, m24h)
    mask16 = masks0(place, 0, 16)

    def span(reach, x):
        left = reach - max(-x, x - BX + 1, 0)
        if left <= 0:
            return 16, 16, mask16, False
        if left <= 4:
            return 12, 24, mask24, True
        return 8, 32, mask32, True


    def level1_mask(first_row, rows):
        lane = lanes(rows)
        inside = row_mask(place, first_row, rows, 8)
        return (inside & ((lane < 64) | rim_lanes(place, rows, 64, 72))).astype(jnp.float32)

    def scaled_masks(masks, factor, weight):
        factor = factor if weight is None else factor * weight
        return [m * factor for m in masks]

    def sweep0(target, iterate, x, reach):
        r, n, masks, rim = span(reach, x)
        weight = slab_weight(place, x, BX)
        keep, share = scaled_masks(masks, KEEP, weight), scaled_masks(masks, SIXTH, weight)
        for t, (c, s) in enumerate(six0(iterate, x + 8, r, n, rim)):
            target[t, x + 8, r : r + n, :] = keep[t] * c + share[t] * s + sb[t, x + 8, r : r + n, :]

    def scale_source(x, r, n, masks):
        factor = scaled_masks(masks, c0, slab_weight(place, x, BX))
        for t in range(2):
            sb[t, x + 8, r : r + n, :] = factor[t] * b0[t, x + 8, r : r + n, :]

    def first_two0(slabs, reach):
        for x in slabs:
            r, n, masks, rim = span(reach, x)
            factors = scaled_masks(masks, c0, slab_weight(place, x, BX))
            for t, (c, s) in enumerate(six0(b0, x + 8, r, n, rim)):
                v0[t, x + 8, r : r + n, :] = factors[t] * ((1.0 + KEEP) * c + SIXTH * s)

    def down1_and_send(number, r, n):
        pairs = []
        for i in range(3):
            pair = None
            for x in (2 * i, 2 * i + 1):
                c, s = six1(v1, x + 6, 16, 8)
                res = b1[x + 6, 16:24, :] - w1 * (6.0 * c - s)
                pair = res if pair is None else pair + res
            pairs.append(jnp.where(lane8 < 64, pair, 0.0))
        rows2[...] = pick(jnp.concatenate(pairs, axis=1), m_down1[...])
        gathered[number, 2, 1, 2] = (
            rows2[pl.ds(0, 4, stride=2), :] + rows2[pl.ds(1, 4, stride=2), :])
        ex2[number].start()

    def coarse(number, reach):
        for az in range(3):
            for ax in range(5):
                for ay in range(5):
                    merged[az, ax, 4 * ay : 4 * ay + 4, :] = gathered[number, ay, az, ax]
        for x in range(-reach - 3, 3 + reach + 3):
            ax, i = (x + 6) // 3, (x + 6) % 3
            left = turn(merged[0, ax], 96 - 32 * i)
            own = turn(merged[1, ax], -32 * i)
            right = turn(merged[2, ax], 32 - 32 * i)
            c2[x + 6] = jnp.where(
                lane24 < 32, own, jnp.where(lane24 < 40, right, jnp.where(lane24 >= 120, left, 0.0)))
        inside = row_mask(place, -6, 16, 4)
        mask2 = (inside & ((lane16 < 32) | rim_lanes(place, 16, 32, 40))).astype(jnp.float32)
        for x in range(-reach - 2, 3 + reach + 2):
            c, s = six1(c2, x + 6, 2, 16)
            value = (1.0 + KEEP) * c2s * c + SIXTH * c2s * s
            e2a[x + 6, 2:18, :] = scaled(value, mask2, slab_weight(place, x, 3))
        here, there = e2a, e2b
        for more in (1, 0):
            for x in range(-reach - more, 3 + reach + more):
                c, s = six1(here, x + 6, 2, 16)
                value = KEEP * c + SIXTH * s + c2s * c2[x + 6, 2:18, :]
                there[x + 6, 2:18, :] = scaled(value, mask2, slab_weight(place, x, 3))
            here, there = there, here
        return here

    def spread1(here, reach, y, n):
        slabs = 3 + 2 * reach
        spread = pick(
            jnp.concatenate([here[x - reach + 6, y + 8 : y + 8 + n, :] for x in range(slabs)], axis=0),
            m_up1[...])
        for j in range(slabs):
            value = spread[n * j : n * j + n, :]
            up1[j, pl.ds(0, n, stride=2), :] = value
            up1[j, pl.ds(1, n, stride=2), :] = value

    def last_two1(reach, r, n, mask):
        for x in range(-reach - 1, 6 + reach + 1):
            c, s = six1(v1, x + 6, r, n)
            value = KEEP * c + SIXTH * s + c1 * b1[x + 6, r : r + n, :]
            t1[x + 6, r : r + n, :] = scaled(value, mask, slab_weight(place, x, 6))
        for x in range(-reach, 6 + reach):
            c, s = six1(t1, x + 6, r, n)
            value = KEEP * c + SIXTH * s + c1 * b1[x + 6, r : r + n, :]
            v1[x + 6, r : r + n, :] = scaled(value, mask, slab_weight(place, x, 6))

    def spread0(reach, n):
        y = -(n - 8) // 2
        slabs = 6 + 2 * reach
        spread = pick(
            jnp.concatenate(
                [v1[x - reach + 6, y + 16 : y + 32, :] for x in range(slabs)], axis=0),
            m_up0[...])
        for j in range(slabs):
            for t in range(2):
                value = spread[16 * j : 16 * j + n, 128 * t : 128 * t + 128]
                up0[t, j, pl.ds(0, n, stride=2), :] = value
                up0[t, j, pl.ds(1, n, stride=2), :] = value

    ex0.wait_recv()
    for x in range(-6, BX + 6):
        r, n = span(6, x)[:2]
        b0[1, x + 8, r : r + n, :] = unpack0(zr0.at[:, :, pl.ds(r - 8, n), :], x, n)
    first_two0(range(-5, BX + 5), 5)
    for i in range(10):
        pair = [None, None]
        r, n, rim = (12, 24, True) if 0 < i < 9 else (16, 16, False)
        for x in (2 * i - 4, 2 * i - 3):
            for t, (c, s) in enumerate(six0(v0, x + 8, r, n, rim)):
                res = b0[t, x + 8, r : r + n, :] - (6.0 * c - s)
                pair[t] = res if pair[t] is None else pair[t] + res
        for t in range(1 + rim):
            rows0[t, i, r - 12 : r - 12 + n, :] = pair[t]
    cells = [
        jnp.concatenate(
            [rows0[t, i, pl.ds(0, 16, stride=2), :] + rows0[t, i, pl.ds(1, 16, stride=2), :]
             for t in range(2)], axis=1)
        for i in range(10)
    ]
    source = pick(jnp.concatenate(cells, axis=0), m_down0[...])
    mask = level1_mask(-2, 16)
    for x in range(-2, 8):
        b1[x + 6, 14:30, :] = scaled(
            source[16 * (x + 2) : 16 * (x + 2) + 16, :], mask, slab_weight(place, x, 6))
    for x in range(-1, 7):
        c, s = six1(b1, x + 6, 14, 16)
        value = (1.0 + KEEP) * c1 * c + SIXTH * c1 * s
        v1[x + 6, 14:30, :] = scaled(value, mask, slab_weight(place, x, 6))
    down1_and_send(0, 14, 16)

    low = jnp.zeros((8, 128), jnp.float32)
    high = jnp.zeros((8, 128), jnp.float32)
    for i in range(6):
        block_b, block_v = b1[i + 6, 16:24, :], v1[i + 6, 16:24, :]
        bv[i + 6, 16:24, :] = jnp.where(lane8 < 64, block_b, pltpu.roll(block_v, 64, 1))
        for block, lead in ((block_b, 0), (block_v, 64)):
            group = (lane8 >= lead + 8 * i) & (lane8 < lead + 8 * i + 8)
            low = jnp.where(group, turn(block, lead + 8 * i), low)
            high = jnp.where(group, turn(block, lead + 8 * i - 56), high)
    zsb[0] = high
    zsb[1] = low
    exb.start()
    ex0.wait_send()
    ex_far.wait_recv()
    for side in range(2):
        for k in range(3):
            x = k - 8 if side == 0 else BX + 5 + k
            distance = -x if side == 0 else x - BX + 1
            if distance > 6:
                b0[0, x + 8, 16:32, :] = far[side, k, 16:32, :]
            if distance < 8:
                for r in (8, 32):
                    b0[0, x + 8, r : r + 8, :] = far[side, k, r : r + 8, :]
    outer = [x for k in range(1, 9) for x in (-k, BX - 1 + k)]
    for x in outer:
        b0[1, x + 8, 8:40, :] = unpack0(zr0, x, 32)
    first_two0(outer[:14], 7)
    for x in range(-6, BX + 6):
        scale_source(x, 8, 32, mask32)
    ex_far.wait_send()
    exw.wait_recv()
    for x in range(-3, BX + 3):
        ones = scaled_masks(mask24, 1.0, slab_weight(place, x, BX))
        halves = scaled_masks(mask24, 0.5, slab_weight(place, x, BX))
        for d in range(3):
            if 0 <= x < BX:
                rim = unpack_columns(zrw[0, d, 4:28, :], zrw[1, d, 4:28, :], x, 24)
            else:
                high, i = (0, x + 3) if x < 0 else (1, x - BX)
                rim = unpack_columns(
                    zrx[0, high, 4:28, :], zrx[1, high, 4:28, :], 3 * d + i, 24)
            for t, w in enumerate((wind[d, 0, x + 3, 4:28, :], rim)):
                half = halves[t] * w
                coef[d, 0, t, x + 3] = half - ones[t]
                coef[d, 1, t, x + 3] = -half - ones[t]
    exw.wait_send()
    ex2[0].wait_recv()
    here = coarse(0, 3)
    spread1(here, 3, -4, 16)
    exb.wait_recv()
    mask = level1_mask(-8, 24)
    for x in range(-6, 12):
        dx, i = beside(x, 6)
        near = bv[x + 6, 8:32, :]
        left, right = zrb[0, dx + 1], zrb[1, dx + 1]
        for lead, ref in ((0, b1), (64, v1)):
            value = jnp.where(
                lane24 < 64, turn(near, -lead),
                jnp.where(lane24 < 72, turn(right, 64 - 8 * i - lead),
                          jnp.where(lane24 >= 120, turn(left, 120 - 8 * i - lead), 0.0)))
            if ref is v1:
                value = value + up1[(x + 6) // 2, 0:24, :]
            ref[x + 6, 8:32, :] = value
    last_two1(4, 8, 24, mask)
    spread0(4, 16)
    for x in range(-7, BX + 7):
        for t in range(2):
            v0[t, x + 8, 8:40, :] += up0[t, (x + 8) // 2]
    for reach, target, iterate in ((6, t0, v0), (5, v0, t0)):
        for x in range(-reach, BX + reach):
            sweep0(target, iterate, x, reach)
    first = v0

    for x in range(-4, BX + 4):
        r, n, masks, rim = span(4, x)
        halves = scaled_masks(masks, 0.5, slab_weight(place, x, BX))
        i = x + 8
        rows = slice(r, r + n)
        a, h = first[0, i, rows, :], first[1, i, rows, :]
        ba, bh = z_back(a, h)
        na, nh = z_next(a, h)
        for t, (back, ahead) in enumerate(((ba, na), (bh, nh))[: 1 + rim]):
            m = halves[t]
            velocity[0, t, x + 4, rows, :] = (first[t, i + 1, rows, :] - first[t, i - 1, rows, :]) * m
            velocity[1, t, x + 4, rows, :] = (
                first[t, i, r + 1 : r + 1 + n, :] - first[t, i, r - 1 : r - 1 + n, :]) * m
            velocity[2, t, x + 4, rows, :] = (ahead - back) * m
    for x in range(-3, BX + 3):
        r, n, masks, rim = span(3, x)
        i = x + 4
        rows, low_rows = slice(r, r + n), slice(r - 8, r - 8 + n)
        sevens = scaled_masks(masks, 7.0, slab_weight(place, x, BX))
        ways = [
            [[coef[e, k, t, x + 3, r - 12 : r - 12 + n, :] for k in range(2)] for e in range(3)]
            for t in range(1 + rim)
        ]
        for d in range(3):
            u = velocity.at[d]
            a, h = u[0, i, rows, :], u[1, i, rows, :]
            ba, bh = z_back(a, h)
            na, nh = z_next(a, h)
            for t, (c, back, ahead) in enumerate(((a, ba, na), (h, bh, nh))[: 1 + rim]):
                x_low, x_high = u[t, i - 1, rows, :], u[t, i + 1, rows, :]
                y_low, y_high = u[t, i, r - 1 : r - 1 + n, :], u[t, i, r + 1 : r + 1 + n, :]
                along_x, along_y, along_z = ways[t]
                flux[d, t, x + 3, low_rows, :] = (
                    sevens[t] * c
                    + (along_x[0] * x_high + along_x[1] * x_low)
                    + (along_y[0] * y_high + along_y[1] * y_low)
                    + (along_z[0] * ahead + along_z[1] * back)
                )
    for x in range(-2, BX + 2):
        r, n, masks, rim = span(2, x)
        halves = scaled_masks(masks, -0.5, slab_weight(place, x, BX))
        i = x + 3
        q = r - 8
        rows = slice(q, q + n)
        a, h = flux[2, 0, i, rows, :], flux[2, 1, i, rows, :]
        ba, bh = z_back(a, h)
        na, nh = z_next(a, h)
        for t, (back, ahead) in enumerate(((ba, na), (bh, nh))[: 1 + rim]):
            value = (
                (flux[0, t, i + 1, rows, :] - flux[0, t, i - 1, rows, :])
                + (flux[1, t, i, q + 1 : q + 1 + n, :] - flux[1, t, i, q - 1 : q - 1 + n, :])
                + (ahead - back)
            )
            b0[t, x + 8, r : r + n, :] = value * halves[t]

    first_two0(range(-1, BX + 1), 1)
    for i in range(6):
        pair = None
        for x in (2 * i, 2 * i + 1):
            ((c, s),) = six0(v0, x + 8, 16, 16, rim=False)
            res = b0[0, x + 8, 16:32, :] - (6.0 * c - s)
            pair = res if pair is None else pair + res
        rows0[0, i, 0:16, :] = pair
    cells = [rows0[0, i, pl.ds(0, 8, stride=2), :] + rows0[0, i, pl.ds(1, 8, stride=2), :] for i in range(6)]
    source = pick(jnp.concatenate(cells, axis=0), m_down0[0:128, :])
    low = jnp.zeros((8, 128), jnp.float32)
    high = jnp.zeros((8, 128), jnp.float32)
    for i in range(6):
        block = source[8 * i : 8 * i + 8, :]
        s1[i] = block
        l1[4 + i, 8:16, :] = block
        group = (lane8 >= 8 * i) & (lane8 < 8 * i + 8)
        low = jnp.where(group, turn(block, 8 * i), low)
        high = jnp.where(group, turn(block, 8 * i - 56), high)
    zs1[0] = high
    zs1[1] = low
    ex1.start()
    ex1_far.start()
    for x in range(BX):
        vp[x + 2, 16:32, :] = v0[0, x + 8, 16:32, :]
    pack0(lambda i: v0[0, 8 + i, 16:32, :], storer(zsv))
    exv.start()
    ex2[0].wait_send()
    exb.wait_send()
    ex1.wait_recv()
    mask = level1_mask(-4, 16)

    def source1(slabs, block, rim):
        for x in slabs:
            dx, i = beside(x, 6)
            b1[x + 6, 8:32, :] = jnp.where(
                lane24 < 64, block(x + 4),
                jnp.where(lane24 < 72, turn(rim(1, dx + 1), 64 - 8 * i),
                          jnp.where(lane24 >= 120, turn(rim(0, dx + 1), 120 - 8 * i), 0.0)))

    def first_two1(reach):
        for x in range(-reach, 6 + reach):
            factors = scaled_masks((mask,), c1, slab_weight(place, x, 6))
            c, s = six1(b1, x + 6, 12, 16)
            v1[x + 6, 12:28, :] = factors[0] * ((1.0 + KEEP) * c + SIXTH * s)

    source1(range(-2, 8), lambda k: l1[k], lambda side, k: zr1[side, k])
    first_two1(1)
    down1_and_send(1, 12, 16)
    ex1_far.wait_recv()
    source1(
        range(-4, 10), lambda k: l1[k] + l1_far[k],
        lambda side, k: zr1[side, k] + zr1_far[side, k])
    first_two1(3)
    ex1.wait_send()
    ex1_far.wait_send()
    exv.wait_send()
    exv.wait_recv()
    for x in range(-1, BX + 1):
        scale_source(x, 12, 24, mask24)
    for x in range(-2, BX + 2):
        v0[0, x + 8, 12:36, :] = vp[x + 2, 12:36, :]
        v0[1, x + 8, 8:40, :] = unpack0(zrv, x, 32)
    ex2[1].wait_recv()
    here = coarse(1, 2)
    spread1(here, 2, -2, 8)
    for x in range(-3, 9):
        v1[x + 6, 12:28, :] += up1[(x + 4) // 2, 0:16, :]
    last_two1(1, 12, 16, mask)
    spread0(1, 12)
    for x in range(-2, BX + 2):
        for t in range(2):
            v0[t, x + 8, 12:36, :] += up0[t, (x + 2) // 2, 0:24, :]
    for x in range(-1, BX + 1):
        sweep0(t0, v0, x, 1)
    for x in range(BX):
        ((c, s),) = six0(t0, x + 8, 16, 16, rim=False)
        out_ref[x] = KEEP * c + SIXTH * s + sb[0, x + 8, 16:32, :]
    ex2[1].wait_send()


def solution(mesh):
    sizes = tuple(mesh.shape[a] for a in AXES)
    exchanges = 9
    f32 = jnp.float32
    bf16 = jnp.bfloat16

    def vmem(*shape, dtype=f32):
        return pltpu.VMEM(shape, dtype)

    def body(pressure, wind):
        return pl.pallas_call(
            functools.partial(kernel, sizes),
            out_shape=jax.ShapeDtypeStruct((BX, BY, BZ), f32),
            in_specs=[pl.BlockSpec(memory_space=pl.ANY)] * 2,
            out_specs=pl.BlockSpec(memory_space=pltpu.VMEM),
            scratch_shapes=[
                vmem(2, 28, 48, 128),
                vmem(2, 3, 48, 128),
                vmem(2, 28, 48, 128),
                vmem(2, 28, 48, 128),
                vmem(2, 28, 48, 128),
                vmem(2, 16, 128),
                vmem(2, 3, 32, 128),
                vmem(3, 1, 18, 32, 128),
                vmem(2, 3, 16, 128),
                vmem(2, 3, 32, 128),
                vmem(2, 2, 16, 128),
                vmem(2, 2, 32, 128),
                vmem(3, 2, 2, 18, 24, 128),
                vmem(3, 2, 20, 48, 128),
                vmem(3, 2, 18, 32, 128),
                vmem(16, 48, 128),
                vmem(2, 16, 128),
                vmem(2, 3, 32, 128),
                vmem(18, 40, 128),
                vmem(2, 8, 128),
                vmem(2, 3, 24, 128),
                vmem(6, 8, 128),
                vmem(14, 24, 128),
                vmem(14, 24, 128),
                vmem(2, 8, 128),
                vmem(2, 3, 24, 128),
                vmem(2, 3, 24, 128),
                vmem(18, 40, 128),
                vmem(18, 40, 128),
                vmem(18, 40, 128),
                vmem(2, 5, 3, 5, 4, 128),
                vmem(3, 5, 24, 128),
                vmem(15, 24, 128),
                vmem(15, 24, 128),
                vmem(15, 24, 128),
                vmem(2, 10, 32, 128),
                vmem(8, 128),
                vmem(9, 32, 128),
                vmem(2, 14, 32, 128),
                vmem(256, 128, dtype=bf16),
                vmem(384, 128, dtype=bf16),
                vmem(128, 128, dtype=bf16),
                vmem(128, 256, dtype=bf16),
                vmem(512, 4, 128),
                pltpu.SemaphoreType.DMA((exchanges,)),
                pltpu.SemaphoreType.DMA((exchanges,)),
                pltpu.SemaphoreType.DMA((2,)),
            ],
            compiler_params=pltpu.CompilerParams(
                collective_id=0, has_side_effects=True, vmem_limit_bytes=56400000
            ),
            name="schur",
        )(pressure, wind)

    in_specs = (P("gx", "gy", "gz"), P(None, "gx", "gy", "gz"))
    return jax.shard_map(
        body, mesh=mesh, in_specs=in_specs, out_specs=P("gx", "gy", "gz"), check_vma=False
    )
```

```python
import functools

import jax
import jax.numpy as jnp
from jax import lax
from jax.experimental import pallas as pl
from jax.experimental.pallas import tpu as pltpu
from jax.sharding import PartitionSpec as P

MESH = pl.DeviceIdType.MESH
AXES = ("gx", "gy", "gz")
BX, BY, BZ = 12, 16, 128
OMEGA = 0.8
KEEP = 1.0 - OMEGA
SIXTH = OMEGA / 6.0

AROUND = [
    (dx, dy, dz)
    for dz in (0, 1, -1)
    for dx in (0, 1, -1)
    for dy in (0, 1, -1)
    if (dx, dy, dz) != (0, 0, 0)
]
AROUND.sort(key=lambda d: -(abs(d[0]) + abs(d[1]) + abs(d[2])))

NEAR = [d for d in AROUND if sum(map(abs, d)) <= 2]


def coarse_offsets(far_edges):
    out = []
    for dx in range(-2, 3):
        for dy in range(-2, 3):
            for dz in (-1, 0, 1):
                shape = (abs(dx), abs(dy), abs(dz))
                if shape[:2] in ((0, 0), (0, 1), (1, 0), (1, 1), (0, 2), (2, 0), (2, 1)):
                    keep = shape != (0, 0, 0)
                else:
                    keep = far_edges and shape[:2] == (1, 2)
                if keep:
                    out.append((dx, dy, dz))
    return sorted(out, key=lambda d: -sum(map(abs, d)))


COARSE = (coarse_offsets(True), coarse_offsets(False))
GREETED = AROUND


def part(delta, count, width):
    if delta == 0:
        return 0, 0, count
    if delta > 0:
        return count - width, -width, width
    return 0, count, width


class Place:
    def __init__(self, sizes):
        self.sizes = sizes
        self.at = [lax.axis_index(a) for a in AXES]
        self.has = []
        for g, n in zip(self.at, sizes):
            self.has.append({d: (g + d >= 0) & (g + d < n) for d in (-2, -1, 1, 2)})

        kinds = []
        for n in sizes:
            kinds.append(sorted({
                tuple(sum(0 <= g + d < n for d in (-k, k)) for k in (1, 2)) for g in range(n)
            }))
        self.profiles = [(a, b, c) for a in kinds[0] for b in kinds[1] for c in kinds[2]]
        self.kinds = kinds
        self.counts = [
            [t[-k].astype(jnp.int32) + t[k].astype(jnp.int32) for k in (1, 2)] for t in self.has
        ]

    def matches(self, profile):
        found = None
        for counts, wanted, kinds in zip(self.counts, profile, self.kinds):
            for c, v, seen in zip(counts, wanted, zip(*kinds)):
                if len(set(seen)) > 1:
                    found = (c == v) if found is None else found & (c == v)
        return True if found is None else found

    def exists(self, offset):
        found = None
        for table, d in zip(self.has, offset):
            if d:
                found = table[d] if found is None else found & table[d]
        return found

    def device(self, offset):
        return tuple(
            lax.rem(g + (d + n), n) if d else g for g, d, n in zip(self.at, offset, self.sizes)
        )


class Exchange:
    def __init__(self, place, copies, send_sem, recv_sem, ruler):
        self.place, self.items = place, []
        self.send_sem, self.recv_sem, self.ruler = send_sem, recv_sem, ruler
        self.weights = []
        for offset, src, dst in copies:
            copy = pltpu.make_async_remote_copy(
                src_ref=src,
                dst_ref=dst,
                send_sem=send_sem,
                recv_sem=recv_sem,
                device_id=place.device(offset),
                device_id_type=MESH,
            )
            self.items.append((offset, copy))
            units = 1
            for n in src.shape:
                units *= n
            self.weights.append((tuple(abs(d) for d in offset), units // 512))

    def start(self):
        for offset, copy in self.items:
            pl.when(self.place.exists(offset))(copy.start)

    def wait(self, sem):
        for profile in self.place.profiles:
            total = 0
            for shape, units in self.weights:
                share = 8 * units
                for counts, d in zip(profile, shape):
                    share = share * counts[d - 1] // 2 if d else share
                total += share
            total //= 8
            if total:
                rows = self.ruler.at[pl.ds(0, total)]
                pl.when(self.place.matches(profile))(pltpu.make_async_copy(rows, rows, sem).wait)

    def wait_recv(self):
        self.wait(self.recv_sem)

    def wait_send(self):
        self.wait(self.send_sem)


def lanes(rows):
    return lax.broadcasted_iota(jnp.int32, (rows, 128), 1)


def row_mask(place, first_row, rows, extent):
    y = first_row + lax.broadcasted_iota(jnp.int32, (rows, 128), 0)
    has = place.has[1]
    low = jnp.where(has[-2], -64, jnp.where(has[-1], -extent, 0))
    high = jnp.where(has[2], 64, jnp.where(has[1], 2 * extent, extent))
    return (y >= low) & (y < high)


def rim_lanes(place, rows, start, right_end):
    lane = lanes(rows)
    right_stop = jnp.where(place.has[2][1], right_end, 0)
    left_start = jnp.where(place.has[2][-1], 120, 128)
    return ((lane >= start) & (lane < right_stop)) | (lane >= left_start)


def slab_weight(place, x, extent):
    if 0 <= x < extent:
        return None
    return place.has[0][x // extent].astype(jnp.float32)


def z_back(a, h):
    lane0 = lanes(a.shape[0]) == 0
    ra, rh = pltpu.roll(a, 1, 1), pltpu.roll(h, 1, 1)
    return jnp.where(lane0, rh, ra), jnp.where(lane0, ra, rh)


def z_next(a, h):
    lane127 = lanes(a.shape[0]) == 127
    ra, rh = pltpu.roll(a, 127, 1), pltpu.roll(h, 127, 1)
    return jnp.where(lane127, rh, ra), jnp.where(lane127, ra, rh)


def masks0(place, first_row, rows):
    inner = row_mask(place, first_row, rows, BY)
    rim = inner & rim_lanes(place, rows, 0, 8)
    return inner.astype(jnp.float32), rim.astype(jnp.float32)


def scaled(value, mask, weight):
    value = value * mask
    return value if weight is None else value * weight


def six0(ref, i, r, n, rim=True):
    a, h = ref[0, i, r : r + n, :], ref[1, i, r : r + n, :]
    ba, bh = z_back(a, h)
    na, nh = z_next(a, h)
    out = []
    for t, (c, b, f) in enumerate(((a, ba, na), (h, bh, nh))):
        if t and not rim:
            break
        s = (
            (ref[t, i - 1, r : r + n, :] + ref[t, i + 1, r : r + n, :])
            + (ref[t, i, r - 1 : r - 1 + n, :] + ref[t, i, r + 1 : r + 1 + n, :])
            + (b + f)
        )
        out.append((c, s))
    return out


def six1(ref, i, r, n):
    c = ref[i, r : r + n, :]
    s = (
        (ref[i - 1, r : r + n, :] + ref[i + 1, r : r + n, :])
        + (ref[i, r - 1 : r - 1 + n, :] + ref[i, r + 1 : r + 1 + n, :])
        + (pltpu.roll(c, 1, 1) + pltpu.roll(c, 127, 1))
    )
    return c, s


def pick(a, m):
    high = a.astype(jnp.bfloat16)
    low = (a - high.astype(jnp.float32)).astype(jnp.bfloat16)
    return jnp.dot(high, m, preferred_element_type=jnp.float32) + jnp.dot(
        low, m, preferred_element_type=jnp.float32
    )


def turn(value, shift):
    shift %= 128
    return pltpu.roll(value, shift, 1) if shift else value


def pack0(load, store, count=BX):
    lane = lanes(BY)
    first = jnp.zeros((BY, 128), jnp.float32)
    last = jnp.zeros((BY, 128), jnp.float32)
    for i in range(count):
        turned = turn(load(i), 8 * i)
        first = jnp.where((lane >= 8 * i) & (lane < 8 * i + 8), turned, first)
        at = (8 * i - 8) % 128
        last = jnp.where((lane >= at) & (lane < at + 8), turned, last)
    store(first, last)


def beside(x, count):
    return (0, x) if 0 <= x < count else ((-1, x + count) if x < 0 else (1, x - count))


def unpack0(land, x, rows):
    dx, i = beside(x, BX)
    return unpack_columns(land[0, dx + 1], land[1, dx + 1], i, rows)


def unpack_columns(left, right, i, rows):
    left, right = turn(left, -8 * i), turn(right, -8 * i)
    lane = lanes(rows)
    return jnp.where(lane < 8, right, jnp.where(lane >= 120, left, 0.0))


def rim_copies(source, land, offsets):
    out = []
    for offset in offsets:
        dx, dy, dz = offset
        if dz == 0:
            continue
        y0, yd, ny = part(dy, BY, 8)
        side = 0 if dz > 0 else 1
        out.append((offset, source(side, y0, ny), land(side, 1 - dx, yd, ny)))
    return out


def block_copies(source, land, reach, offsets, edge=None):
    out = []
    for offset in offsets:
        dx, dy, dz = offset
        if dz != 0:
            continue
        near, far = edge if edge and dy else reach
        if dx == 0:
            x0, xd, nx = 0, 0, BX
        elif dx > 0:
            x0, xd, nx = BX - far, -far, far - near + 1
        else:
            x0, xd, nx = near - 1, BX + near - 1, far - near + 1
        y0, yd, ny = part(dy, BY, 8)
        out.append((offset, source(x0, nx, y0, ny), land(xd, nx, yd, ny)))
    return out


def ordered(copies):
    return sorted(copies, key=lambda c: -sum(abs(d) for d in c[0]))


def clear_around(ref, lead_x, lead_y, count_y):
    nx, ny = ref.shape[0], ref.shape[1]
    ref[0:lead_x] = jnp.zeros((lead_x, ny, 128), jnp.float32)
    ref[lead_x + BX : nx] = jnp.zeros((nx - lead_x - BX, ny, 128), jnp.float32)
    ref[lead_x : lead_x + BX, 0:lead_y, :] = jnp.zeros((BX, lead_y, 128), jnp.float32)
    end = lead_y + count_y
    ref[lead_x : lead_x + BX, end:ny, :] = jnp.zeros((BX, ny - end, 128), jnp.float32)


def clear(*refs):
    for ref in refs:
        ref[...] = jnp.zeros(ref.shape, ref.dtype)


def kernel(
    sizes, p_ref, w_ref, out_ref,
    b0, far, sb, v0, t0, zs0, zr0, wind, zsw, zrw, zsx, zrx, coef, velocity, flux,
    vp, zsv, zrv,
    bv, zsb, zrb, s1, l1, l1_far, zs1, zr1, zr1_far, b1, v1, t1,
    gathered, merged, c2, e2a, e2b,
    rows0, rows2, up1, up0, m_down0, m_down1, m_up1, m_up0,
    ruler, send_sems, recv_sems, load_sems,
):
    place = Place(sizes)
    load_p = pltpu.make_async_copy(
        p_ref, b0.at[0, pl.ds(8, BX), pl.ds(16, BY), :], load_sems.at[0])
    load_w = pltpu.make_async_copy(
        w_ref, wind.at[:, 0, pl.ds(3, BX), pl.ds(8, BY), :], load_sems.at[1])
    load_p.start()
    load_w.start()

    clear_around(b0.at[0], 8, 16, BY)
    for d in range(3):
        clear_around(wind.at[d, 0], 3, 8, BY)
    clear(far, zr0, zrw, zrx, gathered)

    barrier = pltpu.get_barrier_semaphore()
    total = jnp.int32(0)
    for offset in GREETED:
        there = place.exists(offset)
        total = total + there.astype(jnp.int32)

        def greet(offset=offset):
            pl.semaphore_signal(
                barrier, inc=1, device_id=place.device(offset), device_id_type=MESH
            )

        pl.when(there)(greet)

    def storer(ref):
        def store(f, l):
            ref[0] = l
            ref[1] = f
        return store

    clear(vp, zrv, bv, zrb, l1, l1_far, zr1, zr1_far)
    clear(b0.at[1], v0, t0, rows0)
    load_p.wait()
    pack0(lambda i: b0[0, 8 + i, 16:32, :], storer(zs0))

    used = [0]

    def exchange(copies):
        k = used[0]
        used[0] += 1
        return Exchange(place, ordered(copies), send_sems.at[k], recv_sems.at[k], ruler)

    def far_block(x, nx, y, ny):
        side, lead = (0, 8) if x < 0 else (1, -BX - 5)
        return far.at[side, pl.ds(x + lead, nx), pl.ds(y + 16, ny), :]

    def b0_block(x, nx, y, ny):
        return b0.at[0, pl.ds(x + 8, nx), pl.ds(y + 16, ny), :]

    def wind_block(x, nx, y, ny):
        return wind.at[:, 0, pl.ds(x + 3, nx), pl.ds(y + 8, ny), :]

    def vp_block(x, nx, y, ny):
        return vp.at[pl.ds(x + 2, nx), pl.ds(y + 16, ny), :]

    def wind_side_copies():
        out = []
        for offset in AROUND:
            dx, dy, dz = offset
            if dx and dz:
                y0, yd, ny = part(dy, BY, 8)
                side = 0 if dz > 0 else 1
                out.append((
                    offset, zsx.at[side, (dx + 1) // 2, pl.ds(y0, ny), :],
                    zrx.at[side, (1 - dx) // 2, pl.ds(yd + 8, ny), :]))
        return out

    ex0 = exchange(
        block_copies(b0_block, b0_block, (1, 6), AROUND, (1, 5))
        + rim_copies(
            lambda s, y, ny: zs0.at[s, pl.ds(y, ny), :],
            lambda s, dx, y, ny: zr0.at[s, dx, pl.ds(y + 8, ny), :], AROUND))
    sides = [d for d in AROUND if d[0]]
    ex_far = exchange(
        block_copies(b0_block, far_block, (7, 8), [d for d in sides if d[2] == 0], (6, 7)))
    exw = exchange(
        block_copies(wind_block, wind_block, (1, 3), AROUND, (1, 2))
        + rim_copies(
            lambda s, y, ny: zsw.at[s, :, pl.ds(y, ny), :],
            lambda s, dx, y, ny: zrw.at[s, :, pl.ds(y + 8, ny), :],
            [d for d in AROUND if not d[0]])
        + wind_side_copies())
    exv = exchange(
        block_copies(vp_block, vp_block, (1, 2), NEAR, (1, 1))
        + rim_copies(
            lambda s, y, ny: zsv.at[s, pl.ds(y, ny), :],
            lambda s, dx, y, ny: zrv.at[s, dx, pl.ds(y + 8, ny), :], NEAR))

    def bv_copies():
        out = []
        for offset in AROUND:
            dx, dy, dz = offset
            if dz == 0:
                n = 5 if dx and dy else 6
                skip = 6 - n if dx > 0 else 0
                out.append((
                    offset, bv.at[pl.ds(6 + skip, n), pl.ds(16, 8), :],
                    bv.at[pl.ds(6 - 6 * dx + skip, n), pl.ds(16 - 8 * dy, 8), :]))
            else:
                side = 0 if dz > 0 else 1
                out.append((
                    offset, zsb.at[side], zrb.at[side, 1 - dx, pl.ds(8 - 8 * dy, 8), :]))
        return out

    def level1_copies(reach, edge, offsets, blocks, rims):
        out = []
        for offset in offsets:
            dx, dy, dz = offset
            if dz == 0:
                near, far_end = edge if dx and dy else reach
                if dx == 0:
                    x0, xd, nx = 0, 0, 6
                elif dx > 0:
                    x0, xd, nx = 6 - far_end, -far_end, far_end - near + 1
                else:
                    x0, xd, nx = near - 1, 5 + near, far_end - near + 1
                out.append((
                    offset, s1.at[pl.ds(x0, nx)],
                    blocks.at[pl.ds(xd + 4, nx), pl.ds(8 - 8 * dy, 8), :]))
            else:
                side = 0 if dz > 0 else 1
                out.append((
                    offset, zs1.at[side], rims.at[side, 1 - dx, pl.ds(8 - 8 * dy, 8), :]))
        return out

    def coarse_copies(number):
        return [
            (d, gathered.at[number, 2, 1, 2], gathered.at[number, 2 - d[1], 1 - d[2], 2 - d[0]])
            for d in COARSE[number]
        ]

    exb = exchange(bv_copies())
    ex1 = exchange(level1_copies((1, 2), (1, 1), NEAR, l1, zr1))
    ex1_far = exchange(level1_copies(
        (3, 4), (2, 4), [d for d in AROUND if d[0] and (d[2] == 0 or d[1])], l1_far, zr1_far))
    ex2 = [exchange(coarse_copies(0)), exchange(coarse_copies(1))]

    pl.semaphore_wait(barrier, total)
    ex0.start()
    ex_far.start()

    load_w.wait()
    for d in range(3):
        pack0(lambda i: wind[d, 0, 3 + i, 8:24, :], storer(zsw.at[:, d]))
    for high, lead in ((0, 3), (1, BX)):
        pack0(lambda i: wind[i // 3, 0, lead + i % 3, 8:24, :], storer(zsx.at[:, high]), 9)
    exw.start()

    clear(velocity, flux, sb, b1, v1, t1, merged, c2, e2a, e2b, rows2, up1, up0)

    bf16 = jnp.bfloat16
    k = lax.broadcasted_iota(jnp.int32, (128, 128), 0)
    l = lax.broadcasted_iota(jnp.int32, (128, 128), 1)
    eighth = jnp.float32(0.125)
    m_down0[0:128, :] = jnp.where(k // 2 == l, eighth, 0.0).astype(bf16)
    m_down0[128:256, :] = jnp.where(
        ((k < 8) | (k >= 120)) & (k // 2 + 64 == l), eighth, 0.0).astype(bf16)
    for i in range(3):
        m_down1[i * 128 : i * 128 + 128, :] = jnp.where(
            (l // 32 == i) & (k // 2 == l % 32), eighth, 0.0).astype(bf16)
    m_up1[...] = jnp.where(
        ((l < 72) & (k == l // 2)) | ((l >= 120) & (k == 64 + l // 2)), 1.0, 0.0).astype(bf16)
    m_up0[:, 0:128] = jnp.where(k == l // 2, 1.0, 0.0).astype(bf16)
    m_up0[:, 128:256] = jnp.where(
        ((l < 8) | (l >= 120)) & (k == 64 + l // 2), 1.0, 0.0).astype(bf16)

    c0 = OMEGA / 6.0
    w1 = 0.25
    c1 = OMEGA / (6.0 * w1)
    w2 = 0.0625
    c2s = OMEGA / (6.0 * w2)
    lane8, lane16, lane24, lane40 = lanes(8), lanes(16), lanes(24), lanes(40)
    m32a, m32h = masks0(place, -8, 32)
    m24a, m24h = masks0(place, -4, 24)
    mask32, mask24 = (m32a, m32h), (m24a, m24h)
    mask16 = masks0(place, 0, 16)

    def span(reach, x):
        left = reach - max(-x, x - BX + 1, 0)
        if left <= 0:
            return 16, 16, mask16, False
        if left <= 4:
            return 12, 24, mask24, True
        return 8, 32, mask32, True


    def level1_mask(first_row, rows):
        lane = lanes(rows)
        inside = row_mask(place, first_row, rows, 8)
        return (inside & ((lane < 64) | rim_lanes(place, rows, 64, 72))).astype(jnp.float32)

    def scaled_masks(masks, factor, weight):
        factor = factor if weight is None else factor * weight
        return [m * factor for m in masks]

    def sweep0(target, iterate, x, reach):
        r, n, masks, rim = span(reach, x)
        weight = slab_weight(place, x, BX)
        keep, share = scaled_masks(masks, KEEP, weight), scaled_masks(masks, SIXTH, weight)
        for t, (c, s) in enumerate(six0(iterate, x + 8, r, n, rim)):
            target[t, x + 8, r : r + n, :] = keep[t] * c + share[t] * s + sb[t, x + 8, r : r + n, :]

    def scale_source(x, r, n, masks):
        factor = scaled_masks(masks, c0, slab_weight(place, x, BX))
        for t in range(2):
            sb[t, x + 8, r : r + n, :] = factor[t] * b0[t, x + 8, r : r + n, :]

    def first_two0(slabs, reach):
        for x in slabs:
            r, n, masks, rim = span(reach, x)
            factors = scaled_masks(masks, c0, slab_weight(place, x, BX))
            for t, (c, s) in enumerate(six0(b0, x + 8, r, n, rim)):
                v0[t, x + 8, r : r + n, :] = factors[t] * ((1.0 + KEEP) * c + SIXTH * s)

    def down1_and_send(number, r, n):
        pairs = []
        for i in range(3):
            pair = None
            for x in (2 * i, 2 * i + 1):
                c, s = six1(v1, x + 6, 16, 8)
                res = b1[x + 6, 16:24, :] - w1 * (6.0 * c - s)
                pair = res if pair is None else pair + res
            pairs.append(jnp.where(lane8 < 64, pair, 0.0))
        rows2[...] = pick(jnp.concatenate(pairs, axis=1), m_down1[...])
        gathered[number, 2, 1, 2] = (
            rows2[pl.ds(0, 4, stride=2), :] + rows2[pl.ds(1, 4, stride=2), :])
        ex2[number].start()

    def coarse(number, reach):
        for az in range(3):
            for ax in range(5):
                for ay in range(5):
                    merged[az, ax, 4 * ay : 4 * ay + 4, :] = gathered[number, ay, az, ax]
        for x in range(-reach - 3, 3 + reach + 3):
            ax, i = (x + 6) // 3, (x + 6) % 3
            left = turn(merged[0, ax], 96 - 32 * i)
            own = turn(merged[1, ax], -32 * i)
            right = turn(merged[2, ax], 32 - 32 * i)
            c2[x + 6] = jnp.where(
                lane24 < 32, own, jnp.where(lane24 < 40, right, jnp.where(lane24 >= 120, left, 0.0)))
        inside = row_mask(place, -6, 16, 4)
        mask2 = (inside & ((lane16 < 32) | rim_lanes(place, 16, 32, 40))).astype(jnp.float32)
        for x in range(-reach - 2, 3 + reach + 2):
            c, s = six1(c2, x + 6, 2, 16)
            value = (1.0 + KEEP) * c2s * c + SIXTH * c2s * s
            e2a[x + 6, 2:18, :] = scaled(value, mask2, slab_weight(place, x, 3))
        here, there = e2a, e2b
        for more in (1, 0):
            for x in range(-reach - more, 3 + reach + more):
                c, s = six1(here, x + 6, 2, 16)
                value = KEEP * c + SIXTH * s + c2s * c2[x + 6, 2:18, :]
                there[x + 6, 2:18, :] = scaled(value, mask2, slab_weight(place, x, 3))
            here, there = there, here
        return here

    def spread1(here, reach, y, n):
        slabs = 3 + 2 * reach
        spread = pick(
            jnp.concatenate([here[x - reach + 6, y + 8 : y + 8 + n, :] for x in range(slabs)], axis=0),
            m_up1[...])
        for j in range(slabs):
            value = spread[n * j : n * j + n, :]
            up1[j, pl.ds(0, n, stride=2), :] = value
            up1[j, pl.ds(1, n, stride=2), :] = value

    def last_two1(reach, r, n, mask):
        for x in range(-reach - 1, 6 + reach + 1):
            c, s = six1(v1, x + 6, r, n)
            value = KEEP * c + SIXTH * s + c1 * b1[x + 6, r : r + n, :]
            t1[x + 6, r : r + n, :] = scaled(value, mask, slab_weight(place, x, 6))
        for x in range(-reach, 6 + reach):
            c, s = six1(t1, x + 6, r, n)
            value = KEEP * c + SIXTH * s + c1 * b1[x + 6, r : r + n, :]
            v1[x + 6, r : r + n, :] = scaled(value, mask, slab_weight(place, x, 6))

    def spread0(reach, n):
        y = -(n - 8) // 2
        slabs = 6 + 2 * reach
        spread = pick(
            jnp.concatenate(
                [v1[x - reach + 6, y + 16 : y + 32, :] for x in range(slabs)], axis=0),
            m_up0[...])
        for j in range(slabs):
            for t in range(2):
                value = spread[16 * j : 16 * j + n, 128 * t : 128 * t + 128]
                up0[t, j, pl.ds(0, n, stride=2), :] = value
                up0[t, j, pl.ds(1, n, stride=2), :] = value

    ex0.wait_recv()
    for x in range(-6, BX + 6):
        r, n = span(6, x)[:2]
        b0[1, x + 8, r : r + n, :] = unpack0(zr0.at[:, :, pl.ds(r - 8, n), :], x, n)
    first_two0(range(-5, BX + 5), 5)
    for i in range(10):
        pair = [None, None]
        r, n, rim = (12, 24, True) if 0 < i < 9 else (16, 16, False)
        for x in (2 * i - 4, 2 * i - 3):
            for t, (c, s) in enumerate(six0(v0, x + 8, r, n, rim)):
                res = b0[t, x + 8, r : r + n, :] - (6.0 * c - s)
                pair[t] = res if pair[t] is None else pair[t] + res
        for t in range(1 + rim):
            rows0[t, i, r - 12 : r - 12 + n, :] = pair[t]
    cells = [
        jnp.concatenate(
            [rows0[t, i, pl.ds(0, 16, stride=2), :] + rows0[t, i, pl.ds(1, 16, stride=2), :]
             for t in range(2)], axis=1)
        for i in range(10)
    ]
    source = pick(jnp.concatenate(cells, axis=0), m_down0[...])
    mask = level1_mask(-2, 16)
    for x in range(-2, 8):
        b1[x + 6, 14:30, :] = scaled(
            source[16 * (x + 2) : 16 * (x + 2) + 16, :], mask, slab_weight(place, x, 6))
    for x in range(-1, 7):
        c, s = six1(b1, x + 6, 14, 16)
        value = (1.0 + KEEP) * c1 * c + SIXTH * c1 * s
        v1[x + 6, 14:30, :] = scaled(value, mask, slab_weight(place, x, 6))
    down1_and_send(0, 14, 16)

    low = jnp.zeros((8, 128), jnp.float32)
    high = jnp.zeros((8, 128), jnp.float32)
    for i in range(6):
        block_b, block_v = b1[i + 6, 16:24, :], v1[i + 6, 16:24, :]
        bv[i + 6, 16:24, :] = jnp.where(lane8 < 64, block_b, pltpu.roll(block_v, 64, 1))
        for block, lead in ((block_b, 0), (block_v, 64)):
            group = (lane8 >= lead + 8 * i) & (lane8 < lead + 8 * i + 8)
            low = jnp.where(group, turn(block, lead + 8 * i), low)
            high = jnp.where(group, turn(block, lead + 8 * i - 56), high)
    zsb[0] = high
    zsb[1] = low
    exb.start()
    ex0.wait_send()
    ex_far.wait_recv()
    for side in range(2):
        for k in range(3):
            x = k - 8 if side == 0 else BX + 5 + k
            distance = -x if side == 0 else x - BX + 1
            if distance > 6:
                b0[0, x + 8, 16:32, :] = far[side, k, 16:32, :]
            if distance < 8:
                for r in (8, 32):
                    b0[0, x + 8, r : r + 8, :] = far[side, k, r : r + 8, :]
    outer = [x for k in range(1, 9) for x in (-k, BX - 1 + k)]
    for x in outer:
        b0[1, x + 8, 8:40, :] = unpack0(zr0, x, 32)
    first_two0(outer[:14], 7)
    for x in range(-6, BX + 6):
        scale_source(x, 8, 32, mask32)
    ex_far.wait_send()
    exw.wait_recv()
    for x in range(-3, BX + 3):
        ones = scaled_masks(mask24, 1.0, slab_weight(place, x, BX))
        halves = scaled_masks(mask24, 0.5, slab_weight(place, x, BX))
        for d in range(3):
            if 0 <= x < BX:
                rim = unpack_columns(zrw[0, d, 4:28, :], zrw[1, d, 4:28, :], x, 24)
            else:
                high, i = (0, x + 3) if x < 0 else (1, x - BX)
                rim = unpack_columns(
                    zrx[0, high, 4:28, :], zrx[1, high, 4:28, :], 3 * d + i, 24)
            for t, w in enumerate((wind[d, 0, x + 3, 4:28, :], rim)):
                half = halves[t] * w
                coef[d, 0, t, x + 3] = half - ones[t]
                coef[d, 1, t, x + 3] = -half - ones[t]
    exw.wait_send()
    ex2[0].wait_recv()
    here = coarse(0, 3)
    spread1(here, 3, -4, 16)
    exb.wait_recv()
    mask = level1_mask(-8, 24)
    for x in range(-6, 12):
        dx, i = beside(x, 6)
        near = bv[x + 6, 8:32, :]
        left, right = zrb[0, dx + 1], zrb[1, dx + 1]
        for lead, ref in ((0, b1), (64, v1)):
            value = jnp.where(
                lane24 < 64, turn(near, -lead),
                jnp.where(lane24 < 72, turn(right, 64 - 8 * i - lead),
                          jnp.where(lane24 >= 120, turn(left, 120 - 8 * i - lead), 0.0)))
            if ref is v1:
                value = value + up1[(x + 6) // 2, 0:24, :]
            ref[x + 6, 8:32, :] = value
    last_two1(4, 8, 24, mask)
    spread0(4, 16)
    for x in range(-7, BX + 7):
        for t in range(2):
            v0[t, x + 8, 8:40, :] += up0[t, (x + 8) // 2]
    for reach, target, iterate in ((6, t0, v0), (5, v0, t0)):
        for x in range(-reach, BX + reach):
            sweep0(target, iterate, x, reach)
    first = v0

    for x in range(-4, BX + 4):
        r, n, masks, rim = span(4, x)
        halves = scaled_masks(masks, 0.5, slab_weight(place, x, BX))
        i = x + 8
        rows = slice(r, r + n)
        a, h = first[0, i, rows, :], first[1, i, rows, :]
        ba, bh = z_back(a, h)
        na, nh = z_next(a, h)
        for t, (back, ahead) in enumerate(((ba, na), (bh, nh))[: 1 + rim]):
            m = halves[t]
            velocity[0, t, x + 4, rows, :] = (first[t, i + 1, rows, :] - first[t, i - 1, rows, :]) * m
            velocity[1, t, x + 4, rows, :] = (
                first[t, i, r + 1 : r + 1 + n, :] - first[t, i, r - 1 : r - 1 + n, :]) * m
            velocity[2, t, x + 4, rows, :] = (ahead - back) * m
    for x in range(-3, BX + 3):
        r, n, masks, rim = span(3, x)
        i = x + 4
        rows, low_rows = slice(r, r + n), slice(r - 8, r - 8 + n)
        sevens = scaled_masks(masks, 7.0, slab_weight(place, x, BX))
        ways = [
            [[coef[e, k, t, x + 3, r - 12 : r - 12 + n, :] for k in range(2)] for e in range(3)]
            for t in range(1 + rim)
        ]
        for d in range(3):
            u = velocity.at[d]
            a, h = u[0, i, rows, :], u[1, i, rows, :]
            ba, bh = z_back(a, h)
            na, nh = z_next(a, h)
            for t, (c, back, ahead) in enumerate(((a, ba, na), (h, bh, nh))[: 1 + rim]):
                x_low, x_high = u[t, i - 1, rows, :], u[t, i + 1, rows, :]
                y_low, y_high = u[t, i, r - 1 : r - 1 + n, :], u[t, i, r + 1 : r + 1 + n, :]
                along_x, along_y, along_z = ways[t]
                flux[d, t, x + 3, low_rows, :] = (
                    sevens[t] * c
                    + (along_x[0] * x_high + along_x[1] * x_low)
                    + (along_y[0] * y_high + along_y[1] * y_low)
                    + (along_z[0] * ahead + along_z[1] * back)
                )
    for x in range(-2, BX + 2):
        r, n, masks, rim = span(2, x)
        halves = scaled_masks(masks, -0.5, slab_weight(place, x, BX))
        i = x + 3
        q = r - 8
        rows = slice(q, q + n)
        a, h = flux[2, 0, i, rows, :], flux[2, 1, i, rows, :]
        ba, bh = z_back(a, h)
        na, nh = z_next(a, h)
        for t, (back, ahead) in enumerate(((ba, na), (bh, nh))[: 1 + rim]):
            value = (
                (flux[0, t, i + 1, rows, :] - flux[0, t, i - 1, rows, :])
                + (flux[1, t, i, q + 1 : q + 1 + n, :] - flux[1, t, i, q - 1 : q - 1 + n, :])
                + (ahead - back)
            )
            b0[t, x + 8, r : r + n, :] = value * halves[t]

    first_two0(range(-1, BX + 1), 1)
    for i in range(6):
        pair = None
        for x in (2 * i, 2 * i + 1):
            ((c, s),) = six0(v0, x + 8, 16, 16, rim=False)
            res = b0[0, x + 8, 16:32, :] - (6.0 * c - s)
            pair = res if pair is None else pair + res
        rows0[0, i, 0:16, :] = pair
    cells = [rows0[0, i, pl.ds(0, 8, stride=2), :] + rows0[0, i, pl.ds(1, 8, stride=2), :] for i in range(6)]
    source = pick(jnp.concatenate(cells, axis=0), m_down0[0:128, :])
    low = jnp.zeros((8, 128), jnp.float32)
    high = jnp.zeros((8, 128), jnp.float32)
    for i in range(6):
        block = source[8 * i : 8 * i + 8, :]
        s1[i] = block
        l1[4 + i, 8:16, :] = block
        group = (lane8 >= 8 * i) & (lane8 < 8 * i + 8)
        low = jnp.where(group, turn(block, 8 * i), low)
        high = jnp.where(group, turn(block, 8 * i - 56), high)
    zs1[0] = high
    zs1[1] = low
    ex1.start()
    ex1_far.start()
    for x in range(BX):
        vp[x + 2, 16:32, :] = v0[0, x + 8, 16:32, :]
    pack0(lambda i: v0[0, 8 + i, 16:32, :], storer(zsv))
    exv.start()
    ex2[0].wait_send()
    exb.wait_send()
    ex1.wait_recv()
    mask = level1_mask(-4, 16)

    def source1(slabs, block, rim):
        for x in slabs:
            dx, i = beside(x, 6)
            b1[x + 6, 8:32, :] = jnp.where(
                lane24 < 64, block(x + 4),
                jnp.where(lane24 < 72, turn(rim(1, dx + 1), 64 - 8 * i),
                          jnp.where(lane24 >= 120, turn(rim(0, dx + 1), 120 - 8 * i), 0.0)))

    def first_two1(reach):
        for x in range(-reach, 6 + reach):
            factors = scaled_masks((mask,), c1, slab_weight(place, x, 6))
            c, s = six1(b1, x + 6, 12, 16)
            v1[x + 6, 12:28, :] = factors[0] * ((1.0 + KEEP) * c + SIXTH * s)

    source1(range(-2, 8), lambda k: l1[k], lambda side, k: zr1[side, k])
    first_two1(1)
    down1_and_send(1, 12, 16)
    ex1_far.wait_recv()
    source1(
        range(-4, 10), lambda k: l1[k] + l1_far[k],
        lambda side, k: zr1[side, k] + zr1_far[side, k])
    first_two1(3)
    ex1.wait_send()
    ex1_far.wait_send()
    exv.wait_send()
    exv.wait_recv()
    for x in range(-1, BX + 1):
        scale_source(x, 12, 24, mask24)
    for x in range(-2, BX + 2):
        v0[0, x + 8, 12:36, :] = vp[x + 2, 12:36, :]
        v0[1, x + 8, 8:40, :] = unpack0(zrv, x, 32)
    ex2[1].wait_recv()
    here = coarse(1, 2)
    spread1(here, 2, -2, 8)
    for x in range(-3, 9):
        v1[x + 6, 12:28, :] += up1[(x + 4) // 2, 0:16, :]
    last_two1(1, 12, 16, mask)
    spread0(1, 12)
    for x in range(-2, BX + 2):
        for t in range(2):
            v0[t, x + 8, 12:36, :] += up0[t, (x + 2) // 2, 0:24, :]
    for x in range(-1, BX + 1):
        sweep0(t0, v0, x, 1)
    for x in range(BX):
        ((c, s),) = six0(t0, x + 8, 16, 16, rim=False)
        out_ref[x] = KEEP * c + SIXTH * s + sb[0, x + 8, 16:32, :]
    ex2[1].wait_send()


def solution(mesh):
    sizes = tuple(mesh.shape[a] for a in AXES)
    exchanges = 9
    f32 = jnp.float32
    bf16 = jnp.bfloat16

    def vmem(*shape, dtype=f32):
        return pltpu.VMEM(shape, dtype)

    def body(pressure, wind):
        return pl.pallas_call(
            functools.partial(kernel, sizes),
            out_shape=jax.ShapeDtypeStruct((BX, BY, BZ), f32),
            in_specs=[pl.BlockSpec(memory_space=pl.ANY)] * 2,
            out_specs=pl.BlockSpec(memory_space=pltpu.VMEM),
            scratch_shapes=[
                vmem(2, 28, 48, 128),
                vmem(2, 3, 48, 128),
                vmem(2, 28, 48, 128),
                vmem(2, 28, 48, 128),
                vmem(2, 28, 48, 128),
                vmem(2, 16, 128),
                vmem(2, 3, 32, 128),
                vmem(3, 1, 18, 32, 128),
                vmem(2, 3, 16, 128),
                vmem(2, 3, 32, 128),
                vmem(2, 2, 16, 128),
                vmem(2, 2, 32, 128),
                vmem(3, 2, 2, 18, 24, 128),
                vmem(3, 2, 20, 48, 128),
                vmem(3, 2, 18, 32, 128),
                vmem(16, 48, 128),
                vmem(2, 16, 128),
                vmem(2, 3, 32, 128),
                vmem(18, 40, 128),
                vmem(2, 8, 128),
                vmem(2, 3, 24, 128),
                vmem(6, 8, 128),
                vmem(14, 24, 128),
                vmem(14, 24, 128),
                vmem(2, 8, 128),
                vmem(2, 3, 24, 128),
                vmem(2, 3, 24, 128),
                vmem(18, 40, 128),
                vmem(18, 40, 128),
                vmem(18, 40, 128),
                vmem(2, 5, 3, 5, 4, 128),
                vmem(3, 5, 24, 128),
                vmem(15, 24, 128),
                vmem(15, 24, 128),
                vmem(15, 24, 128),
                vmem(2, 10, 32, 128),
                vmem(8, 128),
                vmem(9, 32, 128),
                vmem(2, 14, 32, 128),
                vmem(256, 128, dtype=bf16),
                vmem(384, 128, dtype=bf16),
                vmem(128, 128, dtype=bf16),
                vmem(128, 256, dtype=bf16),
                vmem(512, 4, 128),
                pltpu.SemaphoreType.DMA((exchanges,)),
                pltpu.SemaphoreType.DMA((exchanges,)),
                pltpu.SemaphoreType.DMA((2,)),
            ],
            compiler_params=pltpu.CompilerParams(
                collective_id=0, has_side_effects=True, vmem_limit_bytes=56400000
            ),
            name="schur",
        )(pressure, wind)

    in_specs = (P("gx", "gy", "gz"), P(None, "gx", "gy", "gz"))
    return jax.shard_map(
        body, mesh=mesh, in_specs=in_specs, out_specs=P("gx", "gy", "gz"), check_vma=False
    )
```
